256 devices in a mesh: tower: 16 (over z, x_hi), dev: 16 (over x_lo, y, core).
Axes of the slice: x: 4 (x_hi: 2, x_lo: 2; x = x_hi * 2 + x_lo), y: 4, z: 8, core: 2. Of those that a mesh axis runs over, the one named last changes fastest.
Arguments:
- ids: int32 [16, 16, 2048, 32], P('tower', 'dev'), may hold values from 0 to 511
- tables: bfloat16 [16, 16, 512, 128], P('tower', 'dev'), may hold values from -1 to 1
- order: int32 [2048], replicated, may hold values from 0 to 2047, each once
- w_first: bfloat16 [16, 2048, 1024], P('tower', 'dev'), may hold values from -0.125 to 0.125
- w_second: bfloat16 [16, 1024, 512], P('tower'), may hold values from -0.1875 to 0.1875
- w_head: bfloat16 [8192, 128], replicated, may hold values from -0.0625 to 0.0625
- w_interact: float32 [256, 128], replicated, may hold values from -0.1875 to 0.1875
Outputs:
- scores: float32 [16, 128, 128], P('dev', 'tower')
The draws below stay inside these ranges and needn't reach their ends.
Inputs may be any that keep to these rules, and one draw needn't show every extreme that they name: order is a permutation of the batch rows 0 to 2047.
All inputs are finite; a program needn't handle non-finite values.
Results may differ from the reference program's by a relative error of at most 0.0023.
Values may be sent and summed in bfloat16 or wider, within the bound.
A program may use at most 64 MiB of HBM per device.

```python
import math
import jax
import jax.numpy as jnp
from jax import lax

EMB = 128
ACTIVE = 512
BAG = 32
FEATS = 16
HIDDEN_SIZE = 1024
ZWIDTH = 512
HEAD = 128
ROWS_DEV = 128
SAMPLES = 2048
TOWERS = 16
N_TOWER = 16
N_DEV = 16


def set_ends(values, stream_key, least, top_value):
    longest = values.shape.index(max(values.shape))
    spots = []
    for shift in (0, 1):
        where = [jax.random.randint(jax.random.fold_in(stream_key, axis), (), 0, length) for axis, length in enumerate(values.shape)]
        where[longest] = (where[longest] + shift) % values.shape[longest]
        spots.append(tuple(where))
    return values.at[spots[0]].set(least).at[spots[1]].set(top_value)


def block_scale(key, shape, shards, low, top_value):
    loudness = 1.0
    for position, blocks in shards:
        heights = jax.random.uniform(jax.random.fold_in(jax.random.fold_in(key, 6), position), (blocks,), jnp.float32, low / len(shards), top_value / len(shards))
        loudness = loudness * jnp.repeat(jnp.exp(heights), shape[position] // blocks).reshape((-1,) + (1,) * (len(shape) - 1 - position))
    return loudness


def gaussian(own_key, extent, deviation, reach, shards=(), kind=jnp.bfloat16):
    result = jax.random.normal(own_key, extent, jnp.float32) * deviation
    if len(shards) > 0:
        result = block_scale(own_key, extent, shards, -0.22, 0.18) * result
    return jnp.clip(result, min=-reach, max=reach).astype(kind)


def setup_inputs(seed: int = 0) -> dict:
    key_list = jax.random.split(jax.random.key(seed), 8)
    ids = set_ends(jax.random.randint(key_list[0], (TOWERS, FEATS, SAMPLES, BAG), 0, ACTIVE), jax.random.fold_in(key_list[0], 1), 0, ACTIVE - 1).astype(jnp.int32)
    tables = gaussian(key_list[1], (TOWERS, FEATS, ACTIVE, EMB), BAG ** -0.5, 1.0, ((0, 16), (1, 16)))
    order = jax.random.permutation(key_list[2], SAMPLES).astype(jnp.int32)
    w_first = gaussian(key_list[3], (TOWERS, FEATS * EMB, HIDDEN_SIZE), (FEATS * EMB) ** -0.5, 0.125, ((0, 16), (1, 16)))
    w_second = gaussian(key_list[4], (TOWERS, HIDDEN_SIZE, ZWIDTH), HIDDEN_SIZE ** -0.5, 0.1875, ((0, 16),))
    w_head = gaussian(key_list[5], (TOWERS * ZWIDTH, HEAD), (TOWERS * ZWIDTH) ** -0.5, 0.0625)
    w_interact = gaussian(key_list[6], (TOWERS * TOWERS, HEAD), (4 * TOWERS * TOWERS) ** -0.5, 0.1875, (), jnp.float32)
    return {"ids": ids, "tables": tables, "order": order, "w_first": w_first, "w_second": w_second, "w_head": w_head, "w_interact": w_interact}


def reference(ids, tables, order, w_first, w_second, w_head, w_interact):
    stacked_list = []
    for tower_index in range(N_TOWER):
        pieces = []
        for feature in range(FEATS):
            looked = jnp.take(tables[tower_index, feature], ids[tower_index, feature].astype(jnp.int32), axis=0)
            pooled = lax.optimization_barrier(jnp.sum(looked.astype(jnp.float32), axis=1))
            pieces.append(pooled.astype(jnp.bfloat16))
        features = jnp.take(jnp.concatenate(pieces, axis=1), order.astype(jnp.int32), axis=0)
        preact = jnp.dot(features, w_first[tower_index], preferred_element_type=jnp.float32)
        hidden = jnp.maximum(preact, 0.0).astype(jnp.bfloat16)
        outputs = jnp.dot(hidden, w_second[tower_index], preferred_element_type=jnp.float32).astype(jnp.bfloat16)
        stacked_list.append(outputs)
    stacked = jnp.stack(stacked_list)
    samples = stacked.shape[1]
    joined = jnp.transpose(stacked, (1, 0, 2)).reshape(samples, N_TOWER * ZWIDTH)
    head = jnp.dot(joined, w_head, preferred_element_type=jnp.float32)
    widened = stacked.astype(jnp.float32)
    products = jnp.einsum('tbz,sbz->bts', widened, widened, precision=lax.Precision.HIGHEST) / math.sqrt(ZWIDTH)
    interact_term = jnp.dot(products.reshape(samples, N_TOWER * N_TOWER), w_interact, precision=lax.Precision.HIGHEST)
    return (head + interact_term).reshape(N_DEV, ROWS_DEV, HEAD)
```

```python
import functools
import math

import jax
import jax.numpy as jnp
from jax import lax
from jax.experimental import pallas as pl
from jax.experimental.pallas import tpu as pltpu
from jax.sharding import PartitionSpec as P

MESH = pl.DeviceIdType.MESH
RING = 4
CORES = 2


def load(src, dst, sem):
    return pltpu.make_async_copy(src, dst, sem)


def pool(ids_ref, table_ref, pooled_ref):
    bag, samples = ids_ref.shape
    active = table_ref.shape[0]
    lanes = 128
    fields = active // lanes
    places = lax.broadcasted_iota(jnp.int32, (lanes, lanes), 0)

    def chunk(index, carry):
        start = pl.multiple_of(index * lanes, lanes)
        packed = jnp.zeros((lanes, lanes), jnp.int32)
        for j in range(bag):
            row = ids_ref[pl.ds(j, 1), pl.ds(start, lanes)]
            low = row & (lanes - 1)
            unit = jnp.left_shift(1, (row >> 7) << 3)
            packed = packed + jnp.where(low == places, unit, 0)
        turned = packed.T
        counts = jnp.concatenate(
            [
                ((turned >> (8 * field)) & 255).astype(jnp.float32).astype(jnp.bfloat16)
                for field in range(fields)
            ],
            axis=1,
        )
        pooled_ref[pl.ds(start, lanes), :] = jnp.dot(
            counts, table_ref[...], preferred_element_type=jnp.float32
        )
        return carry

    lax.fori_loop(0, samples // lanes, chunk, 0)


def kernel(
    ids_hbm,
    table_hbm,
    order_ref,
    first_hbm,
    second_hbm,
    head_hbm,
    inter_hbm,
    out_ref,
    ids_v,
    table_v,
    pooled,
    permuted,
    xsend,
    wbuf,
    xbuf,
    total,
    partial,
    second_v,
    outbox,
    inbox,
    head_v,
    inter_v,
    spread_hi,
    spread_lo,
    load_sem,
    w_send,
    w_recv,
    x_send,
    x_recv,
    p_send,
    p_recv,
    o_send,
    o_recv,
    towers,
    chips,
):
    tower = lax.axis_index("tower")
    dev = lax.axis_index("dev")
    core = lax.rem(dev, CORES)
    chip = dev // CORES
    col = chip // RING
    row = lax.rem(chip, RING)
    cols = chips // RING
    partner = dev + 1 - 2 * core

    def shifted(step, sign):
        dx, dy = step // RING, lax.rem(step, RING)
        return lax.rem(col + cols + sign * dx, cols) * RING + lax.rem(row + RING + sign * dy, RING)

    loads = [
        load(ids_hbm, ids_v, load_sem.at[0]),
        load(table_hbm, table_v, load_sem.at[1]),
        load(first_hbm, wbuf.at[chip], load_sem.at[2]),
        load(second_hbm, second_v, load_sem.at[3]),
        load(head_hbm, head_v, load_sem.at[4]),
        load(inter_hbm, inter_v, load_sem.at[5]),
    ]
    for copy in loads:
        copy.start()

    barrier = pltpu.get_barrier_semaphore()
    for step in range(1, towers):
        pl.semaphore_signal(
            barrier, inc=1, device_id={"tower": lax.rem(tower + step, towers)}, device_id_type=MESH
        )
    for step in range(1, chips):
        pl.semaphore_signal(
            barrier, inc=1, device_id={"dev": shifted(step, 1) * CORES + core}, device_id_type=MESH
        )
    pl.semaphore_signal(barrier, inc=1, device_id={"dev": partner}, device_id_type=MESH)

    loads[0].wait()
    loads[1].wait()
    pool(ids_v, table_v, pooled)
    loads[2].wait()
    pl.semaphore_wait(barrier, towers + chips - 1)

    def send_w(step):
        return pltpu.make_async_remote_copy(
            src_ref=wbuf.at[chip],
            dst_ref=wbuf.at[chip],
            send_sem=w_send.at[step],
            recv_sem=w_recv.at[chip],
            device_id={"dev": shifted(step, 1) * CORES + core},
            device_id_type=MESH,
        )

    def send_x(step):
        return pltpu.make_async_remote_copy(
            src_ref=xsend.at[shifted(step, 1)],
            dst_ref=xbuf.at[chip],
            send_sem=x_send.at[step],
            recv_sem=x_recv.at[chip],
            device_id={"dev": shifted(step, 1) * CORES + core},
            device_id_type=MESH,
        )

    for step in range(1, chips):
        send_w(step).start()

    rows = xsend.shape[1]

    def permute_block(block):
        def group(index, carry):
            base = block * rows + index * 16
            for q in range(16):
                source = order_ref[base + q]
                permuted[pl.ds(index * 16 + q, 1), :] = pooled[pl.ds(source, 1), :]
            return carry

        lax.fori_loop(0, rows // 16, group, 0)
        xsend[block] = permuted[...].astype(jnp.bfloat16)

    for step in range(1, chips):
        permute_block(shifted(step, 1))
        send_x(step).start()
    permute_block(chip)

    loads[5].wait()
    half_k = inter_v.shape[0]

    def widen(index, carry):
        start = pl.multiple_of(index * 16, 16)
        block = inter_v[pl.ds(start, 16), :]
        wide = jnp.broadcast_to(block[:, None, :], (16, 8, block.shape[1])).reshape(
            128, block.shape[1]
        )
        high = wide.astype(jnp.bfloat16)
        low = (wide - high.astype(jnp.float32)).astype(jnp.bfloat16)
        target = pl.multiple_of(index * 128, 128)
        spread_hi[pl.ds(target, 128), :] = high
        spread_lo[pl.ds(target, 128), :] = low
        return carry

    lax.fori_loop(0, half_k // 16, widen, 0)

    width = total.shape[2]
    tile = 256

    def product(x, w, first):
        for n in range(width // tile):
            part = jnp.dot(
                x, w[:, n * tile : (n + 1) * tile], preferred_element_type=jnp.float32
            ).reshape(2, rows // 2, tile)
            span = slice(n * tile, (n + 1) * tile)
            if first:
                total[:, :, span] = part
            else:
                total[:, :, span] += part

    product(xsend[chip], wbuf.at[chip], True)

    def arrive(step, carry):
        source = shifted(step, -1)
        pltpu.make_async_remote_copy(
            src_ref=wbuf.at[source],
            dst_ref=wbuf.at[source],
            send_sem=w_send.at[step],
            recv_sem=w_recv.at[source],
            device_id={"dev": partner},
            device_id_type=MESH,
        ).wait_recv()
        pltpu.make_async_remote_copy(
            src_ref=xbuf.at[source],
            dst_ref=xbuf.at[source],
            send_sem=x_send.at[step],
            recv_sem=x_recv.at[source],
            device_id={"dev": partner},
            device_id_type=MESH,
        ).wait_recv()
        product(xbuf[source], wbuf.at[source], False)
        return carry

    lax.fori_loop(1, chips, arrive, 0)

    swap = pltpu.make_async_remote_copy(
        src_ref=total.at[1 - core],
        dst_ref=partial,
        send_sem=p_send,
        recv_sem=p_recv,
        device_id={"dev": partner},
        device_id_type=MESH,
    )
    swap.start()
    loads[3].wait()
    swap.wait_recv()
    hidden = jnp.maximum(total[core] + partial[...], 0.0).astype(jnp.bfloat16)
    outputs = jnp.dot(hidden, second_v[...], preferred_element_type=jnp.float32)
    share = outbox.shape[1]
    outbox[...] = outputs.reshape(towers, share, outputs.shape[1]).astype(jnp.bfloat16)

    def send_o(step):
        peer = lax.rem(tower + step, towers)
        return pltpu.make_async_remote_copy(
            src_ref=outbox.at[peer],
            dst_ref=inbox.at[tower],
            send_sem=o_send.at[step],
            recv_sem=o_recv.at[tower],
            device_id={"tower": peer},
            device_id_type=MESH,
        )

    for step in range(1, towers):
        send_o(step).start()
    inbox[tower] = outbox[tower]
    loads[4].wait()

    def head_part(source):
        return jnp.dot(inbox[source], head_v[source], preferred_element_type=jnp.float32)

    def collect(step, value):
        source = lax.rem(tower + towers - step, towers)
        pltpu.make_async_remote_copy(
            src_ref=outbox.at[source],
            dst_ref=inbox.at[source],
            send_sem=o_send.at[step],
            recv_sem=o_recv.at[source],
            device_id={"dev": partner},
            device_id_type=MESH,
        ).wait_recv()
        return value + head_part(source)

    head = lax.fori_loop(1, towers, collect, head_part(tower))

    zwidth = inbox.shape[2]
    stacked = (
        inbox[...].astype(jnp.float32).reshape(towers * share, zwidth).astype(jnp.bfloat16)
    )
    gram = lax.dot_general(
        stacked, stacked, (((1,), (1,)), ((), ())), preferred_element_type=jnp.float32
    )
    left = lax.rem(lax.broadcasted_iota(jnp.int32, gram.shape, 0), share)
    right = lax.rem(lax.broadcasted_iota(jnp.int32, gram.shape, 1), share)
    gram = jnp.where(left == right, gram / math.sqrt(zwidth), 0.0)
    flat = jnp.concatenate(
        [gram[t * share : (t + 1) * share, :] for t in range(towers)], axis=1
    )
    flat_hi = flat.astype(jnp.bfloat16)
    flat_lo = (flat - flat_hi.astype(jnp.float32)).astype(jnp.bfloat16)
    interact = (
        jnp.dot(flat_hi, spread_hi[...], preferred_element_type=jnp.float32)
        + jnp.dot(flat_lo, spread_hi[...], preferred_element_type=jnp.float32)
        + jnp.dot(flat_hi, spread_lo[...], preferred_element_type=jnp.float32)
    )
    out_ref[...] = head + interact

    for step in range(1, chips):
        send_w(step).wait_send()
        send_x(step).wait_send()
    swap.wait_send()
    for step in range(1, towers):
        send_o(step).wait_send()


def on_device(ids, tables, order, w_first, w_second, w_head, w_interact):
    towers = lax.axis_size("tower")
    chips = lax.axis_size("dev") // CORES
    samples, bag = ids.shape[2:]
    active, emb = tables.shape[2:]
    hidden = w_first.shape[2]
    zwidth = w_second.shape[2]
    heads = w_head.shape[1]
    rows = samples // chips
    share = rows // CORES // towers
    pairs = w_interact.shape[0]
    vmem = pltpu.VMEM
    dma = pltpu.SemaphoreType.DMA
    anywhere = pl.BlockSpec(memory_space=pl.ANY)
    scores = pl.pallas_call(
        functools.partial(kernel, towers=towers, chips=chips),
        out_shape=jax.ShapeDtypeStruct((share, heads), jnp.float32),
        in_specs=[
            anywhere,
            anywhere,
            pl.BlockSpec(memory_space=pltpu.SMEM),
            anywhere,
            anywhere,
            anywhere,
            anywhere,
        ],
        out_specs=pl.BlockSpec(memory_space=vmem),
        scratch_shapes=[
            vmem((bag, samples), jnp.int32),
            vmem((active, emb), jnp.bfloat16),
            vmem((samples, emb), jnp.float32),
            vmem((rows, emb), jnp.float32),
            vmem((chips, rows, emb), jnp.bfloat16),
            vmem((chips, emb, hidden), jnp.bfloat16),
            vmem((chips, rows, emb), jnp.bfloat16),
            vmem((CORES, rows // CORES, hidden), jnp.float32),
            vmem((rows // CORES, hidden), jnp.float32),
            vmem((hidden, zwidth), jnp.bfloat16),
            vmem((towers, share, zwidth), jnp.bfloat16),
            vmem((towers, share, zwidth), jnp.bfloat16),
            vmem((towers, zwidth, heads), jnp.bfloat16),
            vmem((pairs, heads), jnp.float32),
            vmem((pairs * share, heads), jnp.bfloat16),
            vmem((pairs * share, heads), jnp.bfloat16),
            dma((6,)),
            dma((chips,)),
            dma((chips,)),
            dma((chips,)),
            dma((chips,)),
            dma,
            dma,
            dma((towers,)),
            dma((towers,)),
        ],
        compiler_params=pltpu.CompilerParams(
            collective_id=0, has_side_effects=True, vmem_limit_bytes=48 * 1024 * 1024
        ),
    )(
        jnp.swapaxes(ids[0, 0], 0, 1),
        tables[0, 0],
        order,
        w_first[0],
        w_second[0],
        w_head.reshape(towers, zwidth, heads),
        w_interact,
    )
    return scores[None]


def solution(mesh):
    return jax.shard_map(
        on_device,
        mesh=mesh,
        in_specs=(
            P("tower", "dev", None, None),
            P("tower", "dev", None, None),
            P(),
            P("tower", "dev", None),
            P("tower", None, None),
            P(),
            P(),
        ),
        out_specs=P("dev", "tower", None),
        check_vma=False,
    )
```

```python
import functools
import math

import jax
import jax.numpy as jnp
from jax import lax
from jax.experimental import pallas as pl
from jax.experimental.pallas import tpu as pltpu
from jax.sharding import PartitionSpec as P

MESH = pl.DeviceIdType.MESH
RING = 4
CORES = 2
CHUNKS = 4


def pool(ids_ref, table_ref, pooled_ref):
    bag, samples = ids_ref.shape
    active = table_ref.shape[0]
    lanes = 128
    fields = active // lanes
    places = lax.broadcasted_iota(jnp.int32, (lanes, lanes), 0)

    def chunk(index, carry):
        start = pl.multiple_of(index * lanes, lanes)
        packed = jnp.zeros((lanes, lanes), jnp.int32)
        for j in range(bag):
            row = ids_ref[pl.ds(j, 1), pl.ds(start, lanes)]
            low = row & (lanes - 1)
            unit = jnp.left_shift(1, (row >> 7) << 3)
            packed = packed + jnp.where(low == places, unit, 0)
        turned = packed.T
        counts = jnp.concatenate(
            [
                ((turned >> (8 * field)) & 255).astype(jnp.float32).astype(jnp.bfloat16)
                for field in range(fields)
            ],
            axis=1,
        )
        pooled_ref[pl.ds(start, lanes), :] = jnp.dot(
            counts, table_ref[...], preferred_element_type=jnp.float32
        )
        return carry

    lax.fori_loop(0, samples // lanes, chunk, 0)


def kernel(
    ids_hbm,
    table_hbm,
    order_ref,
    first_hbm,
    second_hbm,
    head_hbm,
    inter_hbm,
    out_ref,
    ids_v,
    table_v,
    pooled,
    permuted,
    xsend,
    xall,
    wall,
    total,
    cross,
    relay,
    final,
    outsum,
    second_v,
    outbox,
    inbox,
    head_v,
    inter_v,
    spread_hi,
    spread_lo,
    load_sem,
    first_sem,
    w_send,
    w_recv,
    x_send,
    x_recv,
    c_send,
    c_recv,
    f_send,
    f_recv,
    o_send,
    o_recv,
    towers,
):
    tower = lax.axis_index("tower")
    dev = lax.axis_index("dev")
    core = lax.rem(dev, CORES)
    chip = dev // CORES
    col = chip // RING
    row = lax.rem(chip, RING)
    chunks, _, tile = wall.shape
    emb = table_v.shape[1]
    block = permuted.shape[0]

    def along(step):
        return lax.rem(row + step, RING)

    def at_row(place):
        return {"dev": (col * RING + place) * CORES + core}

    partner = {"dev": dev + 1 - 2 * core}
    across = {"dev": ((1 - col) * RING + row) * CORES + core}

    mine = pl.ds(pl.multiple_of(row * emb, emb), emb)
    loads = [
        pltpu.make_async_copy(ids_hbm, ids_v, load_sem.at[0]),
        pltpu.make_async_copy(table_hbm, table_v, load_sem.at[1]),
        pltpu.make_async_copy(second_hbm, second_v, load_sem.at[2]),
        pltpu.make_async_copy(head_hbm, head_v, load_sem.at[3]),
        pltpu.make_async_copy(inter_hbm, inter_v, load_sem.at[4]),
    ]
    firsts = [
        pltpu.make_async_copy(
            first_hbm.at[:, pl.ds(n * tile, tile)], wall.at[n, mine, :], first_sem.at[n]
        )
        for n in range(chunks)
    ]
    loads[0].start()
    loads[1].start()
    for copy in firsts:
        copy.start()
    for copy in loads[2:]:
        copy.start()

    barrier = pltpu.get_barrier_semaphore()
    for step in range(1, towers):
        pl.semaphore_signal(
            barrier, inc=1, device_id={"tower": lax.rem(tower + step, towers)}, device_id_type=MESH
        )
    for step in range(1, RING):
        pl.semaphore_signal(barrier, inc=1, device_id=at_row(along(step)), device_id_type=MESH)
    pl.semaphore_signal(barrier, inc=1, device_id=partner, device_id_type=MESH)
    pl.semaphore_signal(barrier, inc=1, device_id=across, device_id_type=MESH)

    loads[0].wait()
    loads[1].wait()
    pool(ids_v, table_v, pooled)
    for copy in firsts:
        copy.wait()
    pl.semaphore_wait(barrier, towers - 1 + RING - 1 + 2)

    steps = (1, 3, 2)

    def send_w(n, step):
        return pltpu.make_async_remote_copy(
            src_ref=wall.at[n, mine, :],
            dst_ref=wall.at[n, mine, :],
            send_sem=w_send.at[n, step],
            recv_sem=w_recv.at[n, row],
            device_id=at_row(along(step)),
            device_id_type=MESH,
        )

    def send_x(step):
        return pltpu.make_async_remote_copy(
            src_ref=xsend.at[along(step)],
            dst_ref=xall.at[:, mine],
            send_sem=x_send.at[step],
            recv_sem=x_recv.at[row],
            device_id=at_row(along(step)),
            device_id_type=MESH,
        )

    def permute_rows(place, store):
        for c in range(CORES):
            for x in range(2):
                start = ((x * RING + place) * CORES + c) * block

                def group(index, carry):
                    for q in range(16):
                        source = order_ref[start + index * 16 + q]
                        permuted[pl.ds(index * 16 + q, 1), :] = pooled[pl.ds(source, 1), :]
                    return carry

                lax.fori_loop(0, block // 16, group, 0)
                store(c * 2 + x, permuted[...].astype(jnp.bfloat16))

    for step in steps:
        send_w(0, step).start()
    for step in steps:
        place = along(step)

        def keep(part, value):
            xsend[place, part * block : (part + 1) * block, :] = value

        permute_rows(place, keep)
        send_x(step).start()
    for n in range(1, chunks):
        for step in steps:
            send_w(n, step).start()

    def keep_own(part, value):
        xall[part * block : (part + 1) * block, mine] = value

    permute_rows(row, keep_own)

    loads[4].wait()
    pairs = inter_v.shape[0]

    def widen(index, carry):
        start = pl.multiple_of(index * 16, 16)
        some = inter_v[pl.ds(start, 16), :]
        wide = jnp.broadcast_to(some[:, None, :], (16, 8, some.shape[1])).reshape(
            128, some.shape[1]
        )
        high = wide.astype(jnp.bfloat16)
        low = (wide - high.astype(jnp.float32)).astype(jnp.bfloat16)
        target = pl.multiple_of(index * 128, 128)
        spread_hi[pl.ds(target, 128), :] = high
        spread_lo[pl.ds(target, 128), :] = low
        return carry

    lax.fori_loop(0, pairs // 16, widen, 0)
    loads[2].wait()
    loads[3].wait()

    def arrived_w(n, step):
        source = along(step)
        span = pl.ds(pl.multiple_of(source * emb, emb), emb)
        return pltpu.make_async_remote_copy(
            src_ref=wall.at[n, span, :],
            dst_ref=wall.at[n, span, :],
            send_sem=w_send.at[n, step],
            recv_sem=w_recv.at[n, source],
            device_id=partner,
            device_id_type=MESH,
        )

    def arrived_x(step):
        source = along(step)
        span = pl.ds(pl.multiple_of(source * emb, emb), emb)
        return pltpu.make_async_remote_copy(
            src_ref=xsend.at[source],
            dst_ref=xall.at[:, span],
            send_sem=x_send.at[step],
            recv_sem=x_recv.at[source],
            device_id=partner,
            device_id_type=MESH,
        )

    def cross_copy(n):
        return pltpu.make_async_remote_copy(
            src_ref=total.at[n, 1 - core],
            dst_ref=cross.at[n],
            send_sem=c_send.at[n],
            recv_sem=c_recv.at[n],
            device_id=partner,
            device_id_type=MESH,
        )

    def final_copy(n):
        return pltpu.make_async_remote_copy(
            src_ref=relay.at[n],
            dst_ref=final.at[n],
            send_sem=f_send.at[n],
            recv_sem=f_recv.at[n],
            device_id=across,
            device_id_type=MESH,
        )

    def first_layer(n):
        if n == 0:
            for step in steps:
                arrived_x(step).wait_recv()
        for step in steps:
            arrived_w(n, step).wait_recv()
        part = jnp.dot(xall[...], wall[n], preferred_element_type=jnp.float32)
        total[n] = part.reshape(CORES, 2, block, tile)
        cross_copy(n).start()

    def add_cores(n):
        cross_copy(n).wait_recv()
        relay[n] = total[n, core, 1 - col] + cross[n, 1 - col]
        final_copy(n).start()

    def second_layer(n):
        final_copy(n).wait_recv()
        preact = total[n, core, col] + cross[n, col] + final[n]
        hidden = jnp.maximum(preact, 0.0).astype(jnp.bfloat16)
        part = jnp.dot(
            hidden, second_v[n * tile : (n + 1) * tile, :], preferred_element_type=jnp.float32
        )
        if n == 0:
            outsum[...] = part
        else:
            outsum[...] += part

    for n in range(chunks + 2):
        if n < chunks:
            first_layer(n)
        if 1 <= n <= chunks:
            add_cores(n - 1)
        if n >= 2:
            second_layer(n - 2)

    share = outbox.shape[1]
    outbox[...] = outsum[...].reshape(towers, share, outsum.shape[1]).astype(jnp.bfloat16)

    def send_o(step):
        peer = lax.rem(tower + step, towers)
        return pltpu.make_async_remote_copy(
            src_ref=outbox.at[peer],
            dst_ref=inbox.at[tower],
            send_sem=o_send.at[step],
            recv_sem=o_recv.at[tower],
            device_id={"tower": peer},
            device_id_type=MESH,
        )

    for step in range(1, towers):
        send_o(step).start()
    inbox[tower] = outbox[tower]

    def head_part(source):
        return jnp.dot(inbox[source], head_v[source], preferred_element_type=jnp.float32)

    def collect(step, value):
        source = lax.rem(tower + towers - step, towers)
        pltpu.make_async_remote_copy(
            src_ref=outbox.at[source],
            dst_ref=inbox.at[source],
            send_sem=o_send.at[step],
            recv_sem=o_recv.at[source],
            device_id=partner,
            device_id_type=MESH,
        ).wait_recv()
        return value + head_part(source)

    head = lax.fori_loop(1, towers, collect, head_part(tower))

    zwidth = inbox.shape[2]
    stacked = (
        inbox[...].astype(jnp.float32).reshape(towers * share, zwidth).astype(jnp.bfloat16)
    )
    gram = lax.dot_general(
        stacked, stacked, (((1,), (1,)), ((), ())), preferred_element_type=jnp.float32
    )
    left = lax.rem(lax.broadcasted_iota(jnp.int32, gram.shape, 0), share)
    right = lax.rem(lax.broadcasted_iota(jnp.int32, gram.shape, 1), share)
    gram = jnp.where(left == right, gram / math.sqrt(zwidth), 0.0)
    flat = jnp.concatenate(
        [gram[t * share : (t + 1) * share, :] for t in range(towers)], axis=1
    )
    flat_hi = flat.astype(jnp.bfloat16)
    flat_lo = (flat - flat_hi.astype(jnp.float32)).astype(jnp.bfloat16)
    interact = (
        jnp.dot(flat_hi, spread_hi[...], preferred_element_type=jnp.float32)
        + jnp.dot(flat_lo, spread_hi[...], preferred_element_type=jnp.float32)
        + jnp.dot(flat_hi, spread_lo[...], preferred_element_type=jnp.float32)
    )
    out_ref[...] = head + interact

    for step in steps:
        send_x(step).wait_send()
        for n in range(chunks):
            send_w(n, step).wait_send()
    for n in range(chunks):
        cross_copy(n).wait_send()
        final_copy(n).wait_send()
    for step in range(1, towers):
        send_o(step).wait_send()


def on_device(ids, tables, order, w_first, w_second, w_head, w_interact):
    towers = lax.axis_size("tower")
    devices = lax.axis_size("dev")
    samples, bag = ids.shape[2:]
    active, emb = tables.shape[2:]
    hidden = w_first.shape[2]
    zwidth = w_second.shape[2]
    heads = w_head.shape[1]
    block = samples // devices
    share = block // towers
    quarter = samples // RING
    pairs = w_interact.shape[0]
    tile = hidden // CHUNKS
    vmem = pltpu.VMEM
    dma = pltpu.SemaphoreType.DMA
    anywhere = pl.BlockSpec(memory_space=pl.ANY)
    scores = pl.pallas_call(
        functools.partial(kernel, towers=towers),
        out_shape=jax.ShapeDtypeStruct((share, heads), jnp.float32),
        in_specs=[
            anywhere,
            anywhere,
            pl.BlockSpec(memory_space=pltpu.SMEM),
            anywhere,
            anywhere,
            anywhere,
            anywhere,
        ],
        out_specs=pl.BlockSpec(memory_space=vmem),
        scratch_shapes=[
            vmem((bag, samples), jnp.int32),
            vmem((active, emb), jnp.bfloat16),
            vmem((samples, emb), jnp.float32),
            vmem((block, emb), jnp.float32),
            vmem((RING, quarter, emb), jnp.bfloat16),
            vmem((quarter, RING * emb), jnp.bfloat16),
            vmem((CHUNKS, RING * emb, tile), jnp.bfloat16),
            vmem((CHUNKS, CORES, 2, block, tile), jnp.float32),
            vmem((CHUNKS, 2, block, tile), jnp.float32),
            vmem((CHUNKS, block, tile), jnp.float32),
            vmem((CHUNKS, block, tile), jnp.float32),
            vmem((block, zwidth), jnp.float32),
            vmem((hidden, zwidth), jnp.bfloat16),
            vmem((towers, share, zwidth), jnp.bfloat16),
            vmem((towers, share, zwidth), jnp.bfloat16),
            vmem((towers, zwidth, heads), jnp.bfloat16),
            vmem((pairs, heads), jnp.float32),
            vmem((pairs * share, heads), jnp.bfloat16),
            vmem((pairs * share, heads), jnp.bfloat16),
            dma((5,)),
            dma((CHUNKS,)),
            dma((CHUNKS, RING)),
            dma((CHUNKS, RING)),
            dma((RING,)),
            dma((RING,)),
            dma((CHUNKS,)),
            dma((CHUNKS,)),
            dma((CHUNKS,)),
            dma((CHUNKS,)),
            dma((towers,)),
            dma((towers,)),
        ],
        compiler_params=pltpu.CompilerParams(
            collective_id=0, has_side_effects=True, vmem_limit_bytes=63 * 1024 * 1024
        ),
    )(
        jnp.swapaxes(ids[0, 0], 0, 1),
        tables[0, 0],
        order,
        w_first[0],
        w_second[0],
        w_head.reshape(towers, zwidth, heads),
        w_interact,
    )
    return scores[None]


def solution(mesh):
    return jax.shard_map(
        on_device,
        mesh=mesh,
        in_specs=(
            P("tower", "dev", None, None),
            P("tower", "dev", None, None),
            P(),
            P("tower", "dev", None),
            P("tower", None, None),
            P(),
            P(),
        ),
        out_specs=P("dev", "tower", None),
        check_vma=False,
    )
```

```python
import functools
import math

import jax
import jax.numpy as jnp
from jax import lax
from jax.experimental import pallas as pl
from jax.experimental.pallas import tpu as pltpu
from jax.sharding import PartitionSpec as P

MESH = pl.DeviceIdType.MESH
RING = 4
CORES = 2
CHUNKS = 4
EARLY = 2


def fold(words, shift, mask):
    return words & mask, lax.shift_right_logical(words, shift) & mask


def tally(ids_ref, start, places):
    bag = ids_ref.shape[0]
    lanes = places.shape[1]
    low_bits = places.shape[0]
    shift = low_bits.bit_length() - 1
    rows = [ids_ref[pl.ds(8 * g, 8), pl.ds(start, lanes)] for g in range(bag // 8)]
    lows = [row & (low_bits - 1) for row in rows]
    units = [jnp.left_shift(1, (row >> shift) << 1) for row in rows]

    def mark(j):
        low = lows[j // 8][j % 8 : j % 8 + 1, :]
        unit = units[j // 8][j % 8 : j % 8 + 1, :]
        return jnp.where(low == places, unit, 0)

    def add(left, right):
        return right if left is None else [a + b for a, b in zip(left, right)]

    nibbles = None
    bytes_ = None
    held = 0
    for start_j in range(0, bag, 3):
        group = range(start_j, min(start_j + 3, bag))
        words = mark(group[0])
        for j in group[1:]:
            words = words + mark(j)
        nibbles = add(nibbles, fold(words, 2, 0x33333333))
        held += len(group)
        if held > 12 or group[-1] == bag - 1:
            even = fold(nibbles[0], 4, 0x0F0F0F0F)
            odd = fold(nibbles[1], 4, 0x0F0F0F0F)
            bytes_ = add(bytes_, [even[0], odd[0], even[1], odd[1]])
            nibbles = None
            held = 0
    return jnp.concatenate(bytes_, axis=0)


def pool(ids_ref, table_ref, pooled_ref):
    samples = ids_ref.shape[1]
    active = table_ref.shape[0]
    lanes = 128
    fields = active // lanes
    places = lax.broadcasted_iota(jnp.int32, (lanes // 4, lanes), 0)

    def finish(packed, index):
        turned = packed.T
        counts = jnp.concatenate(
            [
                ((turned >> (8 * field)) & 255).astype(jnp.float32).astype(jnp.bfloat16)
                for field in range(fields)
            ],
            axis=1,
        )
        pooled_ref[pl.ds(pl.multiple_of(index * lanes, lanes), lanes), :] = jnp.dot(
            counts, table_ref[...], preferred_element_type=jnp.float32
        )

    def chunk(index, packed):
        finish(packed, index - 1)
        return tally(ids_ref, pl.multiple_of(index * lanes, lanes), places)

    chunks = samples // lanes
    last = lax.fori_loop(1, chunks, chunk, tally(ids_ref, 0, places))
    finish(last, chunks - 1)


def kernel(
    ids_hbm,
    table_hbm,
    order_ref,
    first_hbm,
    second_hbm,
    head_hbm,
    inter_hbm,
    out_ref,
    ids_v,
    table_v,
    pooled,
    permuted,
    xsend,
    xall,
    wall,
    total,
    cross,
    relay,
    final,
    outsum,
    second_v,
    outbox,
    inbox,
    head_v,
    inter_v,
    spread_hi,
    spread_lo,
    load_sem,
    first_sem,
    w_send,
    w_recv,
    x_send,
    x_recv,
    c_send,
    c_recv,
    f_send,
    f_recv,
    o_send,
    o_recv,
    towers,
):
    tower = lax.axis_index("tower")
    dev = lax.axis_index("dev")
    core = lax.rem(dev, CORES)
    chip = dev // CORES
    col = chip // RING
    row = lax.rem(chip, RING)
    chunks, _, tile = wall.shape
    emb = table_v.shape[1]
    block = permuted.shape[0]

    def along(step):
        return lax.rem(row + step, RING)

    def at_row(place):
        return {"dev": (col * RING + place) * CORES + core}

    partner = {"dev": dev + 1 - 2 * core}
    across = {"dev": ((1 - col) * RING + row) * CORES + core}

    mine = pl.ds(pl.multiple_of(row * emb, emb), emb)
    loads = [
        pltpu.make_async_copy(ids_hbm, ids_v, load_sem.at[0]),
        pltpu.make_async_copy(table_hbm, table_v, load_sem.at[1]),
        pltpu.make_async_copy(second_hbm, second_v, load_sem.at[2]),
        pltpu.make_async_copy(head_hbm, head_v, load_sem.at[3]),
        pltpu.make_async_copy(inter_hbm, inter_v, load_sem.at[4]),
    ]
    firsts = [
        pltpu.make_async_copy(
            first_hbm.at[:, pl.ds(n * tile, tile)], wall.at[n, mine, :], first_sem.at[n]
        )
        for n in range(chunks)
    ]
    loads[0].start()
    loads[1].start()
    for copy in firsts:
        copy.start()
    for copy in loads[2:]:
        copy.start()

    barrier = pltpu.get_barrier_semaphore()
    for step in range(1, towers):
        pl.semaphore_signal(
            barrier, inc=1, device_id={"tower": lax.rem(tower + step, towers)}, device_id_type=MESH
        )
    for step in range(1, RING):
        pl.semaphore_signal(barrier, inc=1, device_id=at_row(along(step)), device_id_type=MESH)
    pl.semaphore_signal(barrier, inc=1, device_id=partner, device_id_type=MESH)
    pl.semaphore_signal(barrier, inc=1, device_id=across, device_id_type=MESH)

    for copy in firsts:
        copy.wait()
    pl.semaphore_wait(barrier, towers - 1 + RING - 1 + 2)

    steps = (1, 3, 2)

    def send_w(n, step):
        return pltpu.make_async_remote_copy(
            src_ref=wall.at[n, mine, :],
            dst_ref=wall.at[n, mine, :],
            send_sem=w_send.at[n, step],
            recv_sem=w_recv.at[n, row],
            device_id=at_row(along(step)),
            device_id_type=MESH,
        )

    def send_x(step):
        return pltpu.make_async_remote_copy(
            src_ref=xsend.at[along(step)],
            dst_ref=xall.at[:, mine],
            send_sem=x_send.at[step],
            recv_sem=x_recv.at[row],
            device_id=at_row(along(step)),
            device_id_type=MESH,
        )

    def permute_rows(place, store):
        for c in range(CORES):
            for x in range(2):
                start = ((x * RING + place) * CORES + c) * block

                def group(index, carry):
                    for q in range(16):
                        source = order_ref[start + index * 16 + q]
                        permuted[pl.ds(index * 16 + q, 1), :] = pooled[pl.ds(source, 1), :]
                    return carry

                lax.fori_loop(0, block // 16, group, 0)
                store(c * 2 + x, permuted[...].astype(jnp.bfloat16))

    for n in range(EARLY):
        for step in steps:
            send_w(n, step).start()
    loads[0].wait()
    loads[1].wait()
    pool(ids_v, table_v, pooled)
    for step in steps:
        place = along(step)

        def keep(part, value):
            xsend[place, part * block : (part + 1) * block, :] = value

        permute_rows(place, keep)
        send_x(step).start()
    for n in range(EARLY, chunks):
        for step in steps:
            send_w(n, step).start()

    def keep_own(part, value):
        xall[part * block : (part + 1) * block, mine] = value

    permute_rows(row, keep_own)

    loads[4].wait()
    pairs = inter_v.shape[0]

    def widen(index, carry):
        start = pl.multiple_of(index * 16, 16)
        some = inter_v[pl.ds(start, 16), :]
        wide = jnp.broadcast_to(some[:, None, :], (16, 8, some.shape[1])).reshape(
            128, some.shape[1]
        )
        high = wide.astype(jnp.bfloat16)
        low = (wide - high.astype(jnp.float32)).astype(jnp.bfloat16)
        target = pl.multiple_of(index * 128, 128)
        spread_hi[pl.ds(target, 128), :] = high
        spread_lo[pl.ds(target, 128), :] = low
        return carry

    lax.fori_loop(0, pairs // 16, widen, 0)
    loads[2].wait()
    loads[3].wait()

    def arrived_w(n, step):
        source = along(step)
        span = pl.ds(pl.multiple_of(source * emb, emb), emb)
        return pltpu.make_async_remote_copy(
            src_ref=wall.at[n, span, :],
            dst_ref=wall.at[n, span, :],
            send_sem=w_send.at[n, step],
            recv_sem=w_recv.at[n, source],
            device_id=partner,
            device_id_type=MESH,
        )

    def arrived_x(step):
        source = along(step)
        span = pl.ds(pl.multiple_of(source * emb, emb), emb)
        return pltpu.make_async_remote_copy(
            src_ref=xsend.at[source],
            dst_ref=xall.at[:, span],
            send_sem=x_send.at[step],
            recv_sem=x_recv.at[source],
            device_id=partner,
            device_id_type=MESH,
        )

    def cross_copy(n):
        return pltpu.make_async_remote_copy(
            src_ref=total.at[n, 1 - core],
            dst_ref=cross.at[n],
            send_sem=c_send.at[n],
            recv_sem=c_recv.at[n],
            device_id=partner,
            device_id_type=MESH,
        )

    def final_copy(n):
        return pltpu.make_async_remote_copy(
            src_ref=relay.at[n],
            dst_ref=final.at[n],
            send_sem=f_send.at[n],
            recv_sem=f_recv.at[n],
            device_id=across,
            device_id_type=MESH,
        )

    def first_layer(n):
        if n == 0:
            for step in steps:
                arrived_x(step).wait_recv()
        for step in steps:
            arrived_w(n, step).wait_recv()
        part = jnp.dot(xall[...], wall[n], preferred_element_type=jnp.float32)
        total[n] = part.reshape(CORES, 2, block, tile)
        cross_copy(n).start()

    def add_cores(n):
        cross_copy(n).wait_recv()
        relay[n] = total[n, core, 1 - col] + cross[n, 1 - col]
        final_copy(n).start()

    def second_layer(n):
        final_copy(n).wait_recv()
        preact = total[n, core, col] + cross[n, col] + final[n]
        hidden = jnp.maximum(preact, 0.0).astype(jnp.bfloat16)
        part = jnp.dot(
            hidden, second_v[n * tile : (n + 1) * tile, :], preferred_element_type=jnp.float32
        )
        if n == 0:
            outsum[...] = part
        else:
            outsum[...] += part

    for n in range(chunks + 2):
        if n < chunks:
            first_layer(n)
        if 1 <= n <= chunks:
            add_cores(n - 1)
        if n >= 2:
            second_layer(n - 2)

    share = outbox.shape[1]
    outbox[...] = outsum[...].reshape(towers, share, outsum.shape[1]).astype(jnp.bfloat16)

    def send_o(step):
        peer = lax.rem(tower + step, towers)
        return pltpu.make_async_remote_copy(
            src_ref=outbox.at[peer],
            dst_ref=inbox.at[tower],
            send_sem=o_send.at[step],
            recv_sem=o_recv.at[tower],
            device_id={"tower": peer},
            device_id_type=MESH,
        )

    for step in range(1, towers):
        send_o(step).start()
    inbox[tower] = outbox[tower]

    def head_part(source):
        return jnp.dot(inbox[source], head_v[source], preferred_element_type=jnp.float32)

    def collect(step, value):
        source = lax.rem(tower + towers - step, towers)
        pltpu.make_async_remote_copy(
            src_ref=outbox.at[source],
            dst_ref=inbox.at[source],
            send_sem=o_send.at[step],
            recv_sem=o_recv.at[source],
            device_id=partner,
            device_id_type=MESH,
        ).wait_recv()
        return value + head_part(source)

    head = lax.fori_loop(1, towers, collect, head_part(tower))

    zwidth = inbox.shape[2]
    stacked = (
        inbox[...].astype(jnp.float32).reshape(towers * share, zwidth).astype(jnp.bfloat16)
    )
    gram = lax.dot_general(
        stacked, stacked, (((1,), (1,)), ((), ())), preferred_element_type=jnp.float32
    )
    left = lax.rem(lax.broadcasted_iota(jnp.int32, gram.shape, 0), share)
    right = lax.rem(lax.broadcasted_iota(jnp.int32, gram.shape, 1), share)
    gram = jnp.where(left == right, gram / math.sqrt(zwidth), 0.0)
    flat = jnp.concatenate(
        [gram[t * share : (t + 1) * share, :] for t in range(towers)], axis=1
    )
    flat_hi = flat.astype(jnp.bfloat16)
    flat_lo = (flat - flat_hi.astype(jnp.float32)).astype(jnp.bfloat16)
    interact = (
        jnp.dot(flat_hi, spread_hi[...], preferred_element_type=jnp.float32)
        + jnp.dot(flat_lo, spread_hi[...], preferred_element_type=jnp.float32)
        + jnp.dot(flat_hi, spread_lo[...], preferred_element_type=jnp.float32)
    )
    out_ref[...] = head + interact

    for step in steps:
        send_x(step).wait_send()
        for n in range(chunks):
            send_w(n, step).wait_send()
    for n in range(chunks):
        cross_copy(n).wait_send()
        final_copy(n).wait_send()
    for step in range(1, towers):
        send_o(step).wait_send()


def on_device(ids, tables, order, w_first, w_second, w_head, w_interact):
    towers = lax.axis_size("tower")
    devices = lax.axis_size("dev")
    samples, bag = ids.shape[2:]
    active, emb = tables.shape[2:]
    hidden = w_first.shape[2]
    zwidth = w_second.shape[2]
    heads = w_head.shape[1]
    block = samples // devices
    share = block // towers
    quarter = samples // RING
    pairs = w_interact.shape[0]
    tile = hidden // CHUNKS
    vmem = pltpu.VMEM
    dma = pltpu.SemaphoreType.DMA
    anywhere = pl.BlockSpec(memory_space=pltpu.HBM)
    scores = pl.pallas_call(
        functools.partial(kernel, towers=towers),
        out_shape=jax.ShapeDtypeStruct((share, heads), jnp.float32),
        in_specs=[
            anywhere,
            anywhere,
            pl.BlockSpec(memory_space=pltpu.SMEM),
            anywhere,
            anywhere,
            anywhere,
            anywhere,
        ],
        out_specs=pl.BlockSpec(memory_space=vmem),
        scratch_shapes=[
            vmem((bag, samples), jnp.int32),
            vmem((active, emb), jnp.bfloat16),
            vmem((samples, emb), jnp.float32),
            vmem((block, emb), jnp.float32),
            vmem((RING, quarter, emb), jnp.bfloat16),
            vmem((quarter, RING * emb), jnp.bfloat16),
            vmem((CHUNKS, RING * emb, tile), jnp.bfloat16),
            vmem((CHUNKS, CORES, 2, block, tile), jnp.float32),
            vmem((CHUNKS, 2, block, tile), jnp.float32),
            vmem((CHUNKS, block, tile), jnp.float32),
            vmem((CHUNKS, block, tile), jnp.float32),
            vmem((block, zwidth), jnp.float32),
            vmem((hidden, zwidth), jnp.bfloat16),
            vmem((towers, share, zwidth), jnp.bfloat16),
            vmem((towers, share, zwidth), jnp.bfloat16),
            vmem((towers, zwidth, heads), jnp.bfloat16),
            vmem((pairs, heads), jnp.float32),
            vmem((pairs * share, heads), jnp.bfloat16),
            vmem((pairs * share, heads), jnp.bfloat16),
            dma((5,)),
            dma((CHUNKS,)),
            dma((CHUNKS, RING)),
            dma((CHUNKS, RING)),
            dma((RING,)),
            dma((RING,)),
            dma((CHUNKS,)),
            dma((CHUNKS,)),
            dma((CHUNKS,)),
            dma((CHUNKS,)),
            dma((towers,)),
            dma((towers,)),
        ],
        compiler_params=pltpu.CompilerParams(
            collective_id=0, has_side_effects=True, vmem_limit_bytes=32 * 1024 * 1024
        ),
    )(
        *(
            pltpu.with_memory_space_constraint(value, pltpu.HBM)
            for value in (
                jnp.swapaxes(ids[0, 0], 0, 1),
                tables[0, 0],
                order,
                w_first[0],
                w_second[0],
                w_head.reshape(towers, zwidth, heads),
                w_interact,
            )
        ),
    )
    return scores[None]


def solution(mesh):
    return jax.shard_map(
        on_device,
        mesh=mesh,
        in_specs=(
            P("tower", "dev", None, None),
            P("tower", "dev", None, None),
            P(),
            P("tower", "dev", None),
            P("tower", None, None),
            P(),
            P(),
        ),
        out_specs=P("dev", "tower", None),
        check_vma=False,
    )
```

```python
import functools
import math

import jax
import jax.numpy as jnp
from jax import lax
from jax.experimental import pallas as pl
from jax.experimental.pallas import tpu as pltpu
from jax.sharding import PartitionSpec as P

MESH = pl.DeviceIdType.MESH
RING = 4
CORES = 2
CHUNKS = 4
EARLY = 2
LEVELS = 32767


def fold(words, shift, mask):
    return words & mask, lax.shift_right_logical(words, shift) & mask


def tally(ids_ref, start, places):
    bag = ids_ref.shape[0]
    lanes = places.shape[1]
    low_bits = places.shape[0]
    shift = low_bits.bit_length() - 1
    rows = [ids_ref[pl.ds(8 * g, 8), pl.ds(start, lanes)] for g in range(bag // 8)]
    lows = [row & (low_bits - 1) for row in rows]
    units = [jnp.left_shift(1, (row >> shift) << 1) for row in rows]

    def mark(j):
        low = lows[j // 8][j % 8 : j % 8 + 1, :]
        unit = units[j // 8][j % 8 : j % 8 + 1, :]
        return jnp.where(low == places, unit, 0)

    def add(left, right):
        return right if left is None else [a + b for a, b in zip(left, right)]

    nibbles = None
    bytes_ = None
    held = 0
    for start_j in range(0, bag, 3):
        group = range(start_j, min(start_j + 3, bag))
        words = mark(group[0])
        for j in group[1:]:
            words = words + mark(j)
        nibbles = add(nibbles, fold(words, 2, 0x33333333))
        held += len(group)
        if held > 12 or group[-1] == bag - 1:
            even = fold(nibbles[0], 4, 0x0F0F0F0F)
            odd = fold(nibbles[1], 4, 0x0F0F0F0F)
            bytes_ = add(bytes_, [even[0], odd[0], even[1], odd[1]])
            nibbles = None
            held = 0
    return jnp.concatenate(bytes_, axis=0)


def pool(ids_ref, table_ref, pooled_ref):
    samples = ids_ref.shape[1]
    active = table_ref.shape[0]
    lanes = 128
    fields = active // lanes
    places = lax.broadcasted_iota(jnp.int32, (lanes // 4, lanes), 0)

    def finish(packed, index):
        turned = packed.T
        counts = jnp.concatenate(
            [
                ((turned >> (8 * field)) & 255).astype(jnp.float32).astype(jnp.bfloat16)
                for field in range(fields)
            ],
            axis=1,
        )
        pooled_ref[pl.ds(pl.multiple_of(index * lanes, lanes), lanes), :] = jnp.dot(
            counts, table_ref[...], preferred_element_type=jnp.float32
        )

    def chunk(index, packed):
        finish(packed, index - 1)
        return tally(ids_ref, pl.multiple_of(index * lanes, lanes), places)

    chunks = samples // lanes
    last = lax.fori_loop(1, chunks, chunk, tally(ids_ref, 0, places))
    finish(last, chunks - 1)


def kernel(
    ids_hbm,
    table_hbm,
    order_ref,
    first_hbm,
    second_hbm,
    head_hbm,
    inter_hbm,
    out_ref,
    ids_v,
    table_v,
    pooled,
    permuted,
    xsend,
    xall,
    wall,
    total,
    cross,
    relay,
    final,
    relay_top,
    final_top,
    outsum,
    second_v,
    outbox,
    inbox,
    head_v,
    inter_v,
    spread_hi,
    spread_lo,
    load_sem,
    first_sem,
    w_send,
    w_recv,
    x_send,
    x_recv,
    c_send,
    c_recv,
    f_send,
    f_recv,
    o_send,
    o_recv,
    towers,
):
    tower = lax.axis_index("tower")
    dev = lax.axis_index("dev")
    core = lax.rem(dev, CORES)
    chip = dev // CORES
    col = chip // RING
    row = lax.rem(chip, RING)
    chunks, _, tile = wall.shape
    emb = table_v.shape[1]
    block = permuted.shape[0]

    def along(step):
        return lax.rem(row + step, RING)

    def at_row(place):
        return {"dev": (col * RING + place) * CORES + core}

    partner = {"dev": dev + 1 - 2 * core}
    across = {"dev": ((1 - col) * RING + row) * CORES + core}

    mine = pl.ds(pl.multiple_of(row * emb, emb), emb)
    loads = [
        pltpu.make_async_copy(ids_hbm, ids_v, load_sem.at[0]),
        pltpu.make_async_copy(table_hbm, table_v, load_sem.at[1]),
        pltpu.make_async_copy(second_hbm, second_v, load_sem.at[2]),
        pltpu.make_async_copy(head_hbm, head_v, load_sem.at[3]),
        pltpu.make_async_copy(inter_hbm, inter_v, load_sem.at[4]),
    ]
    firsts = [
        pltpu.make_async_copy(
            first_hbm.at[:, pl.ds(n * tile, tile)], wall.at[n, mine, :], first_sem.at[n]
        )
        for n in range(chunks)
    ]
    loads[0].start()
    loads[1].start()
    for copy in firsts:
        copy.start()
    for copy in loads[2:]:
        copy.start()

    barrier = pltpu.get_barrier_semaphore()
    for step in range(1, towers):
        pl.semaphore_signal(
            barrier, inc=1, device_id={"tower": lax.rem(tower + step, towers)}, device_id_type=MESH
        )
    for step in range(1, RING):
        pl.semaphore_signal(barrier, inc=1, device_id=at_row(along(step)), device_id_type=MESH)
    pl.semaphore_signal(barrier, inc=1, device_id=partner, device_id_type=MESH)
    pl.semaphore_signal(barrier, inc=1, device_id=across, device_id_type=MESH)

    for copy in firsts:
        copy.wait()
    pl.semaphore_wait(barrier, towers - 1 + RING - 1 + 2)

    steps = (1, 3, 2)

    def send_w(n, step):
        return pltpu.make_async_remote_copy(
            src_ref=wall.at[n, mine, :],
            dst_ref=wall.at[n, mine, :],
            send_sem=w_send.at[n, step],
            recv_sem=w_recv.at[n, row],
            device_id=at_row(along(step)),
            device_id_type=MESH,
        )

    def send_x(step):
        return pltpu.make_async_remote_copy(
            src_ref=xsend.at[along(step)],
            dst_ref=xall.at[:, mine],
            send_sem=x_send.at[step],
            recv_sem=x_recv.at[row],
            device_id=at_row(along(step)),
            device_id_type=MESH,
        )

    def permute_rows(place, store):
        for c in range(CORES):
            for x in range(2):
                start = ((x * RING + place) * CORES + c) * block

                def group(index, carry):
                    for q in range(16):
                        source = order_ref[start + index * 16 + q]
                        permuted[pl.ds(index * 16 + q, 1), :] = pooled[pl.ds(source, 1), :]
                    return carry

                lax.fori_loop(0, block // 16, group, 0)
                store(c * 2 + x, permuted[...].astype(jnp.bfloat16))

    for n in range(EARLY):
        for step in steps:
            send_w(n, step).start()
    loads[0].wait()
    loads[1].wait()
    pool(ids_v, table_v, pooled)
    for step in steps:
        place = along(step)

        def keep(part, value):
            xsend[place, part * block : (part + 1) * block, :] = value

        permute_rows(place, keep)
        send_x(step).start()
    for n in range(EARLY, chunks):
        for step in steps:
            send_w(n, step).start()

    def keep_own(part, value):
        xall[part * block : (part + 1) * block, mine] = value

    permute_rows(row, keep_own)

    loads[4].wait()
    pairs = inter_v.shape[0]

    def widen(index, carry):
        start = pl.multiple_of(index * 16, 16)
        some = inter_v[pl.ds(start, 16), :]
        wide = jnp.broadcast_to(some[:, None, :], (16, 8, some.shape[1])).reshape(
            128, some.shape[1]
        )
        high = wide.astype(jnp.bfloat16)
        low = (wide - high.astype(jnp.float32)).astype(jnp.bfloat16)
        target = pl.multiple_of(index * 128, 128)
        spread_hi[pl.ds(target, 128), :] = high
        spread_lo[pl.ds(target, 128), :] = low
        return carry

    lax.fori_loop(0, pairs // 16, widen, 0)
    loads[2].wait()
    loads[3].wait()

    def arrived_w(n, step):
        source = along(step)
        span = pl.ds(pl.multiple_of(source * emb, emb), emb)
        return pltpu.make_async_remote_copy(
            src_ref=wall.at[n, span, :],
            dst_ref=wall.at[n, span, :],
            send_sem=w_send.at[n, step],
            recv_sem=w_recv.at[n, source],
            device_id=partner,
            device_id_type=MESH,
        )

    def arrived_x(step):
        source = along(step)
        span = pl.ds(pl.multiple_of(source * emb, emb), emb)
        return pltpu.make_async_remote_copy(
            src_ref=xsend.at[source],
            dst_ref=xall.at[:, span],
            send_sem=x_send.at[step],
            recv_sem=x_recv.at[source],
            device_id=partner,
            device_id_type=MESH,
        )

    def cross_copy(n):
        return pltpu.make_async_remote_copy(
            src_ref=total.at[n, 1 - core],
            dst_ref=cross.at[n],
            send_sem=c_send.at[n],
            recv_sem=c_recv.at[n],
            device_id=partner,
            device_id_type=MESH,
        )

    def final_copies(n):
        return [
            pltpu.make_async_remote_copy(
                src_ref=source.at[n],
                dst_ref=target.at[n],
                send_sem=f_send.at[n, which],
                recv_sem=f_recv.at[n, which],
                device_id=across,
                device_id_type=MESH,
            )
            for which, (source, target) in enumerate(((relay_top, final_top), (relay, final)))
        ]

    def first_layer(n):
        if n == 0:
            for step in steps:
                arrived_x(step).wait_recv()
        for step in steps:
            arrived_w(n, step).wait_recv()
        part = jnp.dot(xall[...], wall[n], preferred_element_type=jnp.float32)
        total[n] = part.reshape(CORES, 2, block, tile)
        cross_copy(n).start()

    def add_cores(n):
        cross_copy(n).wait_recv()
        part = total[n, core, 1 - col] + cross[n, 1 - col]
        top = jnp.max(jnp.abs(part), axis=0, keepdims=True)
        steps_up = part * (LEVELS / jnp.maximum(top, 1e-30)) + (LEVELS + 1.5)
        relay[n] = (steps_up.astype(jnp.int32) - (LEVELS + 1)).astype(jnp.int16)
        relay_top[n] = jnp.broadcast_to(top, relay_top.shape[1:])
        for copy in final_copies(n):
            copy.start()

    def second_layer(n):
        for copy in final_copies(n):
            copy.wait_recv()
        other = final[n].astype(jnp.float32) * (final_top[n, 0:1, :] * (1.0 / LEVELS))
        preact = total[n, core, col] + cross[n, col] + other
        hidden = jnp.maximum(preact, 0.0).astype(jnp.bfloat16)
        part = jnp.dot(
            hidden, second_v[n * tile : (n + 1) * tile, :], preferred_element_type=jnp.float32
        )
        if n == 0:
            outsum[...] = part
        else:
            outsum[...] += part

    for n in range(chunks + 2):
        if n < chunks:
            first_layer(n)
        if 1 <= n <= chunks:
            add_cores(n - 1)
        if n >= 2:
            second_layer(n - 2)

    share = outbox.shape[1]
    outbox[...] = outsum[...].reshape(towers, share, outsum.shape[1]).astype(jnp.bfloat16)

    def send_o(step):
        peer = lax.rem(tower + step, towers)
        return pltpu.make_async_remote_copy(
            src_ref=outbox.at[peer],
            dst_ref=inbox.at[tower],
            send_sem=o_send.at[step],
            recv_sem=o_recv.at[tower],
            device_id={"tower": peer},
            device_id_type=MESH,
        )

    for step in range(1, towers):
        send_o(step).start()
    inbox[tower] = outbox[tower]

    def head_part(source):
        return jnp.dot(inbox[source], head_v[source], preferred_element_type=jnp.float32)

    def collect(step, value):
        source = lax.rem(tower + towers - step, towers)
        pltpu.make_async_remote_copy(
            src_ref=outbox.at[source],
            dst_ref=inbox.at[source],
            send_sem=o_send.at[step],
            recv_sem=o_recv.at[source],
            device_id=partner,
            device_id_type=MESH,
        ).wait_recv()
        return value + head_part(source)

    head = lax.fori_loop(1, towers, collect, head_part(tower))

    zwidth = inbox.shape[2]
    stacked = (
        inbox[...].astype(jnp.float32).reshape(towers * share, zwidth).astype(jnp.bfloat16)
    )
    gram = lax.dot_general(
        stacked, stacked, (((1,), (1,)), ((), ())), preferred_element_type=jnp.float32
    )
    left = lax.rem(lax.broadcasted_iota(jnp.int32, gram.shape, 0), share)
    right = lax.rem(lax.broadcasted_iota(jnp.int32, gram.shape, 1), share)
    gram = jnp.where(left == right, gram / math.sqrt(zwidth), 0.0)
    flat = jnp.concatenate(
        [gram[t * share : (t + 1) * share, :] for t in range(towers)], axis=1
    )
    flat_hi = flat.astype(jnp.bfloat16)
    flat_lo = (flat - flat_hi.astype(jnp.float32)).astype(jnp.bfloat16)
    interact = (
        jnp.dot(flat_hi, spread_hi[...], preferred_element_type=jnp.float32)
        + jnp.dot(flat_lo, spread_hi[...], preferred_element_type=jnp.float32)
        + jnp.dot(flat_hi, spread_lo[...], preferred_element_type=jnp.float32)
    )
    out_ref[...] = head + interact

    for step in steps:
        send_x(step).wait_send()
        for n in range(chunks):
            send_w(n, step).wait_send()
    for n in range(chunks):
        cross_copy(n).wait_send()
        for copy in final_copies(n):
            copy.wait_send()
    for step in range(1, towers):
        send_o(step).wait_send()


def on_device(ids, tables, order, w_first, w_second, w_head, w_interact):
    towers = lax.axis_size("tower")
    devices = lax.axis_size("dev")
    samples, bag = ids.shape[2:]
    active, emb = tables.shape[2:]
    hidden = w_first.shape[2]
    zwidth = w_second.shape[2]
    heads = w_head.shape[1]
    block = samples // devices
    share = block // towers
    quarter = samples // RING
    pairs = w_interact.shape[0]
    tile = hidden // CHUNKS
    vmem = pltpu.VMEM
    dma = pltpu.SemaphoreType.DMA
    anywhere = pl.BlockSpec(memory_space=pltpu.HBM)
    scores = pl.pallas_call(
        functools.partial(kernel, towers=towers),
        out_shape=jax.ShapeDtypeStruct((share, heads), jnp.float32),
        in_specs=[
            anywhere,
            anywhere,
            pl.BlockSpec(memory_space=pltpu.SMEM),
            anywhere,
            anywhere,
            anywhere,
            anywhere,
        ],
        out_specs=pl.BlockSpec(memory_space=vmem),
        scratch_shapes=[
            vmem((bag, samples), jnp.int32),
            vmem((active, emb), jnp.bfloat16),
            vmem((samples, emb), jnp.float32),
            vmem((block, emb), jnp.float32),
            vmem((RING, quarter, emb), jnp.bfloat16),
            vmem((quarter, RING * emb), jnp.bfloat16),
            vmem((CHUNKS, RING * emb, tile), jnp.bfloat16),
            vmem((CHUNKS, CORES, 2, block, tile), jnp.float32),
            vmem((CHUNKS, 2, block, tile), jnp.float32),
            vmem((CHUNKS, block, tile), jnp.int16),
            vmem((CHUNKS, block, tile), jnp.int16),
            vmem((CHUNKS, 8, tile), jnp.float32),
            vmem((CHUNKS, 8, tile), jnp.float32),
            vmem((block, zwidth), jnp.float32),
            vmem((hidden, zwidth), jnp.bfloat16),
            vmem((towers, share, zwidth), jnp.bfloat16),
            vmem((towers, share, zwidth), jnp.bfloat16),
            vmem((towers, zwidth, heads), jnp.bfloat16),
            vmem((pairs, heads), jnp.float32),
            vmem((pairs * share, heads), jnp.bfloat16),
            vmem((pairs * share, heads), jnp.bfloat16),
            dma((5,)),
            dma((CHUNKS,)),
            dma((CHUNKS, RING)),
            dma((CHUNKS, RING)),
            dma((RING,)),
            dma((RING,)),
            dma((CHUNKS,)),
            dma((CHUNKS,)),
            dma((CHUNKS, 2)),
            dma((CHUNKS, 2)),
            dma((towers,)),
            dma((towers,)),
        ],
        compiler_params=pltpu.CompilerParams(
            collective_id=0, has_side_effects=True, vmem_limit_bytes=32 * 1024 * 1024
        ),
    )(
        *(
            pltpu.with_memory_space_constraint(value, pltpu.HBM)
            for value in (
                jnp.swapaxes(ids[0, 0], 0, 1),
                tables[0, 0],
                order,
                w_first[0],
                w_second[0],
                w_head.reshape(towers, zwidth, heads),
                w_interact,
            )
        ),
    )
    return scores[None]


def solution(mesh):
    return jax.shard_map(
        on_device,
        mesh=mesh,
        in_specs=(
            P("tower", "dev", None, None),
            P("tower", "dev", None, None),
            P(),
            P("tower", "dev", None),
            P("tower", None, None),
            P(),
            P(),
        ),
        out_specs=P("dev", "tower", None),
        check_vma=False,
    )
```

```python
import functools
import math

import jax
import jax.numpy as jnp
from jax import lax
from jax.experimental import pallas as pl
from jax.experimental.pallas import tpu as pltpu
from jax.sharding import PartitionSpec as P

MESH = pl.DeviceIdType.MESH
RING = 4
CORES = 2
CHUNKS = 4
SPANS = ((0, 2), (2, 1), (3, 1))
EARLY = 1
LEVELS = 32767
HOPS = (
    (1, 0),
    (7, 0),
    (2, 0),
    (6, 0),
    (0, 1),
    (1, 1),
    (7, 1),
    (3, 0),
    (5, 0),
    (2, 1),
    (6, 1),
    (4, 0),
    (3, 1),
    (5, 1),
    (4, 1),
)


def fold(words, shift, mask):
    return words & mask, lax.shift_right_logical(words, shift) & mask


def tally(ids_ref, start, places):
    bag = ids_ref.shape[0]
    lanes = places.shape[1]
    low_bits = places.shape[0]
    shift = low_bits.bit_length() - 1
    rows = [ids_ref[pl.ds(8 * g, 8), pl.ds(start, lanes)] for g in range(bag // 8)]
    lows = [row & (low_bits - 1) for row in rows]
    units = [jnp.left_shift(1, (row >> shift) << 1) for row in rows]

    def mark(j):
        low = lows[j // 8][j % 8 : j % 8 + 1, :]
        unit = units[j // 8][j % 8 : j % 8 + 1, :]
        return jnp.where(low == places, unit, 0)

    def add(left, right):
        return right if left is None else [a + b for a, b in zip(left, right)]

    nibbles = None
    bytes_ = None
    held = 0
    for start_j in range(0, bag, 3):
        group = range(start_j, min(start_j + 3, bag))
        words = mark(group[0])
        for j in group[1:]:
            words = words + mark(j)
        nibbles = add(nibbles, fold(words, 2, 0x33333333))
        held += len(group)
        if held > 12 or group[-1] == bag - 1:
            even = fold(nibbles[0], 4, 0x0F0F0F0F)
            odd = fold(nibbles[1], 4, 0x0F0F0F0F)
            bytes_ = add(bytes_, [even[0], odd[0], even[1], odd[1]])
            nibbles = None
            held = 0
    return jnp.concatenate(bytes_, axis=0)


def pool(ids_ref, table_ref, pooled_ref):
    samples = ids_ref.shape[1]
    active = table_ref.shape[0]
    lanes = 128
    fields = active // lanes
    places = lax.broadcasted_iota(jnp.int32, (lanes // 4, lanes), 0)

    def finish(packed, index):
        turned = packed.T
        counts = jnp.concatenate(
            [
                ((turned >> (8 * field)) & 255).astype(jnp.float32).astype(jnp.bfloat16)
                for field in range(fields)
            ],
            axis=1,
        )
        pooled_ref[pl.ds(pl.multiple_of(index * lanes, lanes), lanes), :] = jnp.dot(
            counts, table_ref[...], preferred_element_type=jnp.float32
        )

    def chunk(index, packed):
        finish(packed, index - 1)
        return tally(ids_ref, pl.multiple_of(index * lanes, lanes), places)

    chunks = samples // lanes
    last = lax.fori_loop(1, chunks, chunk, tally(ids_ref, 0, places))
    finish(last, chunks - 1)


def kernel(
    ids_hbm,
    table_hbm,
    order_ref,
    first_hbm,
    second_hbm,
    head_hbm,
    inter_hbm,
    out_ref,
    ids_v,
    table_v,
    pooled,
    permuted,
    xsend,
    xall,
    wall,
    total,
    cross,
    relay,
    final,
    relay_top,
    final_top,
    outsum,
    second_v,
    outbox,
    inbox,
    head_v,
    inter_v,
    spread_hi,
    spread_lo,
    load_sem,
    first_sem,
    w_send,
    w_recv,
    x_send,
    x_recv,
    c_send,
    c_recv,
    f_send,
    f_recv,
    o_send,
    o_recv,
    near_sem,
    far_sem,
    open_sem,
    towers,
):
    tower = lax.axis_index("tower")
    dev = lax.axis_index("dev")
    core = lax.rem(dev, CORES)
    chip = dev // CORES
    col = chip // RING
    row = lax.rem(chip, RING)
    chunks, _, tile = wall.shape
    emb = table_v.shape[1]
    block = permuted.shape[0]

    def along(step):
        return lax.rem(row + step, RING)

    def at_row(place):
        return {"dev": (col * RING + place) * CORES + core}

    partner = {"dev": dev + 1 - 2 * core}
    across = {"dev": ((1 - col) * RING + row) * CORES + core}

    mine = pl.ds(pl.multiple_of(row * emb, emb), emb)
    loads = [
        pltpu.make_async_copy(ids_hbm, ids_v, load_sem.at[0]),
        pltpu.make_async_copy(table_hbm, table_v, load_sem.at[1]),
        pltpu.make_async_copy(second_hbm, second_v, load_sem.at[2]),
        pltpu.make_async_copy(head_hbm, head_v, load_sem.at[3]),
        pltpu.make_async_copy(inter_hbm, inter_v, load_sem.at[4]),
    ]
    firsts = [
        pltpu.make_async_copy(
            first_hbm.at[:, pl.ds(n * tile, tile)], wall.at[n, mine, :], first_sem.at[n]
        )
        for n in range(chunks)
    ]
    loads[0].start()
    loads[1].start()
    for copy in firsts:
        copy.start()
    for copy in loads[2:]:
        copy.start()

    barrier = pltpu.get_barrier_semaphore()
    devices = CORES * RING * 2
    gate = dev == 0
    peers = [at_row(along(step))["dev"] for step in range(1, RING)]
    peers += [partner["dev"], across["dev"]]
    near = jnp.int32(0)
    for peer in peers:
        near = near + jnp.where(peer == 0, 1, 0)

    @pl.when(jnp.logical_not(gate))
    def _():
        for peer in peers:

            @pl.when(peer != 0)
            def _():
                pl.semaphore_signal(
                    barrier, inc=1, device_id={"dev": peer}, device_id_type=MESH
                )

        pl.semaphore_wait(barrier, len(peers) + 1 - near)

        @pl.when(near == 1)
        def _():
            pl.semaphore_signal(near_sem, inc=1, device_id={"dev": 0}, device_id_type=MESH)

        @pl.when(near == 0)
        def _():
            pl.semaphore_signal(far_sem, inc=1, device_id={"dev": 0}, device_id_type=MESH)

    @pl.when(gate)
    def _():
        for other in range(1, devices):
            pl.semaphore_signal(barrier, inc=1, device_id={"dev": other}, device_id_type=MESH)
        pl.semaphore_wait(near_sem, len(peers))

    def gate_towers():
        pl.semaphore_wait(far_sem, devices - 1 - len(peers))
        for step in range(1, towers):
            pl.semaphore_signal(
                barrier,
                inc=1,
                device_id={"tower": lax.rem(tower + step, towers)},
                device_id_type=MESH,
            )

    def gate_open():
        pl.semaphore_wait(barrier, towers - 1)
        for other in range(1, devices):
            pl.semaphore_signal(open_sem, inc=1, device_id={"dev": other}, device_id_type=MESH)

    for copy in firsts:
        copy.wait()

    steps = (1, 3, 2)

    def send_w(n, step):
        return pltpu.make_async_remote_copy(
            src_ref=wall.at[pl.ds(*SPANS[n]), mine, :],
            dst_ref=wall.at[pl.ds(*SPANS[n]), mine, :],
            send_sem=w_send.at[n, step],
            recv_sem=w_recv.at[n, row],
            device_id=at_row(along(step)),
            device_id_type=MESH,
        )

    def send_x(step):
        return pltpu.make_async_remote_copy(
            src_ref=xsend.at[along(step)],
            dst_ref=xall.at[:, mine],
            send_sem=x_send.at[step],
            recv_sem=x_recv.at[row],
            device_id=at_row(along(step)),
            device_id_type=MESH,
        )

    def permute_rows(place, store):
        for c in range(CORES):
            for x in range(2):
                start = ((x * RING + place) * CORES + c) * block

                def group(index, carry):
                    for q in range(16):
                        source = order_ref[start + index * 16 + q]
                        permuted[pl.ds(index * 16 + q, 1), :] = pooled[pl.ds(source, 1), :]
                    return carry

                lax.fori_loop(0, block // 16, group, 0)
                store(c * 2 + x, permuted[...].astype(jnp.bfloat16))

    for n in range(EARLY):
        for step in steps:
            send_w(n, step).start()
    pl.when(gate)(gate_towers)
    loads[0].wait()
    loads[1].wait()
    pool(ids_v, table_v, pooled)
    for step in steps:
        place = along(step)

        def keep(part, value):
            xsend[place, part * block : (part + 1) * block, :] = value

        permute_rows(place, keep)
        send_x(step).start()
    for n in range(EARLY, len(SPANS)):
        for step in steps:
            send_w(n, step).start()

    def keep_own(part, value):
        xall[part * block : (part + 1) * block, mine] = value

    permute_rows(row, keep_own)
    pl.when(gate)(gate_open)

    loads[4].wait()
    pairs = inter_v.shape[0]

    def widen(index, carry):
        start = pl.multiple_of(index * 16, 16)
        some = inter_v[pl.ds(start, 16), :]
        wide = jnp.broadcast_to(some[:, None, :], (16, 8, some.shape[1])).reshape(
            128, some.shape[1]
        )
        high = wide.astype(jnp.bfloat16)
        low = (wide - high.astype(jnp.float32)).astype(jnp.bfloat16)
        target = pl.multiple_of(index * 128, 128)
        spread_hi[pl.ds(target, 128), :] = high
        spread_lo[pl.ds(target, 128), :] = low
        return carry

    lax.fori_loop(0, pairs // 16, widen, 0)
    loads[2].wait()
    loads[3].wait()

    def arrived_w(n, step):
        source = along(step)
        span = pl.ds(pl.multiple_of(source * emb, emb), emb)
        return pltpu.make_async_remote_copy(
            src_ref=wall.at[pl.ds(*SPANS[n]), span, :],
            dst_ref=wall.at[pl.ds(*SPANS[n]), span, :],
            send_sem=w_send.at[n, step],
            recv_sem=w_recv.at[n, source],
            device_id=partner,
            device_id_type=MESH,
        )

    def arrived_x(step):
        source = along(step)
        span = pl.ds(pl.multiple_of(source * emb, emb), emb)
        return pltpu.make_async_remote_copy(
            src_ref=xsend.at[source],
            dst_ref=xall.at[:, span],
            send_sem=x_send.at[step],
            recv_sem=x_recv.at[source],
            device_id=partner,
            device_id_type=MESH,
        )

    def cross_copy(n):
        return pltpu.make_async_remote_copy(
            src_ref=total.at[n, 1 - core],
            dst_ref=cross.at[n],
            send_sem=c_send.at[n],
            recv_sem=c_recv.at[n],
            device_id=partner,
            device_id_type=MESH,
        )

    def final_copies(n):
        return [
            pltpu.make_async_remote_copy(
                src_ref=source.at[n],
                dst_ref=target.at[n],
                send_sem=f_send.at[n, which],
                recv_sem=f_recv.at[n, which],
                device_id=across,
                device_id_type=MESH,
            )
            for which, (source, target) in enumerate(((relay_top, final_top), (relay, final)))
        ]

    def first_layer(n):
        if n == 0:
            for step in steps:
                arrived_x(step).wait_recv()
        for index, (begin, _) in enumerate(SPANS):
            if begin == n:
                for step in steps:
                    arrived_w(index, step).wait_recv()
        part = jnp.dot(xall[...], wall[n], preferred_element_type=jnp.float32)
        total[n] = part.reshape(CORES, 2, block, tile)
        cross_copy(n).start()

    def add_cores(n):
        cross_copy(n).wait_recv()
        part = total[n, core, 1 - col] + cross[n, 1 - col]
        top = jnp.max(jnp.abs(part), axis=0, keepdims=True)
        steps_up = part * (LEVELS / jnp.maximum(top, 1e-30)) + (LEVELS + 1.5)
        relay[n] = (steps_up.astype(jnp.int32) - (LEVELS + 1)).astype(jnp.int16)
        relay_top[n] = jnp.broadcast_to(top, relay_top.shape[1:])
        for copy in final_copies(n):
            copy.start()

    def second_layer(n):
        for copy in final_copies(n):
            copy.wait_recv()
        other = final[n].astype(jnp.float32) * (final_top[n, 0:1, :] * (1.0 / LEVELS))
        preact = total[n, core, col] + cross[n, col] + other
        hidden = jnp.maximum(preact, 0.0).astype(jnp.bfloat16)
        part = jnp.dot(
            hidden, second_v[n * tile : (n + 1) * tile, :], preferred_element_type=jnp.float32
        )
        if n == 0:
            outsum[...] = part
        else:
            outsum[...] += part

    for n in range(chunks + 2):
        if n < chunks:
            first_layer(n)
        if 1 <= n <= chunks:
            add_cores(n - 1)
        if n >= 2:
            second_layer(n - 2)

    share = outbox.shape[1]
    outbox[...] = outsum[...].reshape(towers, share, outsum.shape[1]).astype(jnp.bfloat16)

    depth = towers // 2

    def other_tower(dz, dx):
        return lax.rem(tower // 2 + dz, depth) * 2 + lax.rem(lax.rem(tower, 2) + dx, 2)

    def send_o(dz, dx):
        peer = other_tower(dz, dx)
        return pltpu.make_async_remote_copy(
            src_ref=outbox.at[peer],
            dst_ref=inbox.at[tower],
            send_sem=o_send.at[dz * 2 + dx],
            recv_sem=o_recv.at[tower],
            device_id={"tower": peer},
            device_id_type=MESH,
        )

    @pl.when(jnp.logical_not(gate))
    def _():
        pl.semaphore_wait(open_sem, 1)

    for dz, dx in reversed(HOPS):
        send_o(dz, dx).start()
    inbox[tower] = outbox[tower]

    def head_part(source):
        return jnp.dot(inbox[source], head_v[source], preferred_element_type=jnp.float32)

    head = head_part(tower)
    for dz, dx in HOPS:
        source = other_tower(dz, dx)
        pltpu.make_async_remote_copy(
            src_ref=outbox.at[source],
            dst_ref=inbox.at[source],
            send_sem=o_send.at[dz * 2 + dx],
            recv_sem=o_recv.at[source],
            device_id=partner,
            device_id_type=MESH,
        ).wait_recv()
        head = head + head_part(source)

    zwidth = inbox.shape[2]
    stacked = (
        inbox[...].astype(jnp.float32).reshape(towers * share, zwidth).astype(jnp.bfloat16)
    )
    gram = lax.dot_general(
        stacked, stacked, (((1,), (1,)), ((), ())), preferred_element_type=jnp.float32
    )
    left = lax.rem(lax.broadcasted_iota(jnp.int32, gram.shape, 0), share)
    right = lax.rem(lax.broadcasted_iota(jnp.int32, gram.shape, 1), share)
    gram = jnp.where(left == right, gram / math.sqrt(zwidth), 0.0)
    flat = jnp.concatenate(
        [gram[t * share : (t + 1) * share, :] for t in range(towers)], axis=1
    )
    flat_hi = flat.astype(jnp.bfloat16)
    rest = flat - flat_hi.astype(jnp.float32)
    both = jnp.concatenate([flat_hi.astype(jnp.float32), rest], axis=0).astype(jnp.bfloat16)
    twice = jnp.dot(both, spread_hi[...], preferred_element_type=jnp.float32)
    interact = twice[:share] + twice[share:]
    interact += jnp.dot(flat_hi, spread_lo[...], preferred_element_type=jnp.float32)
    out_ref[...] = head + interact

    for step in steps:
        send_x(step).wait_send()
        for n in range(len(SPANS)):
            send_w(n, step).wait_send()
    for n in range(chunks):
        cross_copy(n).wait_send()
        for copy in final_copies(n):
            copy.wait_send()
    for dz, dx in HOPS:
        send_o(dz, dx).wait_send()


def on_device(ids, tables, order, w_first, w_second, w_head, w_interact):
    towers = lax.axis_size("tower")
    devices = lax.axis_size("dev")
    samples, bag = ids.shape[2:]
    active, emb = tables.shape[2:]
    hidden = w_first.shape[2]
    zwidth = w_second.shape[2]
    heads = w_head.shape[1]
    block = samples // devices
    share = block // towers
    quarter = samples // RING
    pairs = w_interact.shape[0]
    tile = hidden // CHUNKS
    vmem = pltpu.VMEM
    dma = pltpu.SemaphoreType.DMA
    anywhere = pl.BlockSpec(memory_space=pltpu.HBM)
    scores = pl.pallas_call(
        functools.partial(kernel, towers=towers),
        out_shape=jax.ShapeDtypeStruct((share, heads), jnp.float32),
        in_specs=[
            anywhere,
            anywhere,
            pl.BlockSpec(memory_space=pltpu.SMEM),
            anywhere,
            anywhere,
            anywhere,
            anywhere,
        ],
        out_specs=pl.BlockSpec(memory_space=vmem),
        scratch_shapes=[
            vmem((bag, samples), jnp.int32),
            vmem((active, emb), jnp.bfloat16),
            vmem((samples, emb), jnp.float32),
            vmem((block, emb), jnp.float32),
            vmem((RING, quarter, emb), jnp.bfloat16),
            vmem((quarter, RING * emb), jnp.bfloat16),
            vmem((CHUNKS, RING * emb, tile), jnp.bfloat16),
            vmem((CHUNKS, CORES, 2, block, tile), jnp.float32),
            vmem((CHUNKS, 2, block, tile), jnp.float32),
            vmem((CHUNKS, block, tile), jnp.int16),
            vmem((CHUNKS, block, tile), jnp.int16),
            vmem((CHUNKS, 8, tile), jnp.float32),
            vmem((CHUNKS, 8, tile), jnp.float32),
            vmem((block, zwidth), jnp.float32),
            vmem((hidden, zwidth), jnp.bfloat16),
            vmem((towers, share, zwidth), jnp.bfloat16),
            vmem((towers, share, zwidth), jnp.bfloat16),
            vmem((towers, zwidth, heads), jnp.bfloat16),
            vmem((pairs, heads), jnp.float32),
            vmem((pairs * share, heads), jnp.bfloat16),
            vmem((pairs * share, heads), jnp.bfloat16),
            dma((5,)),
            dma((CHUNKS,)),
            dma((len(SPANS), RING)),
            dma((len(SPANS), RING)),
            dma((RING,)),
            dma((RING,)),
            dma((CHUNKS,)),
            dma((CHUNKS,)),
            dma((CHUNKS, 2)),
            dma((CHUNKS, 2)),
            dma((towers,)),
            dma((towers,)),
            pltpu.SemaphoreType.REGULAR,
            pltpu.SemaphoreType.REGULAR,
            pltpu.SemaphoreType.REGULAR,
        ],
        compiler_params=pltpu.CompilerParams(
            collective_id=0, has_side_effects=True, vmem_limit_bytes=32 * 1024 * 1024
        ),
    )(
        *(
            pltpu.with_memory_space_constraint(value, pltpu.HBM)
            for value in (
                jnp.swapaxes(ids[0, 0], 0, 1),
                tables[0, 0],
                order,
                w_first[0],
                w_second[0],
                w_head.reshape(towers, zwidth, heads),
                w_interact,
            )
        ),
    )
    return scores[None]


def solution(mesh):
    return jax.shard_map(
        on_device,
        mesh=mesh,
        in_specs=(
            P("tower", "dev", None, None),
            P("tower", "dev", None, None),
            P(),
            P("tower", "dev", None),
            P("tower", None, None),
            P(),
            P(),
        ),
        out_specs=P("dev", "tower", None),
        check_vma=False,
    )
```

```python
import functools
import math

import jax
import jax.numpy as jnp
from jax import lax
from jax.experimental import pallas as pl
from jax.experimental.pallas import tpu as pltpu
from jax.sharding import PartitionSpec as P

MESH = pl.DeviceIdType.MESH
RING = 4
CORES = 2
CHUNKS = 8
SPANS = ((0, 4), (4, 2), (6, 2))
GROUPS = ((0, 2), (2, 2), (4, 2), (6, 2))
EARLY = 1
RELAYED = 0
LEVELS = 32767
HOPS = (
    (1, 0),
    (7, 0),
    (2, 0),
    (6, 0),
    (0, 1),
    (1, 1),
    (7, 1),
    (3, 0),
    (5, 0),
    (2, 1),
    (6, 1),
    (4, 0),
    (3, 1),
    (5, 1),
    (4, 1),
)


def fold(words, shift, mask):
    return words & mask, lax.shift_right_logical(words, shift) & mask


def tally(ids_ref, start, places):
    bag = ids_ref.shape[0]
    lanes = places.shape[1]
    low_bits = places.shape[0]
    shift = low_bits.bit_length() - 1
    rows = [ids_ref[pl.ds(8 * g, 8), pl.ds(start, lanes)] for g in range(bag // 8)]
    lows = [row & (low_bits - 1) for row in rows]
    units = [jnp.left_shift(1, (row >> shift) << 1) for row in rows]

    def mark(j):
        low = lows[j // 8][j % 8 : j % 8 + 1, :]
        unit = units[j // 8][j % 8 : j % 8 + 1, :]
        return jnp.where(low == places, unit, 0)

    def add(left, right):
        return right if left is None else [a + b for a, b in zip(left, right)]

    nibbles = None
    bytes_ = None
    held = 0
    for start_j in range(0, bag, 3):
        group = range(start_j, min(start_j + 3, bag))
        words = mark(group[0])
        for j in group[1:]:
            words = words + mark(j)
        nibbles = add(nibbles, fold(words, 2, 0x33333333))
        held += len(group)
        if held > 12 or group[-1] == bag - 1:
            even = fold(nibbles[0], 4, 0x0F0F0F0F)
            odd = fold(nibbles[1], 4, 0x0F0F0F0F)
            bytes_ = add(bytes_, [even[0], odd[0], even[1], odd[1]])
            nibbles = None
            held = 0
    return jnp.concatenate(bytes_, axis=0)


def pool(ids_ref, table_ref, pooled_ref):
    samples = ids_ref.shape[1]
    active = table_ref.shape[0]
    lanes = 128
    fields = active // lanes
    places = lax.broadcasted_iota(jnp.int32, (lanes // 4, lanes), 0)

    def finish(packed, index):
        turned = packed.T
        counts = jnp.concatenate(
            [
                ((turned >> (8 * field)) & 255).astype(jnp.float32).astype(jnp.bfloat16)
                for field in range(fields)
            ],
            axis=1,
        )
        pooled_ref[pl.ds(pl.multiple_of(index * lanes, lanes), lanes), :] = jnp.dot(
            counts, table_ref[...], preferred_element_type=jnp.float32
        )

    def chunk(index, packed):
        finish(packed, index - 1)
        return tally(ids_ref, pl.multiple_of(index * lanes, lanes), places)

    chunks = samples // lanes
    last = lax.fori_loop(1, chunks, chunk, tally(ids_ref, 0, places))
    finish(last, chunks - 1)


def kernel(
    ids_hbm,
    table_hbm,
    order_ref,
    first_hbm,
    second_hbm,
    head_hbm,
    inter_hbm,
    out_ref,
    ids_v,
    table_v,
    pooled,
    permuted,
    xsend,
    xall,
    wall,
    total,
    cross,
    relay,
    final,
    relay_top,
    final_top,
    outsum,
    second_v,
    outbox,
    inbox,
    head_v,
    inter_v,
    spread_hi,
    spread_lo,
    load_sem,
    first_sem,
    w_send,
    w_recv,
    r_send,
    r_recv,
    x_send,
    x_recv,
    c_send,
    c_recv,
    f_send,
    f_recv,
    o_send,
    o_recv,
    near_sem,
    far_sem,
    open_sem,
    towers,
):
    tower = lax.axis_index("tower")
    dev = lax.axis_index("dev")
    core = lax.rem(dev, CORES)
    chip = dev // CORES
    col = chip // RING
    row = lax.rem(chip, RING)
    chunks, _, tile = wall.shape
    emb = table_v.shape[1]
    block = permuted.shape[0]

    def along(step):
        return lax.rem(row + step, RING)

    def at_row(place):
        return {"dev": (col * RING + place) * CORES + core}

    partner = {"dev": dev + 1 - 2 * core}
    across = {"dev": ((1 - col) * RING + row) * CORES + core}

    mine = pl.ds(pl.multiple_of(row * emb, emb), emb)
    loads = [
        pltpu.make_async_copy(ids_hbm, ids_v, load_sem.at[0]),
        pltpu.make_async_copy(table_hbm, table_v, load_sem.at[1]),
        pltpu.make_async_copy(second_hbm, second_v, load_sem.at[2]),
        pltpu.make_async_copy(head_hbm, head_v, load_sem.at[3]),
        pltpu.make_async_copy(inter_hbm, inter_v, load_sem.at[4]),
    ]
    firsts = [
        pltpu.make_async_copy(
            first_hbm.at[:, pl.ds(n * tile, tile)], wall.at[n, mine, :], first_sem.at[n]
        )
        for n in range(chunks)
    ]
    loads[0].start()
    loads[1].start()
    for copy in firsts:
        copy.start()
    for copy in loads[2:]:
        copy.start()

    barrier = pltpu.get_barrier_semaphore()
    devices = CORES * RING * 2
    gate = dev == 0
    peers = [at_row(along(step))["dev"] for step in range(1, RING)]
    peers += [partner["dev"], across["dev"]]
    near = jnp.int32(0)
    for peer in peers:
        near = near + jnp.where(peer == 0, 1, 0)

    @pl.when(jnp.logical_not(gate))
    def _():
        for peer in peers:

            @pl.when(peer != 0)
            def _():
                pl.semaphore_signal(
                    barrier, inc=1, device_id={"dev": peer}, device_id_type=MESH
                )

        pl.semaphore_wait(barrier, len(peers) + 1 - near)

        @pl.when(near == 1)
        def _():
            pl.semaphore_signal(near_sem, inc=1, device_id={"dev": 0}, device_id_type=MESH)

        @pl.when(near == 0)
        def _():
            pl.semaphore_signal(far_sem, inc=1, device_id={"dev": 0}, device_id_type=MESH)

    @pl.when(gate)
    def _():
        for other in range(1, devices):
            pl.semaphore_signal(barrier, inc=1, device_id={"dev": other}, device_id_type=MESH)
        pl.semaphore_wait(near_sem, len(peers))

    def gate_towers():
        pl.semaphore_wait(far_sem, devices - 1 - len(peers))
        for step in range(1, towers):
            pl.semaphore_signal(
                barrier,
                inc=1,
                device_id={"tower": lax.rem(tower + step, towers)},
                device_id_type=MESH,
            )

    def gate_open():
        pl.semaphore_wait(barrier, towers - 1)
        for other in range(1, devices):
            pl.semaphore_signal(open_sem, inc=1, device_id={"dev": other}, device_id_type=MESH)

    for copy in firsts:
        copy.wait()

    steps = (1, 3, 2)

    def send_w(n, step):
        return pltpu.make_async_remote_copy(
            src_ref=wall.at[pl.ds(*SPANS[n]), mine, :],
            dst_ref=wall.at[pl.ds(*SPANS[n]), mine, :],
            send_sem=w_send.at[n, step],
            recv_sem=w_recv.at[n, row],
            device_id=at_row(along(step)),
            device_id_type=MESH,
        )

    def forward(n, half):
        source = along(3) if half == 0 else along(1)
        span = pl.ds(pl.multiple_of(source * emb + half * (emb // 2), emb // 2), emb // 2)
        return pltpu.make_async_remote_copy(
            src_ref=wall.at[pl.ds(*SPANS[n]), span, :],
            dst_ref=wall.at[pl.ds(*SPANS[n]), span, :],
            send_sem=r_send.at[n, half],
            recv_sem=r_recv.at[n, half],
            device_id=at_row(along(1) if half == 0 else along(3)),
            device_id_type=MESH,
        )

    def forwarded(n, half):
        source = along(2)
        span = pl.ds(pl.multiple_of(source * emb + half * (emb // 2), emb // 2), emb // 2)
        return pltpu.make_async_remote_copy(
            src_ref=wall.at[pl.ds(*SPANS[n]), span, :],
            dst_ref=wall.at[pl.ds(*SPANS[n]), span, :],
            send_sem=r_send.at[n, half],
            recv_sem=r_recv.at[n, half],
            device_id=partner,
            device_id_type=MESH,
        )

    def w_steps(n):
        return steps[:2] if n < RELAYED else steps

    def arrived_w(n, step):
        source = along(step)
        span = pl.ds(pl.multiple_of(source * emb, emb), emb)
        return pltpu.make_async_remote_copy(
            src_ref=wall.at[pl.ds(*SPANS[n]), span, :],
            dst_ref=wall.at[pl.ds(*SPANS[n]), span, :],
            send_sem=w_send.at[n, step],
            recv_sem=w_recv.at[n, source],
            device_id=partner,
            device_id_type=MESH,
        )

    def send_x(kind, step):
        return pltpu.make_async_remote_copy(
            src_ref=xsend.at[kind, along(step)],
            dst_ref=xall.at[kind, :, mine],
            send_sem=x_send.at[kind, step],
            recv_sem=x_recv.at[kind, row],
            device_id=at_row(along(step)),
            device_id_type=MESH,
        )

    def arrived_x(kind, step):
        source = along(step)
        span = pl.ds(pl.multiple_of(source * emb, emb), emb)
        return pltpu.make_async_remote_copy(
            src_ref=xsend.at[kind, source],
            dst_ref=xall.at[kind, :, span],
            send_sem=x_send.at[kind, step],
            recv_sem=x_recv.at[kind, source],
            device_id=partner,
            device_id_type=MESH,
        )

    def permute_rows(kind, place, store):
        x = 1 - col if kind == 0 else col
        for c in range(CORES):
            start = ((x * RING + place) * CORES + c) * block

            def group(index, carry):
                for q in range(16):
                    source = order_ref[start + index * 16 + q]
                    permuted[pl.ds(index * 16 + q, 1), :] = pooled[pl.ds(source, 1), :]
                return carry

            lax.fori_loop(0, block // 16, group, 0)
            store(c, permuted[...].astype(jnp.bfloat16))

    def permute_send(kind):
        for step in steps:
            place = along(step)

            def keep(part, value):
                xsend[kind, place, part * block : (part + 1) * block, :] = value

            permute_rows(kind, place, keep)
            send_x(kind, step).start()

    def permute_own(kind):
        def keep(part, value):
            xall[kind, part * block : (part + 1) * block, mine] = value

        permute_rows(kind, row, keep)

    for n in range(EARLY):
        for step in w_steps(n):
            send_w(n, step).start()
    pl.when(gate)(gate_towers)
    loads[0].wait()
    loads[1].wait()
    pool(ids_v, table_v, pooled)
    permute_send(0)
    for n in range(RELAYED):
        for half, near_step in ((0, 3), (1, 1)):
            arrived_w(n, near_step).wait_recv()
            forward(n, half).start()
    for n in range(EARLY, len(SPANS)):
        for step in w_steps(n):
            send_w(n, step).start()
    permute_own(0)
    permute_send(1)
    permute_own(1)
    pl.when(gate)(gate_open)

    loads[4].wait()
    pairs = inter_v.shape[0]

    def widen(index, carry):
        start = pl.multiple_of(index * 16, 16)
        some = inter_v[pl.ds(start, 16), :]
        wide = jnp.broadcast_to(some[:, None, :], (16, 8, some.shape[1])).reshape(
            128, some.shape[1]
        )
        high = wide.astype(jnp.bfloat16)
        low = (wide - high.astype(jnp.float32)).astype(jnp.bfloat16)
        target = pl.multiple_of(index * 128, 128)
        spread_hi[pl.ds(target, 128), :] = high
        spread_lo[pl.ds(target, 128), :] = low
        return carry

    lax.fori_loop(0, pairs // 16, widen, 0)
    loads[2].wait()
    loads[3].wait()

    def cross_copy(kind, g):
        return pltpu.make_async_remote_copy(
            src_ref=total.at[kind, pl.ds(*GROUPS[g]), 1 - core],
            dst_ref=cross.at[kind, pl.ds(*GROUPS[g])],
            send_sem=c_send.at[kind, g],
            recv_sem=c_recv.at[kind, g],
            device_id=partner,
            device_id_type=MESH,
        )

    def final_copies(g):
        return [
            pltpu.make_async_remote_copy(
                src_ref=source.at[pl.ds(*GROUPS[g])],
                dst_ref=target.at[pl.ds(*GROUPS[g])],
                send_sem=f_send.at[g, which],
                recv_sem=f_recv.at[g, which],
                device_id=across,
                device_id_type=MESH,
            )
            for which, (source, target) in enumerate(((relay_top, final_top), (relay, final)))
        ]

    def tiles(g):
        return range(GROUPS[g][0], sum(GROUPS[g]))

    def arrived_span(g):
        for index, (begin, _) in enumerate(SPANS):
            if begin in tiles(g):
                if index < RELAYED:
                    for half in range(2):
                        forwarded(index, half).wait_recv()
                else:
                    for step in steps:
                        arrived_w(index, step).wait_recv()

    def first_layer(kind, g):
        for n in tiles(g):
            part = jnp.dot(xall[kind], wall[n], preferred_element_type=jnp.float32)
            total[kind, n] = part.reshape(CORES, block, tile)
        cross_copy(kind, g).start()

    def add_cores(g):
        cross_copy(0, g).wait_recv()
        for n in tiles(g):
            part = total[0, n, core] + cross[0, n]
            top = jnp.max(jnp.abs(part), axis=0, keepdims=True)
            steps_up = part * (LEVELS / jnp.maximum(top, 1e-30)) + (LEVELS + 1.5)
            relay[n] = (steps_up.astype(jnp.int32) - (LEVELS + 1)).astype(jnp.int16)
            relay_top[n] = jnp.broadcast_to(top, relay_top.shape[1:])
        for copy in final_copies(g):
            copy.start()

    def second_layer(g):
        cross_copy(1, g).wait_recv()
        for copy in final_copies(g):
            copy.wait_recv()
        hidden = []
        for n in tiles(g):
            other = final[n].astype(jnp.float32) * (final_top[n, 0:1, :] * (1.0 / LEVELS))
            preact = total[1, n, core] + cross[1, n] + other
            hidden.append(jnp.maximum(preact, 0.0).astype(jnp.bfloat16))
        begin, count = GROUPS[g]
        part = jnp.dot(
            jnp.concatenate(hidden, axis=1),
            second_v[begin * tile : (begin + count) * tile, :],
            preferred_element_type=jnp.float32,
        )
        if g == 0:
            outsum[...] = part
        else:
            outsum[...] += part

    groups = len(GROUPS)
    for step in steps:
        arrived_x(0, step).wait_recv()
    for g in range(groups + 1):
        if g < groups:
            arrived_span(g)
            first_layer(0, g)
        if g >= 1:
            add_cores(g - 1)
    for step in steps:
        arrived_x(1, step).wait_recv()
    for g in range(groups):
        first_layer(1, g)
    for g in range(groups):
        second_layer(g)

    share = outbox.shape[1]
    outbox[...] = outsum[...].reshape(towers, share, outsum.shape[1]).astype(jnp.bfloat16)

    depth = towers // 2

    def other_tower(dz, dx):
        return lax.rem(tower // 2 + dz, depth) * 2 + lax.rem(lax.rem(tower, 2) + dx, 2)

    def send_o(dz, dx):
        peer = other_tower(dz, dx)
        return pltpu.make_async_remote_copy(
            src_ref=outbox.at[peer],
            dst_ref=inbox.at[tower],
            send_sem=o_send.at[dz * 2 + dx],
            recv_sem=o_recv.at[tower],
            device_id={"tower": peer},
            device_id_type=MESH,
        )

    @pl.when(jnp.logical_not(gate))
    def _():
        pl.semaphore_wait(open_sem, 1)

    for dz, dx in reversed(HOPS):
        send_o(dz, dx).start()
    inbox[tower] = outbox[tower]

    def head_part(source):
        return jnp.dot(inbox[source], head_v[source], preferred_element_type=jnp.float32)

    head = head_part(tower)
    for dz, dx in HOPS:
        source = other_tower(dz, dx)
        pltpu.make_async_remote_copy(
            src_ref=outbox.at[source],
            dst_ref=inbox.at[source],
            send_sem=o_send.at[dz * 2 + dx],
            recv_sem=o_recv.at[source],
            device_id=partner,
            device_id_type=MESH,
        ).wait_recv()
        head = head + head_part(source)

    zwidth = inbox.shape[2]
    stacked = (
        inbox[...].astype(jnp.float32).reshape(towers * share, zwidth).astype(jnp.bfloat16)
    )
    gram = lax.dot_general(
        stacked, stacked, (((1,), (1,)), ((), ())), preferred_element_type=jnp.float32
    )
    left = lax.rem(lax.broadcasted_iota(jnp.int32, gram.shape, 0), share)
    right = lax.rem(lax.broadcasted_iota(jnp.int32, gram.shape, 1), share)
    gram = jnp.where(left == right, gram / math.sqrt(zwidth), 0.0)
    flat = jnp.concatenate(
        [gram[t * share : (t + 1) * share, :] for t in range(towers)], axis=1
    )
    flat_hi = flat.astype(jnp.bfloat16)
    rest = flat - flat_hi.astype(jnp.float32)
    both = jnp.concatenate([flat_hi.astype(jnp.float32), rest], axis=0).astype(jnp.bfloat16)
    twice = jnp.dot(both, spread_hi[...], preferred_element_type=jnp.float32)
    interact = twice[:share] + twice[share:]
    interact += jnp.dot(flat_hi, spread_lo[...], preferred_element_type=jnp.float32)
    out_ref[...] = head + interact

    for step in steps:
        send_x(0, step).wait_send()
        send_x(1, step).wait_send()
        for n in range(len(SPANS)):
            if step in w_steps(n):
                send_w(n, step).wait_send()
    for n in range(RELAYED):
        for half in range(2):
            forward(n, half).wait_send()
    for g in range(groups):
        cross_copy(0, g).wait_send()
        cross_copy(1, g).wait_send()
        for copy in final_copies(g):
            copy.wait_send()
    for dz, dx in HOPS:
        send_o(dz, dx).wait_send()


def on_device(ids, tables, order, w_first, w_second, w_head, w_interact):
    towers = lax.axis_size("tower")
    devices = lax.axis_size("dev")
    samples, bag = ids.shape[2:]
    active, emb = tables.shape[2:]
    hidden = w_first.shape[2]
    zwidth = w_second.shape[2]
    heads = w_head.shape[1]
    block = samples // devices
    share = block // towers
    quarter = samples // RING
    pairs = w_interact.shape[0]
    tile = hidden // CHUNKS
    vmem = pltpu.VMEM
    dma = pltpu.SemaphoreType.DMA
    anywhere = pl.BlockSpec(memory_space=pltpu.HBM)
    scores = pl.pallas_call(
        functools.partial(kernel, towers=towers),
        out_shape=jax.ShapeDtypeStruct((share, heads), jnp.float32),
        in_specs=[
            anywhere,
            anywhere,
            pl.BlockSpec(memory_space=pltpu.SMEM),
            anywhere,
            anywhere,
            anywhere,
            anywhere,
        ],
        out_specs=pl.BlockSpec(memory_space=vmem),
        scratch_shapes=[
            vmem((bag, samples), jnp.int32),
            vmem((active, emb), jnp.bfloat16),
            vmem((samples, emb), jnp.float32),
            vmem((block, emb), jnp.float32),
            vmem((2, RING, quarter // 2, emb), jnp.bfloat16),
            vmem((2, quarter // 2, RING * emb), jnp.bfloat16),
            vmem((CHUNKS, RING * emb, tile), jnp.bfloat16),
            vmem((2, CHUNKS, CORES, block, tile), jnp.float32),
            vmem((2, CHUNKS, block, tile), jnp.float32),
            vmem((CHUNKS, block, tile), jnp.int16),
            vmem((CHUNKS, block, tile), jnp.int16),
            vmem((CHUNKS, 8, tile), jnp.float32),
            vmem((CHUNKS, 8, tile), jnp.float32),
            vmem((block, zwidth), jnp.float32),
            vmem((hidden, zwidth), jnp.bfloat16),
            vmem((towers, share, zwidth), jnp.bfloat16),
            vmem((towers, share, zwidth), jnp.bfloat16),
            vmem((towers, zwidth, heads), jnp.bfloat16),
            vmem((pairs, heads), jnp.float32),
            vmem((pairs * share, heads), jnp.bfloat16),
            vmem((pairs * share, heads), jnp.bfloat16),
            dma((5,)),
            dma((CHUNKS,)),
            dma((len(SPANS), RING)),
            dma((len(SPANS), RING)),
            dma((len(SPANS), 2)),
            dma((len(SPANS), 2)),
            dma((2, RING)),
            dma((2, RING)),
            dma((2, CHUNKS)),
            dma((2, CHUNKS)),
            dma((CHUNKS, 2)),
            dma((CHUNKS, 2)),
            dma((towers,)),
            dma((towers,)),
            pltpu.SemaphoreType.REGULAR,
            pltpu.SemaphoreType.REGULAR,
            pltpu.SemaphoreType.REGULAR,
        ],
        compiler_params=pltpu.CompilerParams(
            collective_id=0, has_side_effects=True, vmem_limit_bytes=32 * 1024 * 1024
        ),
    )(
        *(
            pltpu.with_memory_space_constraint(value, pltpu.HBM)
            for value in (
                jnp.swapaxes(ids[0, 0], 0, 1),
                tables[0, 0],
                order,
                w_first[0],
                w_second[0],
                w_head.reshape(towers, zwidth, heads),
                w_interact,
            )
        ),
    )
    return scores[None]


def solution(mesh):
    return jax.shard_map(
        on_device,
        mesh=mesh,
        in_specs=(
            P("tower", "dev", None, None),
            P("tower", "dev", None, None),
            P(),
            P("tower", "dev", None),
            P("tower", None, None),
            P(),
            P(),
        ),
        out_specs=P("dev", "tower", None),
        check_vma=False,
    )
```

```python
import functools
import math

import jax
import jax.numpy as jnp
from jax import lax
from jax.experimental import pallas as pl
from jax.experimental.pallas import tpu as pltpu
from jax.sharding import PartitionSpec as P

MESH = pl.DeviceIdType.MESH
RING = 4
CORES = 2
CHUNKS = 8
BATCH = 8
UNROLL = 1
SPANS = ((0, 4), (4, 2), (6, 2))
GROUPS = ((0, 2), (2, 2), (4, 2), (6, 2))
EARLY = 2
RELAYED = 2
AHEAD = 0
LEVELS = 32752
PARTS = 16384
HOPS = (
    (1, 0),
    (7, 0),
    (2, 0),
    (6, 0),
    (0, 1),
    (1, 1),
    (7, 1),
    (3, 0),
    (5, 0),
    (2, 1),
    (6, 1),
    (4, 0),
    (3, 1),
    (5, 1),
    (4, 1),
)


def fold(words, shift, mask):
    return words & mask, lax.shift_right_logical(words, shift) & mask


def tally(ids_ref, start, places):
    bag = ids_ref.shape[0]
    lanes = places.shape[1]
    low_bits = places.shape[0]
    shift = low_bits.bit_length() - 1
    rows = [ids_ref[pl.ds(8 * g, 8), pl.ds(start, lanes)] for g in range(bag // 8)]
    lows = [row & (low_bits - 1) for row in rows]
    units = [jnp.left_shift(1, (row >> shift) << 1) for row in rows]

    def mark(j):
        low = lows[j // 8][j % 8 : j % 8 + 1, :]
        unit = units[j // 8][j % 8 : j % 8 + 1, :]
        return jnp.where(low == places, unit, 0)

    def add(left, right):
        return right if left is None else [a + b for a, b in zip(left, right)]

    nibbles = None
    bytes_ = None
    held = 0
    for start_j in range(0, bag, 3):
        group = range(start_j, min(start_j + 3, bag))
        words = mark(group[0])
        for j in group[1:]:
            words = words + mark(j)
        nibbles = add(nibbles, fold(words, 2, 0x33333333))
        held += len(group)
        if held > 12 or group[-1] == bag - 1:
            even = fold(nibbles[0], 4, 0x0F0F0F0F)
            odd = fold(nibbles[1], 4, 0x0F0F0F0F)
            bytes_ = add(bytes_, [even[0], odd[0], even[1], odd[1]])
            nibbles = None
            held = 0
    return jnp.concatenate(bytes_, axis=0)


def pool(ids_ref, table_ref, packed_ref, pooled_ref):
    samples = ids_ref.shape[1]
    active = table_ref.shape[0]
    lanes = 128
    fields = active // lanes
    places = lax.broadcasted_iota(jnp.int32, (lanes // 4, lanes), 0)
    chunks = samples // lanes

    def count(index, carry):
        packed_ref[index] = tally(ids_ref, pl.multiple_of(index * lanes, lanes), places)
        return carry

    lax.fori_loop(0, chunks, count, 0, unroll=UNROLL)

    def spread(words):
        turned = words.T
        return jnp.concatenate(
            [
                ((turned >> (8 * field)) & 255).astype(jnp.float32).astype(jnp.bfloat16)
                for field in range(fields)
            ],
            axis=1,
        )

    def look_up(index, carry):
        counts = jnp.concatenate(
            [spread(packed_ref[index * BATCH + part]) for part in range(BATCH)], axis=0
        )
        start = pl.multiple_of(index * BATCH * lanes, BATCH * lanes)
        pooled_ref[pl.ds(start, BATCH * lanes), :] = jnp.dot(
            counts, table_ref[...], preferred_element_type=jnp.float32
        )
        return carry

    lax.fori_loop(0, chunks // BATCH, look_up, 0)


def decode(exponent, fraction):
    return jnp.exp2(exponent.astype(jnp.float32)) * (fraction.astype(jnp.float32) / PARTS)


def encode(top):
    exponent = jnp.floor(jnp.log2(jnp.maximum(top, 1e-30))) + 1.0
    fraction = (top * jnp.exp2(-exponent) * PARTS).astype(jnp.int32) + 1
    return exponent.astype(jnp.int32), fraction


def kernel(
    ids_hbm,
    table_hbm,
    order_ref,
    first_hbm,
    second_hbm,
    head_hbm,
    inter_hbm,
    out_ref,
    ids_v,
    table_v,
    packed,
    pooled,
    permuted,
    xsend,
    xall,
    wall,
    total,
    cross,
    relay,
    final,
    outsum,
    second_v,
    outbox,
    inbox,
    head_v,
    inter_v,
    spread_hi,
    spread_lo,
    load_sem,
    first_sem,
    w_send,
    w_recv,
    r_send,
    r_recv,
    x_send,
    x_recv,
    c_send,
    c_recv,
    f_send,
    f_recv,
    o_send,
    o_recv,
    near_sem,
    far_sem,
    open_sem,
    towers,
):
    tower = lax.axis_index("tower")
    dev = lax.axis_index("dev")
    core = lax.rem(dev, CORES)
    chip = dev // CORES
    col = chip // RING
    row = lax.rem(chip, RING)
    chunks, _, tile = wall.shape
    emb = table_v.shape[1]
    block = permuted.shape[0]

    def along(step):
        return lax.rem(row + step, RING)

    def at_row(place):
        return {"dev": (col * RING + place) * CORES + core}

    partner = {"dev": dev + 1 - 2 * core}
    across = {"dev": ((1 - col) * RING + row) * CORES + core}

    mine = pl.ds(pl.multiple_of(row * emb, emb), emb)
    loads = [
        pltpu.make_async_copy(ids_hbm, ids_v, load_sem.at[0]),
        pltpu.make_async_copy(table_hbm, table_v, load_sem.at[1]),
        pltpu.make_async_copy(second_hbm, second_v, load_sem.at[2]),
        pltpu.make_async_copy(head_hbm, head_v, load_sem.at[3]),
        pltpu.make_async_copy(inter_hbm, inter_v, load_sem.at[4]),
    ]
    firsts = [
        pltpu.make_async_copy(
            first_hbm.at[:, pl.ds(n * tile, tile)], wall.at[n, mine, :], first_sem.at[n]
        )
        for n in range(chunks)
    ]
    loads[0].start()
    loads[1].start()
    for copy in firsts:
        copy.start()
    for copy in loads[2:]:
        copy.start()

    barrier = pltpu.get_barrier_semaphore()
    devices = CORES * RING * 2
    gate = dev == 0
    peers = [at_row(along(step))["dev"] for step in range(1, RING)]
    peers += [partner["dev"], across["dev"]]
    near = jnp.int32(0)
    for peer in peers:
        near = near + jnp.where(peer == 0, 1, 0)

    @pl.when(jnp.logical_not(gate))
    def _():
        for peer in peers:

            @pl.when(peer != 0)
            def _():
                pl.semaphore_signal(
                    barrier, inc=1, device_id={"dev": peer}, device_id_type=MESH
                )

        pl.semaphore_wait(barrier, len(peers) + 1 - near)

        @pl.when(near == 1)
        def _():
            pl.semaphore_signal(near_sem, inc=1, device_id={"dev": 0}, device_id_type=MESH)

        @pl.when(near == 0)
        def _():
            pl.semaphore_signal(far_sem, inc=1, device_id={"dev": 0}, device_id_type=MESH)

    @pl.when(gate)
    def _():
        for other in range(1, devices):
            pl.semaphore_signal(barrier, inc=1, device_id={"dev": other}, device_id_type=MESH)
        pl.semaphore_wait(near_sem, len(peers))

    def gate_towers():
        pl.semaphore_wait(far_sem, devices - 1 - len(peers))
        for step in range(1, towers):
            pl.semaphore_signal(
                barrier,
                inc=1,
                device_id={"tower": lax.rem(tower + step, towers)},
                device_id_type=MESH,
            )

    def gate_open():
        pl.semaphore_wait(barrier, towers - 1)
        for other in range(1, devices):
            pl.semaphore_signal(open_sem, inc=1, device_id={"dev": other}, device_id_type=MESH)

    for copy in firsts:
        copy.wait()

    steps = (1, 3, 2)

    def send_w(n, step):
        return pltpu.make_async_remote_copy(
            src_ref=wall.at[pl.ds(*SPANS[n]), mine, :],
            dst_ref=wall.at[pl.ds(*SPANS[n]), mine, :],
            send_sem=w_send.at[n, step],
            recv_sem=w_recv.at[n, row],
            device_id=at_row(along(step)),
            device_id_type=MESH,
        )

    def forward(n, half):
        source = along(3) if half == 0 else along(1)
        span = pl.ds(pl.multiple_of(source * emb + half * (emb // 2), emb // 2), emb // 2)
        return pltpu.make_async_remote_copy(
            src_ref=wall.at[pl.ds(*SPANS[n]), span, :],
            dst_ref=wall.at[pl.ds(*SPANS[n]), span, :],
            send_sem=r_send.at[n, half],
            recv_sem=r_recv.at[n, half],
            device_id=at_row(along(1) if half == 0 else along(3)),
            device_id_type=MESH,
        )

    def forwarded(n, half):
        source = along(2)
        span = pl.ds(pl.multiple_of(source * emb + half * (emb // 2), emb // 2), emb // 2)
        return pltpu.make_async_remote_copy(
            src_ref=wall.at[pl.ds(*SPANS[n]), span, :],
            dst_ref=wall.at[pl.ds(*SPANS[n]), span, :],
            send_sem=r_send.at[n, half],
            recv_sem=r_recv.at[n, half],
            device_id=partner,
            device_id_type=MESH,
        )

    def w_steps(n):
        return steps[:2] if n < RELAYED else steps

    def arrived_w(n, step):
        source = along(step)
        span = pl.ds(pl.multiple_of(source * emb, emb), emb)
        return pltpu.make_async_remote_copy(
            src_ref=wall.at[pl.ds(*SPANS[n]), span, :],
            dst_ref=wall.at[pl.ds(*SPANS[n]), span, :],
            send_sem=w_send.at[n, step],
            recv_sem=w_recv.at[n, source],
            device_id=partner,
            device_id_type=MESH,
        )

    def send_x(kind, step):
        return pltpu.make_async_remote_copy(
            src_ref=xsend.at[kind, along(step)],
            dst_ref=xall.at[kind, :, mine],
            send_sem=x_send.at[kind, step],
            recv_sem=x_recv.at[kind, row],
            device_id=at_row(along(step)),
            device_id_type=MESH,
        )

    def arrived_x(kind, step):
        source = along(step)
        span = pl.ds(pl.multiple_of(source * emb, emb), emb)
        return pltpu.make_async_remote_copy(
            src_ref=xsend.at[kind, source],
            dst_ref=xall.at[kind, :, span],
            send_sem=x_send.at[kind, step],
            recv_sem=x_recv.at[kind, source],
            device_id=partner,
            device_id_type=MESH,
        )

    def permute_rows(kind, place, store):
        x = 1 - col if kind == 0 else col
        for c in range(CORES):
            start = ((x * RING + place) * CORES + c) * block

            def group(index, carry):
                for q in range(16):
                    source = order_ref[start + index * 16 + q]
                    permuted[pl.ds(index * 16 + q, 1), :] = pooled[pl.ds(source, 1), :]
                return carry

            lax.fori_loop(0, block // 16, group, 0)
            store(c, permuted[...].astype(jnp.bfloat16))

    def permute_send(kind):
        for step in steps:
            place = along(step)

            def keep(part, value):
                xsend[kind, place, part * block : (part + 1) * block, :] = value

            permute_rows(kind, place, keep)
            send_x(kind, step).start()

    def permute_own(kind):
        def keep(part, value):
            xall[kind, part * block : (part + 1) * block, mine] = value

        permute_rows(kind, row, keep)

    for n in range(EARLY):
        for step in w_steps(n):
            send_w(n, step).start()
    pl.when(gate)(gate_towers)
    loads[0].wait()
    loads[1].wait()
    pool(ids_v, table_v, packed, pooled)
    def relay_rows(n):
        for half, near_step in ((0, 3), (1, 1)):
            arrived_w(n, near_step).wait_recv()
            forward(n, half).start()

    for n in range(AHEAD):
        relay_rows(n)
    permute_send(0)
    for n in range(AHEAD, RELAYED):
        relay_rows(n)
    for n in range(EARLY, len(SPANS)):
        for step in w_steps(n):
            send_w(n, step).start()
    permute_own(0)
    permute_send(1)
    permute_own(1)
    pl.when(gate)(gate_open)

    loads[4].wait()
    pairs = inter_v.shape[0]

    def widen(index, carry):
        start = pl.multiple_of(index * 16, 16)
        some = inter_v[pl.ds(start, 16), :]
        wide = jnp.broadcast_to(some[:, None, :], (16, 8, some.shape[1])).reshape(
            128, some.shape[1]
        )
        high = wide.astype(jnp.bfloat16)
        low = (wide - high.astype(jnp.float32)).astype(jnp.bfloat16)
        target = pl.multiple_of(index * 128, 128)
        spread_hi[pl.ds(target, 128), :] = high
        spread_lo[pl.ds(target, 128), :] = low
        return carry

    lax.fori_loop(0, pairs // 16, widen, 0)
    loads[2].wait()
    loads[3].wait()

    def cross_copy(kind, g):
        return pltpu.make_async_remote_copy(
            src_ref=total.at[kind, pl.ds(*GROUPS[g]), 1 - core],
            dst_ref=cross.at[kind, pl.ds(*GROUPS[g])],
            send_sem=c_send.at[kind, g],
            recv_sem=c_recv.at[kind, g],
            device_id=partner,
            device_id_type=MESH,
        )

    def final_copy(g):
        return pltpu.make_async_remote_copy(
            src_ref=relay.at[pl.ds(*GROUPS[g])],
            dst_ref=final.at[pl.ds(*GROUPS[g])],
            send_sem=f_send.at[g],
            recv_sem=f_recv.at[g],
            device_id=across,
            device_id_type=MESH,
        )

    def tiles(g):
        return range(GROUPS[g][0], sum(GROUPS[g]))

    def arrived_span(g):
        for index, (begin, _) in enumerate(SPANS):
            if begin in tiles(g):
                if index < RELAYED:
                    for half in range(2):
                        forwarded(index, half).wait_recv()
                else:
                    for step in steps:
                        arrived_w(index, step).wait_recv()

    def first_layer(kind, g):
        for n in tiles(g):
            part = jnp.dot(xall[kind], wall[n], preferred_element_type=jnp.float32)
            total[kind, n] = part.reshape(CORES, block, tile)
        cross_copy(kind, g).start()

    def add_cores(g):
        cross_copy(0, g).wait_recv()
        for n in tiles(g):
            part = total[0, n, core] + cross[0, n]
            exponent, fraction = encode(jnp.max(jnp.abs(part), axis=0, keepdims=True))
            steps_up = part * (LEVELS / decode(exponent, fraction)) + (LEVELS + 1.5)
            relay[n, :block, :] = (steps_up.astype(jnp.int32) - (LEVELS + 1)).astype(jnp.int16)
            line = lax.broadcasted_iota(jnp.int32, (16, tile), 0)
            code = jnp.where(line == 0, exponent, jnp.where(line == 1, fraction, 0))
            relay[n, block:, :] = code.astype(jnp.int16)
        final_copy(g).start()

    def second_layer(g):
        cross_copy(1, g).wait_recv()
        final_copy(g).wait_recv()
        hidden = []
        for n in tiles(g):
            code = final[n, block:, :].astype(jnp.int32)
            unit = decode(code[0:1], code[1:2]) * (1.0 / LEVELS)
            other = final[n, :block, :].astype(jnp.float32) * unit
            preact = total[1, n, core] + cross[1, n] + other
            hidden.append(jnp.maximum(preact, 0.0).astype(jnp.bfloat16))
        begin, count = GROUPS[g]
        part = jnp.dot(
            jnp.concatenate(hidden, axis=1),
            second_v[begin * tile : (begin + count) * tile, :],
            preferred_element_type=jnp.float32,
        )
        if g == 0:
            outsum[...] = part
        else:
            outsum[...] += part

    groups = len(GROUPS)
    for step in steps:
        arrived_x(0, step).wait_recv()
    for g in range(groups + 1):
        if g < groups:
            arrived_span(g)
            first_layer(0, g)
        if g >= 1:
            add_cores(g - 1)
    for step in steps:
        arrived_x(1, step).wait_recv()
    for g in range(groups):
        first_layer(1, g)
    for g in range(groups):
        second_layer(g)

    share = outbox.shape[1]
    outbox[...] = outsum[...].reshape(towers, share, outsum.shape[1]).astype(jnp.bfloat16)

    depth = towers // 2

    def other_tower(dz, dx):
        return lax.rem(tower // 2 + dz, depth) * 2 + lax.rem(lax.rem(tower, 2) + dx, 2)

    def send_o(dz, dx):
        peer = other_tower(dz, dx)
        return pltpu.make_async_remote_copy(
            src_ref=outbox.at[peer],
            dst_ref=inbox.at[tower],
            send_sem=o_send.at[dz * 2 + dx],
            recv_sem=o_recv.at[tower],
            device_id={"tower": peer},
            device_id_type=MESH,
        )

    @pl.when(jnp.logical_not(gate))
    def _():
        pl.semaphore_wait(open_sem, 1)

    for dz, dx in reversed(HOPS):
        send_o(dz, dx).start()
    inbox[tower] = outbox[tower]

    def head_part(source):
        return jnp.dot(inbox[source], head_v[source], preferred_element_type=jnp.float32)

    head = head_part(tower)
    for dz, dx in HOPS:
        source = other_tower(dz, dx)
        pltpu.make_async_remote_copy(
            src_ref=outbox.at[source],
            dst_ref=inbox.at[source],
            send_sem=o_send.at[dz * 2 + dx],
            recv_sem=o_recv.at[source],
            device_id=partner,
            device_id_type=MESH,
        ).wait_recv()
        head = head + head_part(source)

    zwidth = inbox.shape[2]
    stacked = (
        inbox[...].astype(jnp.float32).reshape(towers * share, zwidth).astype(jnp.bfloat16)
    )
    gram = lax.dot_general(
        stacked, stacked, (((1,), (1,)), ((), ())), preferred_element_type=jnp.float32
    )
    left = lax.rem(lax.broadcasted_iota(jnp.int32, gram.shape, 0), share)
    right = lax.rem(lax.broadcasted_iota(jnp.int32, gram.shape, 1), share)
    gram = jnp.where(left == right, gram / math.sqrt(zwidth), 0.0)
    flat = jnp.concatenate(
        [gram[t * share : (t + 1) * share, :] for t in range(towers)], axis=1
    )
    flat_hi = flat.astype(jnp.bfloat16)
    rest = flat - flat_hi.astype(jnp.float32)
    both = jnp.concatenate([flat_hi.astype(jnp.float32), rest], axis=0).astype(jnp.bfloat16)
    twice = jnp.dot(both, spread_hi[...], preferred_element_type=jnp.float32)
    interact = twice[:share] + twice[share:]
    interact += jnp.dot(flat_hi, spread_lo[...], preferred_element_type=jnp.float32)
    out_ref[...] = head + interact

    for step in steps:
        send_x(0, step).wait_send()
        send_x(1, step).wait_send()
        for n in range(len(SPANS)):
            if step in w_steps(n):
                send_w(n, step).wait_send()
    for n in range(RELAYED):
        for half in range(2):
            forward(n, half).wait_send()
    for g in range(groups):
        cross_copy(0, g).wait_send()
        cross_copy(1, g).wait_send()
        final_copy(g).wait_send()
    for dz, dx in HOPS:
        send_o(dz, dx).wait_send()


def on_device(ids, tables, order, w_first, w_second, w_head, w_interact):
    towers = lax.axis_size("tower")
    devices = lax.axis_size("dev")
    samples, bag = ids.shape[2:]
    active, emb = tables.shape[2:]
    hidden = w_first.shape[2]
    zwidth = w_second.shape[2]
    heads = w_head.shape[1]
    block = samples // devices
    share = block // towers
    quarter = samples // RING
    pairs = w_interact.shape[0]
    tile = hidden // CHUNKS
    vmem = pltpu.VMEM
    dma = pltpu.SemaphoreType.DMA
    anywhere = pl.BlockSpec(memory_space=pltpu.HBM)
    scores = pl.pallas_call(
        functools.partial(kernel, towers=towers),
        out_shape=jax.ShapeDtypeStruct((share, heads), jnp.float32),
        in_specs=[
            anywhere,
            anywhere,
            pl.BlockSpec(memory_space=pltpu.SMEM),
            anywhere,
            anywhere,
            anywhere,
            anywhere,
        ],
        out_specs=pl.BlockSpec(memory_space=vmem),
        scratch_shapes=[
            vmem((bag, samples), jnp.int32),
            vmem((active, emb), jnp.bfloat16),
            vmem((samples // 128, 128, 128), jnp.int32),
            vmem((samples, emb), jnp.float32),
            vmem((block, emb), jnp.float32),
            vmem((2, RING, quarter // 2, emb), jnp.bfloat16),
            vmem((2, quarter // 2, RING * emb), jnp.bfloat16),
            vmem((CHUNKS, RING * emb, tile), jnp.bfloat16),
            vmem((2, CHUNKS, CORES, block, tile), jnp.float32),
            vmem((2, CHUNKS, block, tile), jnp.float32),
            vmem((CHUNKS, block + 16, tile), jnp.int16),
            vmem((CHUNKS, block + 16, tile), jnp.int16),
            vmem((block, zwidth), jnp.float32),
            vmem((hidden, zwidth), jnp.bfloat16),
            vmem((towers, share, zwidth), jnp.bfloat16),
            vmem((towers, share, zwidth), jnp.bfloat16),
            vmem((towers, zwidth, heads), jnp.bfloat16),
            vmem((pairs, heads), jnp.float32),
            vmem((pairs * share, heads), jnp.bfloat16),
            vmem((pairs * share, heads), jnp.bfloat16),
            dma((5,)),
            dma((CHUNKS,)),
            dma((len(SPANS), RING)),
            dma((len(SPANS), RING)),
            dma((len(SPANS), 2)),
            dma((len(SPANS), 2)),
            dma((2, RING)),
            dma((2, RING)),
            dma((2, CHUNKS)),
            dma((2, CHUNKS)),
            dma((CHUNKS,)),
            dma((CHUNKS,)),
            dma((towers,)),
            dma((towers,)),
            pltpu.SemaphoreType.REGULAR,
            pltpu.SemaphoreType.REGULAR,
            pltpu.SemaphoreType.REGULAR,
        ],
        compiler_params=pltpu.CompilerParams(
            collective_id=0, has_side_effects=True, vmem_limit_bytes=32 * 1024 * 1024
        ),
    )(
        *(
            pltpu.with_memory_space_constraint(value, pltpu.HBM)
            for value in (
                jnp.swapaxes(ids[0, 0], 0, 1),
                tables[0, 0],
                order,
                w_first[0],
                w_second[0],
                w_head.reshape(towers, zwidth, heads),
                w_interact,
            )
        ),
    )
    return scores[None]


def solution(mesh):
    return jax.shard_map(
        on_device,
        mesh=mesh,
        in_specs=(
            P("tower", "dev", None, None),
            P("tower", "dev", None, None),
            P(),
            P("tower", "dev", None),
            P("tower", None, None),
            P(),
            P(),
        ),
        out_specs=P("dev", "tower", None),
        check_vma=False,
    )
```

```python
import functools
import math

import jax
import jax.numpy as jnp
from jax import lax
from jax.experimental import pallas as pl
from jax.experimental.pallas import tpu as pltpu
from jax.sharding import PartitionSpec as P

MESH = pl.DeviceIdType.MESH
RING = 4
CORES = 2
CHUNKS = 8
BATCH = 8
UNROLL = 1
SPANS = ((0, 3), (3, 3), (6, 2))
GROUPS = ((0, 3), (3, 3), (6, 2))
EARLY = 2
RELAYED = 2
AHEAD = 0
GATE = 1
LEVELS = 32752
PARTS = 16384
HOPS = (
    (1, 0),
    (7, 0),
    (2, 0),
    (6, 0),
    (0, 1),
    (1, 1),
    (7, 1),
    (3, 0),
    (5, 0),
    (2, 1),
    (6, 1),
    (4, 0),
    (3, 1),
    (5, 1),
    (4, 1),
)


def fold(words, shift, mask):
    return words & mask, lax.shift_right_logical(words, shift) & mask


def tally(ids_ref, start, places):
    bag = ids_ref.shape[0]
    lanes = places.shape[1]
    low_bits = places.shape[0]
    shift = low_bits.bit_length() - 1
    rows = [ids_ref[pl.ds(8 * g, 8), pl.ds(start, lanes)] for g in range(bag // 8)]
    lows = [row & (low_bits - 1) for row in rows]
    units = [jnp.left_shift(1, (row >> shift) << 1) for row in rows]

    def mark(j):
        low = lows[j // 8][j % 8 : j % 8 + 1, :]
        unit = units[j // 8][j % 8 : j % 8 + 1, :]
        return jnp.where(low == places, unit, 0)

    def add(left, right):
        return right if left is None else [a + b for a, b in zip(left, right)]

    nibbles = None
    bytes_ = None
    held = 0
    for start_j in range(0, bag, 3):
        group = range(start_j, min(start_j + 3, bag))
        words = mark(group[0])
        for j in group[1:]:
            words = words + mark(j)
        nibbles = add(nibbles, fold(words, 2, 0x33333333))
        held += len(group)
        if held > 12 or group[-1] == bag - 1:
            even = fold(nibbles[0], 4, 0x0F0F0F0F)
            odd = fold(nibbles[1], 4, 0x0F0F0F0F)
            bytes_ = add(bytes_, [even[0], odd[0], even[1], odd[1]])
            nibbles = None
            held = 0
    return jnp.concatenate(bytes_, axis=0)


def pool(ids_ref, table_ref, packed_ref, pooled_ref):
    samples = ids_ref.shape[1]
    active = table_ref.shape[0]
    lanes = 128
    fields = active // lanes
    places = lax.broadcasted_iota(jnp.int32, (lanes // 4, lanes), 0)
    chunks = samples // lanes

    def count(index, carry):
        packed_ref[index] = tally(ids_ref, pl.multiple_of(index * lanes, lanes), places)
        return carry

    lax.fori_loop(0, chunks, count, 0, unroll=UNROLL)

    def spread(words):
        turned = words.T
        return jnp.concatenate(
            [
                ((turned >> (8 * field)) & 255).astype(jnp.float32).astype(jnp.bfloat16)
                for field in range(fields)
            ],
            axis=1,
        )

    def look_up(index, carry):
        counts = jnp.concatenate(
            [spread(packed_ref[index * BATCH + part]) for part in range(BATCH)], axis=0
        )
        start = pl.multiple_of(index * BATCH * lanes, BATCH * lanes)
        pooled_ref[pl.ds(start, BATCH * lanes), :] = jnp.dot(
            counts, table_ref[...], preferred_element_type=jnp.float32
        )
        return carry

    lax.fori_loop(0, chunks // BATCH, look_up, 0)


def decode(exponent, fraction):
    return jnp.exp2(exponent.astype(jnp.float32)) * (fraction.astype(jnp.float32) / PARTS)


def encode(top):
    exponent = jnp.floor(jnp.log2(jnp.maximum(top, 1e-30))) + 1.0
    fraction = (top * jnp.exp2(-exponent) * PARTS).astype(jnp.int32) + 1
    return exponent.astype(jnp.int32), fraction


def kernel(
    ids_hbm,
    table_hbm,
    order_ref,
    first_hbm,
    second_hbm,
    head_hbm,
    inter_hbm,
    out_ref,
    ids_v,
    table_v,
    packed,
    pooled,
    permuted,
    xsend,
    xall,
    wall,
    total,
    cross,
    relay,
    final,
    outsum,
    second_v,
    outbox,
    inbox,
    head_v,
    inter_v,
    spread_hi,
    spread_lo,
    load_sem,
    first_sem,
    w_send,
    w_recv,
    r_send,
    r_recv,
    x_send,
    x_recv,
    c_send,
    c_recv,
    f_send,
    f_recv,
    o_send,
    o_recv,
    near_sem,
    far_sem,
    open_sem,
    towers,
):
    tower = lax.axis_index("tower")
    dev = lax.axis_index("dev")
    core = lax.rem(dev, CORES)
    chip = dev // CORES
    col = chip // RING
    row = lax.rem(chip, RING)
    chunks, _, tile = wall.shape
    emb = table_v.shape[1]
    block = permuted.shape[0]

    def along(step):
        return lax.rem(row + step, RING)

    def at_row(place):
        return {"dev": (col * RING + place) * CORES + core}

    partner = {"dev": dev + 1 - 2 * core}
    across = {"dev": ((1 - col) * RING + row) * CORES + core}

    mine = pl.ds(pl.multiple_of(row * emb, emb), emb)
    loads = [
        pltpu.make_async_copy(ids_hbm, ids_v, load_sem.at[0]),
        pltpu.make_async_copy(table_hbm, table_v, load_sem.at[1]),
        pltpu.make_async_copy(second_hbm, second_v, load_sem.at[2]),
        pltpu.make_async_copy(head_hbm, head_v, load_sem.at[3]),
        pltpu.make_async_copy(inter_hbm, inter_v, load_sem.at[4]),
    ]
    firsts = [
        pltpu.make_async_copy(
            first_hbm.at[:, pl.ds(n * tile, tile)], wall.at[n, mine, :], first_sem.at[n]
        )
        for n in range(chunks)
    ]
    loads[0].start()
    loads[1].start()
    for copy in firsts:
        copy.start()

    barrier = pltpu.get_barrier_semaphore()
    devices = CORES * RING * 2
    gate = dev == GATE
    peers = [at_row(along(step))["dev"] for step in range(1, RING)]
    peers += [partner["dev"], across["dev"]]
    near = jnp.int32(0)
    others = [other for other in range(devices) if other != GATE]
    for peer in peers:
        near = near + jnp.where(peer == GATE, 1, 0)

    @pl.when(jnp.logical_not(gate))
    def _():
        for peer in peers:

            @pl.when(peer != GATE)
            def _():
                pl.semaphore_signal(
                    barrier, inc=1, device_id={"dev": peer}, device_id_type=MESH
                )

        pl.semaphore_wait(barrier, len(peers) + 1 - near)

        @pl.when(near == 1)
        def _():
            pl.semaphore_signal(near_sem, inc=1, device_id={"dev": GATE}, device_id_type=MESH)

        @pl.when(near == 0)
        def _():
            pl.semaphore_signal(far_sem, inc=1, device_id={"dev": GATE}, device_id_type=MESH)

    @pl.when(gate)
    def _():
        for other in others:
            pl.semaphore_signal(barrier, inc=1, device_id={"dev": other}, device_id_type=MESH)
        pl.semaphore_wait(near_sem, len(peers))

    def gate_towers():
        pl.semaphore_wait(far_sem, devices - 1 - len(peers))
        for step in range(1, towers):
            pl.semaphore_signal(
                barrier,
                inc=1,
                device_id={"tower": lax.rem(tower + step, towers)},
                device_id_type=MESH,
            )

    def gate_open():
        pl.semaphore_wait(barrier, towers - 1)
        for other in others:
            pl.semaphore_signal(open_sem, inc=1, device_id={"dev": other}, device_id_type=MESH)

    for copy in firsts:
        copy.wait()

    steps = (3, 1, 2)

    def send_w(n, step):
        return pltpu.make_async_remote_copy(
            src_ref=wall.at[pl.ds(*SPANS[n]), mine, :],
            dst_ref=wall.at[pl.ds(*SPANS[n]), mine, :],
            send_sem=w_send.at[n, step],
            recv_sem=w_recv.at[n, row],
            device_id=at_row(along(step)),
            device_id_type=MESH,
        )

    def forward(n, half):
        source = along(3) if half == 0 else along(1)
        span = pl.ds(pl.multiple_of(source * emb + half * (emb // 2), emb // 2), emb // 2)
        return pltpu.make_async_remote_copy(
            src_ref=wall.at[pl.ds(*SPANS[n]), span, :],
            dst_ref=wall.at[pl.ds(*SPANS[n]), span, :],
            send_sem=r_send.at[n, half],
            recv_sem=r_recv.at[n, half],
            device_id=at_row(along(1) if half == 0 else along(3)),
            device_id_type=MESH,
        )

    def forwarded(n, half):
        source = along(2)
        span = pl.ds(pl.multiple_of(source * emb + half * (emb // 2), emb // 2), emb // 2)
        return pltpu.make_async_remote_copy(
            src_ref=wall.at[pl.ds(*SPANS[n]), span, :],
            dst_ref=wall.at[pl.ds(*SPANS[n]), span, :],
            send_sem=r_send.at[n, half],
            recv_sem=r_recv.at[n, half],
            device_id=partner,
            device_id_type=MESH,
        )

    def w_steps(n):
        return steps[:2] if n < RELAYED else steps

    def arrived_w(n, step):
        source = along(step)
        span = pl.ds(pl.multiple_of(source * emb, emb), emb)
        return pltpu.make_async_remote_copy(
            src_ref=wall.at[pl.ds(*SPANS[n]), span, :],
            dst_ref=wall.at[pl.ds(*SPANS[n]), span, :],
            send_sem=w_send.at[n, step],
            recv_sem=w_recv.at[n, source],
            device_id=partner,
            device_id_type=MESH,
        )

    def half_of(kind):
        part = 1 - core if kind == 1 else core
        return pl.ds(pl.multiple_of(part * block, block), block)

    def x_slots(kind, place, span):
        if kind == 0:
            return xsend.at[0, place], xall.at[0, :, span]
        return xsend.at[1, place, half_of(kind), :], xall.at[1, half_of(kind), span]

    def send_x(kind, step):
        source, target = x_slots(kind, along(step), mine)
        return pltpu.make_async_remote_copy(
            src_ref=source,
            dst_ref=target,
            send_sem=x_send.at[kind, step],
            recv_sem=x_recv.at[kind, row],
            device_id=at_row(along(step)),
            device_id_type=MESH,
        )

    def arrived_x(kind, step):
        place = along(step)
        span = pl.ds(pl.multiple_of(place * emb, emb), emb)
        source, target = x_slots(kind, place, span)
        return pltpu.make_async_remote_copy(
            src_ref=source,
            dst_ref=target,
            send_sem=x_send.at[kind, step],
            recv_sem=x_recv.at[kind, place],
            device_id=partner,
            device_id_type=MESH,
        )

    def permute_rows(kind, place, store):
        x = 1 - col if kind == 0 else col
        for c in ((0, 1), (1 - core,), (core,))[kind]:
            start = ((x * RING + place) * CORES + c) * block

            def group(index, carry):
                for q in range(16):
                    source = order_ref[start + index * 16 + q]
                    permuted[pl.ds(index * 16 + q, 1), :] = pooled[pl.ds(source, 1), :]
                return carry

            lax.fori_loop(0, block // 16, group, 0)
            part = pl.ds(c * block, block) if kind == 0 else half_of(kind)
            store(part, permuted[...].astype(jnp.bfloat16))

    def permute_send(kind):
        for step in steps:
            place = along(step)

            def keep(part, value):
                xsend[min(kind, 1), place, part, :] = value

            permute_rows(kind, place, keep)
            send_x(kind, step).start()

    def permute_own(kind):
        def keep(part, value):
            xall[min(kind, 1), part, mine] = value

        permute_rows(kind, row, keep)

    for n in range(EARLY):
        for step in w_steps(n):
            send_w(n, step).start()
    pl.when(gate)(gate_towers)
    loads[0].wait()
    loads[1].wait()
    pool(ids_v, table_v, packed, pooled)
    for copy in loads[2:]:
        copy.start()
    def relay_rows(n):
        for half, near_step in ((0, 3), (1, 1)):
            arrived_w(n, near_step).wait_recv()
            forward(n, half).start()

    for n in range(AHEAD):
        relay_rows(n)
    permute_send(0)
    for n in range(AHEAD, RELAYED):
        relay_rows(n)
    for n in range(EARLY, len(SPANS)):
        for step in w_steps(n):
            send_w(n, step).start()
    permute_own(0)
    permute_send(1)
    permute_send(2)
    permute_own(1)
    permute_own(2)
    pl.when(gate)(gate_open)

    loads[4].wait()
    pairs = inter_v.shape[0]

    def widen(index, carry):
        start = pl.multiple_of(index * 16, 16)
        some = inter_v[pl.ds(start, 16), :]
        wide = jnp.broadcast_to(some[:, None, :], (16, 8, some.shape[1])).reshape(
            128, some.shape[1]
        )
        high = wide.astype(jnp.bfloat16)
        low = (wide - high.astype(jnp.float32)).astype(jnp.bfloat16)
        target = pl.multiple_of(index * 128, 128)
        spread_hi[pl.ds(target, 128), :] = high
        spread_lo[pl.ds(target, 128), :] = low
        return carry

    lax.fori_loop(0, pairs // 16, widen, 0)
    loads[2].wait()
    loads[3].wait()

    def cross_copy(kind, g):
        return pltpu.make_async_remote_copy(
            src_ref=total.at[kind, pl.ds(*GROUPS[g]), 1 - core],
            dst_ref=cross.at[kind, pl.ds(*GROUPS[g])],
            send_sem=c_send.at[kind, g],
            recv_sem=c_recv.at[kind, g],
            device_id=partner,
            device_id_type=MESH,
        )

    def final_copy(g):
        return pltpu.make_async_remote_copy(
            src_ref=relay.at[pl.ds(*GROUPS[g])],
            dst_ref=final.at[pl.ds(*GROUPS[g])],
            send_sem=f_send.at[g],
            recv_sem=f_recv.at[g],
            device_id=across,
            device_id_type=MESH,
        )

    def tiles(g):
        return range(GROUPS[g][0], sum(GROUPS[g]))

    def arrived_span(g):
        for index, (begin, _) in enumerate(SPANS):
            if begin in tiles(g):
                if index < RELAYED:
                    for half in range(2):
                        forwarded(index, half).wait_recv()
                else:
                    for step in steps:
                        arrived_w(index, step).wait_recv()

    def first_layer(kind, g):
        for n in tiles(g):
            if kind == 0:
                part = jnp.dot(xall[0], wall[n], preferred_element_type=jnp.float32)
                total[0, n] = part.reshape(CORES, block, tile)
            else:
                total[1, n, 1 - core if kind == 1 else core] = jnp.dot(
                    xall[1, half_of(kind), :], wall[n], preferred_element_type=jnp.float32
                )
        if kind < 2:
            cross_copy(kind, g).start()

    def add_cores(g):
        cross_copy(0, g).wait_recv()
        for n in tiles(g):
            part = total[0, n, core] + cross[0, n]
            exponent, fraction = encode(jnp.max(jnp.abs(part), axis=0, keepdims=True))
            steps_up = part * (LEVELS / decode(exponent, fraction)) + (LEVELS + 1.5)
            relay[n, :block, :] = (steps_up.astype(jnp.int32) - (LEVELS + 1)).astype(jnp.int16)
            line = lax.broadcasted_iota(jnp.int32, (16, tile), 0)
            code = jnp.where(line == 0, exponent, jnp.where(line == 1, fraction, 0))
            relay[n, block:, :] = code.astype(jnp.int16)
        final_copy(g).start()

    def second_layer(g):
        cross_copy(1, g).wait_recv()
        final_copy(g).wait_recv()
        hidden = []
        for n in tiles(g):
            code = final[n, block:, :].astype(jnp.int32)
            unit = decode(code[0:1], code[1:2]) * (1.0 / LEVELS)
            other = final[n, :block, :].astype(jnp.float32) * unit
            preact = total[1, n, core] + cross[1, n] + other
            hidden.append(jnp.maximum(preact, 0.0).astype(jnp.bfloat16))
        begin, count = GROUPS[g]
        part = jnp.dot(
            jnp.concatenate(hidden, axis=1),
            second_v[begin * tile : (begin + count) * tile, :],
            preferred_element_type=jnp.float32,
        )
        if g == 0:
            outsum[...] = part
        else:
            outsum[...] += part

    groups = len(GROUPS)
    for step in steps:
        arrived_x(0, step).wait_recv()
    for g in range(groups + 1):
        if g < groups:
            arrived_span(g)
            first_layer(0, g)
        if g >= 1:
            add_cores(g - 1)
    for step in steps:
        arrived_x(1, step).wait_recv()
    for g in range(groups):
        first_layer(1, g)
    for step in steps:
        arrived_x(2, step).wait_recv()
    for g in range(groups):
        first_layer(2, g)
    for g in range(groups):
        second_layer(g)

    share = outbox.shape[1]
    outbox[...] = outsum[...].reshape(towers, share, outsum.shape[1]).astype(jnp.bfloat16)

    depth = towers // 2

    def other_tower(dz, dx):
        return lax.rem(tower // 2 + dz, depth) * 2 + lax.rem(lax.rem(tower, 2) + dx, 2)

    def send_o(dz, dx):
        peer = other_tower(dz, dx)
        return pltpu.make_async_remote_copy(
            src_ref=outbox.at[peer],
            dst_ref=inbox.at[tower],
            send_sem=o_send.at[dz * 2 + dx],
            recv_sem=o_recv.at[tower],
            device_id={"tower": peer},
            device_id_type=MESH,
        )

    @pl.when(jnp.logical_not(gate))
    def _():
        pl.semaphore_wait(open_sem, 1)

    for dz, dx in reversed(HOPS):
        send_o(dz, dx).start()
    inbox[tower] = outbox[tower]

    def head_part(source):
        return jnp.dot(inbox[source], head_v[source], preferred_element_type=jnp.float32)

    head = head_part(tower)
    for dz, dx in HOPS:
        source = other_tower(dz, dx)
        pltpu.make_async_remote_copy(
            src_ref=outbox.at[source],
            dst_ref=inbox.at[source],
            send_sem=o_send.at[dz * 2 + dx],
            recv_sem=o_recv.at[source],
            device_id=partner,
            device_id_type=MESH,
        ).wait_recv()
        head = head + head_part(source)

    zwidth = inbox.shape[2]
    stacked = (
        inbox[...].astype(jnp.float32).reshape(towers * share, zwidth).astype(jnp.bfloat16)
    )
    gram = lax.dot_general(
        stacked, stacked, (((1,), (1,)), ((), ())), preferred_element_type=jnp.float32
    )
    left = lax.rem(lax.broadcasted_iota(jnp.int32, gram.shape, 0), share)
    right = lax.rem(lax.broadcasted_iota(jnp.int32, gram.shape, 1), share)
    gram = jnp.where(left == right, gram / math.sqrt(zwidth), 0.0)
    flat = jnp.concatenate(
        [gram[t * share : (t + 1) * share, :] for t in range(towers)], axis=1
    )
    flat_hi = flat.astype(jnp.bfloat16)
    rest = flat - flat_hi.astype(jnp.float32)
    both = jnp.concatenate([flat_hi.astype(jnp.float32), rest], axis=0).astype(jnp.bfloat16)
    twice = jnp.dot(both, spread_hi[...], preferred_element_type=jnp.float32)
    interact = twice[:share] + twice[share:]
    interact += jnp.dot(flat_hi, spread_lo[...], preferred_element_type=jnp.float32)
    out_ref[...] = head + interact

    for step in steps:
        send_x(0, step).wait_send()
        send_x(1, step).wait_send()
        send_x(2, step).wait_send()
        for n in range(len(SPANS)):
            if step in w_steps(n):
                send_w(n, step).wait_send()
    for n in range(RELAYED):
        for half in range(2):
            forward(n, half).wait_send()
    for g in range(groups):
        cross_copy(0, g).wait_send()
        cross_copy(1, g).wait_send()
        final_copy(g).wait_send()
    for dz, dx in HOPS:
        send_o(dz, dx).wait_send()


def on_device(ids, tables, order, w_first, w_second, w_head, w_interact):
    towers = lax.axis_size("tower")
    devices = lax.axis_size("dev")
    samples, bag = ids.shape[2:]
    active, emb = tables.shape[2:]
    hidden = w_first.shape[2]
    zwidth = w_second.shape[2]
    heads = w_head.shape[1]
    block = samples // devices
    share = block // towers
    quarter = samples // RING
    pairs = w_interact.shape[0]
    tile = hidden // CHUNKS
    vmem = pltpu.VMEM
    dma = pltpu.SemaphoreType.DMA
    anywhere = pl.BlockSpec(memory_space=pltpu.HBM)
    scores = pl.pallas_call(
        functools.partial(kernel, towers=towers),
        out_shape=jax.ShapeDtypeStruct((share, heads), jnp.float32),
        in_specs=[
            anywhere,
            anywhere,
            pl.BlockSpec(memory_space=pltpu.SMEM),
            anywhere,
            anywhere,
            anywhere,
            anywhere,
        ],
        out_specs=pl.BlockSpec(memory_space=vmem),
        scratch_shapes=[
            vmem((bag, samples), jnp.int32),
            vmem((active, emb), jnp.bfloat16),
            vmem((samples // 128, 128, 128), jnp.int32),
            vmem((samples, emb), jnp.float32),
            vmem((block, emb), jnp.float32),
            vmem((2, RING, quarter // 2, emb), jnp.bfloat16),
            vmem((2, quarter // 2, RING * emb), jnp.bfloat16),
            vmem((CHUNKS, RING * emb, tile), jnp.bfloat16),
            vmem((2, CHUNKS, CORES, block, tile), jnp.float32),
            vmem((2, CHUNKS, block, tile), jnp.float32),
            vmem((CHUNKS, block + 16, tile), jnp.int16),
            vmem((CHUNKS, block + 16, tile), jnp.int16),
            vmem((block, zwidth), jnp.float32),
            vmem((hidden, zwidth), jnp.bfloat16),
            vmem((towers, share, zwidth), jnp.bfloat16),
            vmem((towers, share, zwidth), jnp.bfloat16),
            vmem((towers, zwidth, heads), jnp.bfloat16),
            vmem((pairs, heads), jnp.float32),
            vmem((pairs * share, heads), jnp.bfloat16),
            vmem((pairs * share, heads), jnp.bfloat16),
            dma((5,)),
            dma((CHUNKS,)),
            dma((len(SPANS), RING)),
            dma((len(SPANS), RING)),
            dma((len(SPANS), 2)),
            dma((len(SPANS), 2)),
            dma((3, RING)),
            dma((3, RING)),
            dma((2, CHUNKS)),
            dma((2, CHUNKS)),
            dma((CHUNKS,)),
            dma((CHUNKS,)),
            dma((towers,)),
            dma((towers,)),
            pltpu.SemaphoreType.REGULAR,
            pltpu.SemaphoreType.REGULAR,
            pltpu.SemaphoreType.REGULAR,
        ],
        compiler_params=pltpu.CompilerParams(
            collective_id=0, has_side_effects=True, vmem_limit_bytes=32 * 1024 * 1024
        ),
    )(
        *(
            pltpu.with_memory_space_constraint(value, pltpu.HBM)
            for value in (
                jnp.swapaxes(ids[0, 0], 0, 1),
                tables[0, 0],
                order,
                w_first[0],
                w_second[0],
                w_head.reshape(towers, zwidth, heads),
                w_interact,
            )
        ),
    )
    return scores[None]


def solution(mesh):
    return jax.shard_map(
        on_device,
        mesh=mesh,
        in_specs=(
            P("tower", "dev", None, None),
            P("tower", "dev", None, None),
            P(),
            P("tower", "dev", None),
            P("tower", None, None),
            P(),
            P(),
        ),
        out_specs=P("dev", "tower", None),
        check_vma=False,
    )
```

```python
import functools
import math

import jax
import jax.numpy as jnp
from jax import lax
from jax.experimental import pallas as pl
from jax.experimental.pallas import tpu as pltpu
from jax.sharding import PartitionSpec as P

MESH = pl.DeviceIdType.MESH
RING = 4
CORES = 2
CHUNKS = 8
BATCH = 8
UNROLL = 1
SPANS = ((0, 3), (3, 3), (6, 2))
GROUPS = ((0, 3), (3, 3), (6, 2))
EARLY = 2
RELAYED = 2
AHEAD = 0
GATE = 1
LEVELS = 32752
PARTS = 16384
HOPS = (
    (1, 0),
    (7, 0),
    (2, 0),
    (6, 0),
    (0, 1),
    (1, 1),
    (7, 1),
    (3, 0),
    (5, 0),
    (2, 1),
    (6, 1),
    (4, 0),
    (3, 1),
    (5, 1),
    (4, 1),
)


def fold(words, shift, mask):
    return words & mask, lax.shift_right_logical(words, shift) & mask


def tally(ids_ref, start, places):
    bag = ids_ref.shape[0]
    lanes = places.shape[1]
    low_bits = places.shape[0]
    shift = low_bits.bit_length() - 1
    rows = [ids_ref[pl.ds(8 * g, 8), pl.ds(start, lanes)] for g in range(bag // 8)]
    lows = [row & (low_bits - 1) for row in rows]
    units = [jnp.left_shift(1, (row >> shift) << 1) for row in rows]

    def mark(j):
        low = lows[j // 8][j % 8 : j % 8 + 1, :]
        unit = units[j // 8][j % 8 : j % 8 + 1, :]
        return jnp.where(low == places, unit, 0)

    def add(left, right):
        return right if left is None else [a + b for a, b in zip(left, right)]

    nibbles = None
    bytes_ = None
    held = 0
    for start_j in range(0, bag, 3):
        group = range(start_j, min(start_j + 3, bag))
        words = mark(group[0])
        for j in group[1:]:
            words = words + mark(j)
        nibbles = add(nibbles, fold(words, 2, 0x33333333))
        held += len(group)
        if held > 12 or group[-1] == bag - 1:
            even = fold(nibbles[0], 4, 0x0F0F0F0F)
            odd = fold(nibbles[1], 4, 0x0F0F0F0F)
            bytes_ = add(bytes_, [even[0], odd[0], even[1], odd[1]])
            nibbles = None
            held = 0
    return jnp.concatenate(bytes_, axis=0)


def pool(ids_ref, table_ref, packed_ref, pooled_ref):
    samples = ids_ref.shape[1]
    active = table_ref.shape[0]
    lanes = 128
    fields = active // lanes
    places = lax.broadcasted_iota(jnp.int32, (lanes // 4, lanes), 0)
    chunks = samples // lanes

    def count(index, carry):
        packed_ref[index] = tally(ids_ref, pl.multiple_of(index * lanes, lanes), places)
        return carry

    lax.fori_loop(0, chunks, count, 0, unroll=UNROLL)

    def spread(words):
        turned = words.T
        return jnp.concatenate(
            [
                ((turned >> (8 * field)) & 255).astype(jnp.float32).astype(jnp.bfloat16)
                for field in range(fields)
            ],
            axis=1,
        )

    def look_up(index, carry):
        counts = jnp.concatenate(
            [spread(packed_ref[index * BATCH + part]) for part in range(BATCH)], axis=0
        )
        start = pl.multiple_of(index * BATCH * lanes, BATCH * lanes)
        pooled_ref[pl.ds(start, BATCH * lanes), :] = jnp.dot(
            counts, table_ref[...], preferred_element_type=jnp.float32
        )
        return carry

    lax.fori_loop(0, chunks // BATCH, look_up, 0)


def decode(exponent, fraction):
    return jnp.exp2(exponent.astype(jnp.float32)) * (fraction.astype(jnp.float32) / PARTS)


def encode(top):
    exponent = jnp.floor(jnp.log2(jnp.maximum(top, 1e-30))) + 1.0
    fraction = (top * jnp.exp2(-exponent) * PARTS).astype(jnp.int32) + 1
    return exponent.astype(jnp.int32), fraction


def kernel(
    ids_hbm,
    table_hbm,
    order_ref,
    first_hbm,
    second_hbm,
    head_hbm,
    inter_hbm,
    out_ref,
    ids_v,
    table_v,
    packed,
    pooled,
    permuted,
    xsend,
    xall,
    wall,
    total,
    cross,
    relay,
    final,
    outsum,
    second_v,
    outbox,
    inbox,
    head_v,
    inter_v,
    spread_hi,
    spread_lo,
    load_sem,
    first_sem,
    w_send,
    w_recv,
    r_send,
    r_recv,
    x_send,
    x_recv,
    c_send,
    c_recv,
    f_send,
    f_recv,
    o_send,
    o_recv,
    near_sem,
    far_sem,
    open_sem,
    towers,
):
    tower = lax.axis_index("tower")
    dev = lax.axis_index("dev")
    core = lax.rem(dev, CORES)
    chip = dev // CORES
    col = chip // RING
    row = lax.rem(chip, RING)
    chunks, _, tile = wall.shape
    emb = table_v.shape[1]
    block = permuted.shape[0]

    def along(step):
        return lax.rem(row + step, RING)

    def at_row(place):
        return {"dev": (col * RING + place) * CORES + core}

    partner = {"dev": dev + 1 - 2 * core}
    across = {"dev": ((1 - col) * RING + row) * CORES + core}

    mine = pl.ds(pl.multiple_of(row * emb, emb), emb)
    loads = [
        pltpu.make_async_copy(ids_hbm, ids_v, load_sem.at[0]),
        pltpu.make_async_copy(table_hbm, table_v, load_sem.at[1]),
        pltpu.make_async_copy(second_hbm, second_v, load_sem.at[2]),
        pltpu.make_async_copy(head_hbm, head_v, load_sem.at[3]),
        pltpu.make_async_copy(inter_hbm, inter_v, load_sem.at[4]),
    ]
    firsts = [
        pltpu.make_async_copy(
            first_hbm.at[:, pl.ds(n * tile, tile)], wall.at[n, mine, :], first_sem.at[n]
        )
        for n in range(chunks)
    ]
    loads[0].start()
    loads[1].start()
    for copy in firsts:
        copy.start()

    barrier = pltpu.get_barrier_semaphore()
    devices = CORES * RING * 2
    gate = dev == GATE
    peers = [at_row(along(step))["dev"] for step in range(1, RING)]
    peers += [partner["dev"], across["dev"]]
    near = jnp.int32(0)
    others = [other for other in range(devices) if other != GATE]
    for peer in peers:
        near = near + jnp.where(peer == GATE, 1, 0)

    @pl.when(jnp.logical_not(gate))
    def _():
        for peer in peers:

            @pl.when(peer != GATE)
            def _():
                pl.semaphore_signal(
                    barrier, inc=1, device_id={"dev": peer}, device_id_type=MESH
                )

        pl.semaphore_wait(barrier, len(peers) + 1 - near)

        @pl.when(near == 1)
        def _():
            pl.semaphore_signal(near_sem, inc=1, device_id={"dev": GATE}, device_id_type=MESH)

        @pl.when(near == 0)
        def _():
            pl.semaphore_signal(far_sem, inc=1, device_id={"dev": GATE}, device_id_type=MESH)

    @pl.when(gate)
    def _():
        for other in others:
            pl.semaphore_signal(barrier, inc=1, device_id={"dev": other}, device_id_type=MESH)
        pl.semaphore_wait(near_sem, len(peers))

    def gate_towers():
        pl.semaphore_wait(far_sem, devices - 1 - len(peers))
        for step in range(1, towers):
            pl.semaphore_signal(
                barrier,
                inc=1,
                device_id={"tower": lax.rem(tower + step, towers)},
                device_id_type=MESH,
            )

    def gate_open():
        pl.semaphore_wait(barrier, towers - 1)
        for other in others:
            pl.semaphore_signal(open_sem, inc=1, device_id={"dev": other}, device_id_type=MESH)

    for copy in firsts:
        copy.wait()

    steps = (3, 1, 2)

    def send_w(n, step):
        return pltpu.make_async_remote_copy(
            src_ref=wall.at[pl.ds(*SPANS[n]), mine, :],
            dst_ref=wall.at[pl.ds(*SPANS[n]), mine, :],
            send_sem=w_send.at[n, step],
            recv_sem=w_recv.at[n, row],
            device_id=at_row(along(step)),
            device_id_type=MESH,
        )

    def forward(n, half):
        source = along(3) if half == 0 else along(1)
        span = pl.ds(pl.multiple_of(source * emb + half * (emb // 2), emb // 2), emb // 2)
        return pltpu.make_async_remote_copy(
            src_ref=wall.at[pl.ds(*SPANS[n]), span, :],
            dst_ref=wall.at[pl.ds(*SPANS[n]), span, :],
            send_sem=r_send.at[n, half],
            recv_sem=r_recv.at[n, half],
            device_id=at_row(along(1) if half == 0 else along(3)),
            device_id_type=MESH,
        )

    def forwarded(n, half):
        source = along(2)
        span = pl.ds(pl.multiple_of(source * emb + half * (emb // 2), emb // 2), emb // 2)
        return pltpu.make_async_remote_copy(
            src_ref=wall.at[pl.ds(*SPANS[n]), span, :],
            dst_ref=wall.at[pl.ds(*SPANS[n]), span, :],
            send_sem=r_send.at[n, half],
            recv_sem=r_recv.at[n, half],
            device_id=partner,
            device_id_type=MESH,
        )

    def w_steps(n):
        return steps[:2] if n < RELAYED else steps

    def arrived_w(n, step):
        source = along(step)
        span = pl.ds(pl.multiple_of(source * emb, emb), emb)
        return pltpu.make_async_remote_copy(
            src_ref=wall.at[pl.ds(*SPANS[n]), span, :],
            dst_ref=wall.at[pl.ds(*SPANS[n]), span, :],
            send_sem=w_send.at[n, step],
            recv_sem=w_recv.at[n, source],
            device_id=partner,
            device_id_type=MESH,
        )

    def half_of(kind):
        part = 1 - core if kind == 1 else core
        return pl.ds(pl.multiple_of(part * block, block), block)

    def x_slots(kind, place, span):
        if kind == 0:
            return xsend.at[0, place], xall.at[0, :, span]
        return xsend.at[1, place, half_of(kind), :], xall.at[1, half_of(kind), span]

    def send_x(kind, step):
        source, target = x_slots(kind, along(step), mine)
        return pltpu.make_async_remote_copy(
            src_ref=source,
            dst_ref=target,
            send_sem=x_send.at[kind, step],
            recv_sem=x_recv.at[kind, row],
            device_id=at_row(along(step)),
            device_id_type=MESH,
        )

    def arrived_x(kind, step):
        place = along(step)
        span = pl.ds(pl.multiple_of(place * emb, emb), emb)
        source, target = x_slots(kind, place, span)
        return pltpu.make_async_remote_copy(
            src_ref=source,
            dst_ref=target,
            send_sem=x_send.at[kind, step],
            recv_sem=x_recv.at[kind, place],
            device_id=partner,
            device_id_type=MESH,
        )

    def permute_rows(kind, place, store):
        x = 1 - col if kind == 0 else col
        for c in ((0, 1), (1 - core,), (core,))[kind]:
            start = ((x * RING + place) * CORES + c) * block

            def group(index, carry):
                for q in range(16):
                    source = order_ref[start + index * 16 + q]
                    permuted[pl.ds(index * 16 + q, 1), :] = pooled[pl.ds(source, 1), :]
                return carry

            lax.fori_loop(0, block // 16, group, 0)
            part = pl.ds(c * block, block) if kind == 0 else half_of(kind)
            store(part, permuted[...].astype(jnp.bfloat16))

    def permute_send(kind):
        for step in steps:
            place = along(step)

            def keep(part, value):
                xsend[min(kind, 1), place, part, :] = value

            permute_rows(kind, place, keep)
            send_x(kind, step).start()

    def permute_own(kind):
        def keep(part, value):
            xall[min(kind, 1), part, mine] = value

        permute_rows(kind, row, keep)

    for n in range(EARLY):
        for step in w_steps(n):
            send_w(n, step).start()
    pl.when(gate)(gate_towers)
    loads[0].wait()
    loads[1].wait()
    pool(ids_v, table_v, packed, pooled)
    for copy in loads[2:]:
        copy.start()
    def relay_rows(n):
        for half, near_step in ((0, 3), (1, 1)):
            arrived_w(n, near_step).wait_recv()
            forward(n, half).start()

    for n in range(AHEAD):
        relay_rows(n)
    permute_send(0)
    for n in range(AHEAD, RELAYED):
        relay_rows(n)
    for n in range(EARLY, len(SPANS)):
        for step in w_steps(n):
            send_w(n, step).start()
    permute_own(0)
    permute_send(1)
    permute_send(2)
    permute_own(1)
    permute_own(2)
    pl.when(gate)(gate_open)

    loads[4].wait()
    pairs = inter_v.shape[0]

    def widen(index, carry):
        start = pl.multiple_of(index * 16, 16)
        some = inter_v[pl.ds(start, 16), :]
        wide = jnp.broadcast_to(some[:, None, :], (16, 8, some.shape[1])).reshape(
            128, some.shape[1]
        )
        high = wide.astype(jnp.bfloat16)
        low = (wide - high.astype(jnp.float32)).astype(jnp.bfloat16)
        target = pl.multiple_of(index * 128, 128)
        spread_hi[pl.ds(target, 128), :] = high
        spread_lo[pl.ds(target, 128), :] = low
        return carry

    lax.fori_loop(0, pairs // 16, widen, 0)
    loads[2].wait()
    loads[3].wait()

    def cross_copy(kind, g):
        return pltpu.make_async_remote_copy(
            src_ref=total.at[kind, pl.ds(*GROUPS[g]), 1 - core],
            dst_ref=cross.at[kind, pl.ds(*GROUPS[g])],
            send_sem=c_send.at[kind, g],
            recv_sem=c_recv.at[kind, g],
            device_id=partner,
            device_id_type=MESH,
        )

    def final_copy(g):
        return pltpu.make_async_remote_copy(
            src_ref=relay.at[pl.ds(*GROUPS[g])],
            dst_ref=final.at[pl.ds(*GROUPS[g])],
            send_sem=f_send.at[g],
            recv_sem=f_recv.at[g],
            device_id=across,
            device_id_type=MESH,
        )

    def tiles(g):
        return range(GROUPS[g][0], sum(GROUPS[g]))

    def arrived_span(g):
        for index, (begin, _) in enumerate(SPANS):
            if begin in tiles(g):
                if index < RELAYED:
                    for half in range(2):
                        forwarded(index, half).wait_recv()
                else:
                    for step in steps:
                        arrived_w(index, step).wait_recv()

    def first_layer(kind, g):
        for n in tiles(g):
            if kind == 0:
                part = jnp.dot(xall[0], wall[n], preferred_element_type=jnp.float32)
                total[0, n] = part.reshape(CORES, block, tile)
            else:
                total[1, n, 1 - core if kind == 1 else core] = jnp.dot(
                    xall[1, half_of(kind), :], wall[n], preferred_element_type=jnp.float32
                )
        if kind < 2:
            cross_copy(kind, g).start()

    def add_cores(g):
        cross_copy(0, g).wait_recv()
        for n in tiles(g):
            part = total[0, n, core] + cross[0, n]
            exponent, fraction = encode(jnp.max(jnp.abs(part), axis=0, keepdims=True))
            steps_up = part * (LEVELS / decode(exponent, fraction)) + (LEVELS + 1.5)
            relay[n, :block, :] = (steps_up.astype(jnp.int32) - (LEVELS + 1)).astype(jnp.int16)
            line = lax.broadcasted_iota(jnp.int32, (16, tile), 0)
            code = jnp.where(line == 0, exponent, jnp.where(line == 1, fraction, 0))
            relay[n, block:, :] = code.astype(jnp.int16)
        final_copy(g).start()

    def second_layer(g):
        cross_copy(1, g).wait_recv()
        final_copy(g).wait_recv()
        hidden = []
        for n in tiles(g):
            code = final[n, block:, :].astype(jnp.int32)
            unit = decode(code[0:1], code[1:2]) * (1.0 / LEVELS)
            other = final[n, :block, :].astype(jnp.float32) * unit
            preact = total[1, n, core] + cross[1, n] + other
            hidden.append(jnp.maximum(preact, 0.0).astype(jnp.bfloat16))
        begin, count = GROUPS[g]
        part = jnp.dot(
            jnp.concatenate(hidden, axis=1),
            second_v[begin * tile : (begin + count) * tile, :],
            preferred_element_type=jnp.float32,
        )
        if g == 0:
            outsum[...] = part
        else:
            outsum[...] += part

    groups = len(GROUPS)
    for step in steps:
        arrived_x(0, step).wait_recv()
    for g in range(groups):
        arrived_span(g)
        first_layer(0, g)
        add_cores(g)
    for step in steps:
        arrived_x(1, step).wait_recv()
    for g in range(groups):
        first_layer(1, g)
    for step in steps:
        arrived_x(2, step).wait_recv()
    for g in range(groups):
        first_layer(2, g)
    for g in range(groups):
        second_layer(g)

    share = outbox.shape[1]
    outbox[...] = outsum[...].reshape(towers, share, outsum.shape[1]).astype(jnp.bfloat16)

    depth = towers // 2

    def other_tower(dz, dx):
        return lax.rem(tower // 2 + dz, depth) * 2 + lax.rem(lax.rem(tower, 2) + dx, 2)

    def send_o(dz, dx):
        peer = other_tower(dz, dx)
        return pltpu.make_async_remote_copy(
            src_ref=outbox.at[peer],
            dst_ref=inbox.at[tower],
            send_sem=o_send.at[dz * 2 + dx],
            recv_sem=o_recv.at[tower],
            device_id={"tower": peer},
            device_id_type=MESH,
        )

    @pl.when(jnp.logical_not(gate))
    def _():
        pl.semaphore_wait(open_sem, 1)

    for dz, dx in reversed(HOPS):
        send_o(dz, dx).start()
    inbox[tower] = outbox[tower]

    def head_part(source):
        return jnp.dot(inbox[source], head_v[source], preferred_element_type=jnp.float32)

    head = head_part(tower)
    for dz, dx in HOPS:
        source = other_tower(dz, dx)
        pltpu.make_async_remote_copy(
            src_ref=outbox.at[source],
            dst_ref=inbox.at[source],
            send_sem=o_send.at[dz * 2 + dx],
            recv_sem=o_recv.at[source],
            device_id=partner,
            device_id_type=MESH,
        ).wait_recv()
        head = head + head_part(source)

    zwidth = inbox.shape[2]
    stacked = (
        inbox[...].astype(jnp.float32).reshape(towers * share, zwidth).astype(jnp.bfloat16)
    )
    gram = lax.dot_general(
        stacked, stacked, (((1,), (1,)), ((), ())), preferred_element_type=jnp.float32
    )
    left = lax.rem(lax.broadcasted_iota(jnp.int32, gram.shape, 0), share)
    right = lax.rem(lax.broadcasted_iota(jnp.int32, gram.shape, 1), share)
    gram = jnp.where(left == right, gram / math.sqrt(zwidth), 0.0)
    flat = jnp.concatenate(
        [gram[t * share : (t + 1) * share, :] for t in range(towers)], axis=1
    )
    flat_hi = flat.astype(jnp.bfloat16)
    rest = flat - flat_hi.astype(jnp.float32)
    both = jnp.concatenate([flat_hi.astype(jnp.float32), rest], axis=0).astype(jnp.bfloat16)
    twice = jnp.dot(both, spread_hi[...], preferred_element_type=jnp.float32)
    interact = twice[:share] + twice[share:]
    interact += jnp.dot(flat_hi, spread_lo[...], preferred_element_type=jnp.float32)
    out_ref[...] = head + interact

    for step in steps:
        send_x(0, step).wait_send()
        send_x(1, step).wait_send()
        send_x(2, step).wait_send()
        for n in range(len(SPANS)):
            if step in w_steps(n):
                send_w(n, step).wait_send()
    for n in range(RELAYED):
        for half in range(2):
            forward(n, half).wait_send()
    for g in range(groups):
        cross_copy(0, g).wait_send()
        cross_copy(1, g).wait_send()
        final_copy(g).wait_send()
    for dz, dx in HOPS:
        send_o(dz, dx).wait_send()


def on_device(ids, tables, order, w_first, w_second, w_head, w_interact):
    towers = lax.axis_size("tower")
    devices = lax.axis_size("dev")
    samples, bag = ids.shape[2:]
    active, emb = tables.shape[2:]
    hidden = w_first.shape[2]
    zwidth = w_second.shape[2]
    heads = w_head.shape[1]
    block = samples // devices
    share = block // towers
    quarter = samples // RING
    pairs = w_interact.shape[0]
    tile = hidden // CHUNKS
    vmem = pltpu.VMEM
    dma = pltpu.SemaphoreType.DMA
    anywhere = pl.BlockSpec(memory_space=pltpu.HBM)
    scores = pl.pallas_call(
        functools.partial(kernel, towers=towers),
        out_shape=jax.ShapeDtypeStruct((share, heads), jnp.float32),
        in_specs=[
            anywhere,
            anywhere,
            pl.BlockSpec(memory_space=pltpu.SMEM),
            anywhere,
            anywhere,
            anywhere,
            anywhere,
        ],
        out_specs=pl.BlockSpec(memory_space=vmem),
        scratch_shapes=[
            vmem((bag, samples), jnp.int32),
            vmem((active, emb), jnp.bfloat16),
            vmem((samples // 128, 128, 128), jnp.int32),
            vmem((samples, emb), jnp.float32),
            vmem((block, emb), jnp.float32),
            vmem((2, RING, quarter // 2, emb), jnp.bfloat16),
            vmem((2, quarter // 2, RING * emb), jnp.bfloat16),
            vmem((CHUNKS, RING * emb, tile), jnp.bfloat16),
            vmem((2, CHUNKS, CORES, block, tile), jnp.float32),
            vmem((2, CHUNKS, block, tile), jnp.float32),
            vmem((CHUNKS, block + 16, tile), jnp.int16),
            vmem((CHUNKS, block + 16, tile), jnp.int16),
            vmem((block, zwidth), jnp.float32),
            vmem((hidden, zwidth), jnp.bfloat16),
            vmem((towers, share, zwidth), jnp.bfloat16),
            vmem((towers, share, zwidth), jnp.bfloat16),
            vmem((towers, zwidth, heads), jnp.bfloat16),
            vmem((pairs, heads), jnp.float32),
            vmem((pairs * share, heads), jnp.bfloat16),
            vmem((pairs * share, heads), jnp.bfloat16),
            dma((5,)),
            dma((CHUNKS,)),
            dma((len(SPANS), RING)),
            dma((len(SPANS), RING)),
            dma((len(SPANS), 2)),
            dma((len(SPANS), 2)),
            dma((3, RING)),
            dma((3, RING)),
            dma((2, CHUNKS)),
            dma((2, CHUNKS)),
            dma((CHUNKS,)),
            dma((CHUNKS,)),
            dma((towers,)),
            dma((towers,)),
            pltpu.SemaphoreType.REGULAR,
            pltpu.SemaphoreType.REGULAR,
            pltpu.SemaphoreType.REGULAR,
        ],
        compiler_params=pltpu.CompilerParams(
            collective_id=0, has_side_effects=True, vmem_limit_bytes=32 * 1024 * 1024
        ),
    )(
        *(
            pltpu.with_memory_space_constraint(value, pltpu.HBM)
            for value in (
                jnp.swapaxes(ids[0, 0], 0, 1),
                tables[0, 0],
                order,
                w_first[0],
                w_second[0],
                w_head.reshape(towers, zwidth, heads),
                w_interact,
            )
        ),
    )
    return scores[None]


def solution(mesh):
    return jax.shard_map(
        on_device,
        mesh=mesh,
        in_specs=(
            P("tower", "dev", None, None),
            P("tower", "dev", None, None),
            P(),
            P("tower", "dev", None),
            P("tower", None, None),
            P(),
            P(),
        ),
        out_specs=P("dev", "tower", None),
        check_vma=False,
    )
```

```python
import functools
import math

import jax
import jax.numpy as jnp
from jax import lax
from jax.experimental import pallas as pl
from jax.experimental.pallas import tpu as pltpu
from jax.sharding import PartitionSpec as P

MESH = pl.DeviceIdType.MESH
RING = 4
CORES = 2
CHUNKS = 8
BATCH = 8
UNROLL = 1
SPANS = ((0, 3), (3, 3), (6, 2))
GROUPS = ((0, 3), (3, 3), (6, 1), (7, 1))
EARLY = 2
RELAYED = 2
AHEAD = 0
GATE = 1
LEVELS = 32752
PARTS = 16384
HOPS = (
    (1, 0),
    (7, 0),
    (2, 0),
    (6, 0),
    (0, 1),
    (1, 1),
    (7, 1),
    (3, 0),
    (5, 0),
    (2, 1),
    (6, 1),
    (4, 0),
    (3, 1),
    (5, 1),
    (4, 1),
)


def fold(words, shift, mask):
    return words & mask, lax.shift_right_logical(words, shift) & mask


def tally(ids_ref, start, places):
    bag = ids_ref.shape[0]
    lanes = places.shape[1]
    low_bits = places.shape[0]
    shift = low_bits.bit_length() - 1
    rows = [ids_ref[pl.ds(8 * g, 8), pl.ds(start, lanes)] for g in range(bag // 8)]
    lows = [row & (low_bits - 1) for row in rows]
    units = [jnp.left_shift(1, (row >> shift) << 1) for row in rows]

    def mark(j):
        low = lows[j // 8][j % 8 : j % 8 + 1, :]
        unit = units[j // 8][j % 8 : j % 8 + 1, :]
        return jnp.where(low == places, unit, 0)

    def add(left, right):
        return right if left is None else [a + b for a, b in zip(left, right)]

    nibbles = None
    bytes_ = None
    held = 0
    for start_j in range(0, bag, 3):
        group = range(start_j, min(start_j + 3, bag))
        words = mark(group[0])
        for j in group[1:]:
            words = words + mark(j)
        nibbles = add(nibbles, fold(words, 2, 0x33333333))
        held += len(group)
        if held > 12 or group[-1] == bag - 1:
            even = fold(nibbles[0], 4, 0x0F0F0F0F)
            odd = fold(nibbles[1], 4, 0x0F0F0F0F)
            bytes_ = add(bytes_, [even[0], odd[0], even[1], odd[1]])
            nibbles = None
            held = 0
    return jnp.concatenate(bytes_, axis=0)


def pool(ids_ref, table_ref, packed_ref, pooled_ref):
    samples = ids_ref.shape[1]
    active = table_ref.shape[0]
    lanes = 128
    fields = active // lanes
    places = lax.broadcasted_iota(jnp.int32, (lanes // 4, lanes), 0)
    chunks = samples // lanes

    def count(index, carry):
        packed_ref[index] = tally(ids_ref, pl.multiple_of(index * lanes, lanes), places)
        return carry

    lax.fori_loop(0, chunks, count, 0, unroll=UNROLL)

    def spread(words):
        turned = words.T
        return jnp.concatenate(
            [
                ((turned >> (8 * field)) & 255).astype(jnp.float32).astype(jnp.bfloat16)
                for field in range(fields)
            ],
            axis=1,
        )

    def look_up(index, carry):
        counts = jnp.concatenate(
            [spread(packed_ref[index * BATCH + part]) for part in range(BATCH)], axis=0
        )
        start = pl.multiple_of(index * BATCH * lanes, BATCH * lanes)
        pooled_ref[pl.ds(start, BATCH * lanes), :] = jnp.dot(
            counts, table_ref[...], preferred_element_type=jnp.float32
        )
        return carry

    lax.fori_loop(0, chunks // BATCH, look_up, 0)


def decode(exponent, fraction):
    return jnp.exp2(exponent.astype(jnp.float32)) * (fraction.astype(jnp.float32) / PARTS)


def encode(top):
    exponent = jnp.floor(jnp.log2(jnp.maximum(top, 1e-30))) + 1.0
    fraction = (top * jnp.exp2(-exponent) * PARTS).astype(jnp.int32) + 1
    return exponent.astype(jnp.int32), fraction


def kernel(
    ids_hbm,
    table_hbm,
    order_ref,
    first_hbm,
    second_hbm,
    head_hbm,
    inter_hbm,
    out_ref,
    ids_v,
    table_v,
    packed,
    pooled,
    permuted,
    xsend,
    xall,
    wall,
    total,
    cross,
    relay,
    final,
    outsum,
    second_v,
    outbox,
    inbox,
    head_v,
    inter_v,
    spread_hi,
    spread_lo,
    load_sem,
    first_sem,
    w_send,
    w_recv,
    r_send,
    r_recv,
    x_send,
    x_recv,
    c_send,
    c_recv,
    f_send,
    f_recv,
    o_send,
    o_recv,
    near_sem,
    far_sem,
    open_sem,
    towers,
):
    tower = lax.axis_index("tower")
    dev = lax.axis_index("dev")
    core = lax.rem(dev, CORES)
    chip = dev // CORES
    col = chip // RING
    row = lax.rem(chip, RING)
    chunks, _, tile = wall.shape
    emb = table_v.shape[1]
    block = permuted.shape[0]

    def along(step):
        return lax.rem(row + step, RING)

    def at_row(place):
        return {"dev": (col * RING + place) * CORES + core}

    partner = {"dev": dev + 1 - 2 * core}
    across = {"dev": ((1 - col) * RING + row) * CORES + core}

    mine = pl.ds(pl.multiple_of(row * emb, emb), emb)
    loads = [
        pltpu.make_async_copy(ids_hbm, ids_v, load_sem.at[0]),
        pltpu.make_async_copy(table_hbm, table_v, load_sem.at[1]),
        pltpu.make_async_copy(second_hbm, second_v, load_sem.at[2]),
        pltpu.make_async_copy(head_hbm, head_v, load_sem.at[3]),
        pltpu.make_async_copy(inter_hbm, inter_v, load_sem.at[4]),
    ]
    firsts = [
        pltpu.make_async_copy(
            first_hbm.at[:, pl.ds(n * tile, tile)], wall.at[n, mine, :], first_sem.at[n]
        )
        for n in range(chunks)
    ]
    loads[0].start()
    loads[1].start()
    for copy in firsts:
        copy.start()

    barrier = pltpu.get_barrier_semaphore()
    devices = CORES * RING * 2
    gate = dev == GATE
    peers = [at_row(along(step))["dev"] for step in range(1, RING)]
    peers += [partner["dev"], across["dev"]]
    near = jnp.int32(0)
    others = [other for other in range(devices) if other != GATE]
    for peer in peers:
        near = near + jnp.where(peer == GATE, 1, 0)

    @pl.when(jnp.logical_not(gate))
    def _():
        for peer in peers:

            @pl.when(peer != GATE)
            def _():
                pl.semaphore_signal(
                    barrier, inc=1, device_id={"dev": peer}, device_id_type=MESH
                )

        pl.semaphore_wait(barrier, len(peers) + 1 - near)

        @pl.when(near == 1)
        def _():
            pl.semaphore_signal(near_sem, inc=1, device_id={"dev": GATE}, device_id_type=MESH)

        @pl.when(near == 0)
        def _():
            pl.semaphore_signal(far_sem, inc=1, device_id={"dev": GATE}, device_id_type=MESH)

    @pl.when(gate)
    def _():
        for other in others:
            pl.semaphore_signal(barrier, inc=1, device_id={"dev": other}, device_id_type=MESH)
        pl.semaphore_wait(near_sem, len(peers))

    def gate_towers():
        pl.semaphore_wait(far_sem, devices - 1 - len(peers))
        for step in range(1, towers):
            pl.semaphore_signal(
                barrier,
                inc=1,
                device_id={"tower": lax.rem(tower + step, towers)},
                device_id_type=MESH,
            )

    def gate_open():
        pl.semaphore_wait(barrier, towers - 1)
        for other in others:
            pl.semaphore_signal(open_sem, inc=1, device_id={"dev": other}, device_id_type=MESH)

    for copy in firsts:
        copy.wait()

    steps = (3, 1, 2)

    def send_w(n, step):
        return pltpu.make_async_remote_copy(
            src_ref=wall.at[pl.ds(*SPANS[n]), mine, :],
            dst_ref=wall.at[pl.ds(*SPANS[n]), mine, :],
            send_sem=w_send.at[n, step],
            recv_sem=w_recv.at[n, row],
            device_id=at_row(along(step)),
            device_id_type=MESH,
        )

    def forward(n, half):
        source = along(3) if half == 0 else along(1)
        span = pl.ds(pl.multiple_of(source * emb + half * (emb // 2), emb // 2), emb // 2)
        return pltpu.make_async_remote_copy(
            src_ref=wall.at[pl.ds(*SPANS[n]), span, :],
            dst_ref=wall.at[pl.ds(*SPANS[n]), span, :],
            send_sem=r_send.at[n, half],
            recv_sem=r_recv.at[n, half],
            device_id=at_row(along(1) if half == 0 else along(3)),
            device_id_type=MESH,
        )

    def forwarded(n, half):
        source = along(2)
        span = pl.ds(pl.multiple_of(source * emb + half * (emb // 2), emb // 2), emb // 2)
        return pltpu.make_async_remote_copy(
            src_ref=wall.at[pl.ds(*SPANS[n]), span, :],
            dst_ref=wall.at[pl.ds(*SPANS[n]), span, :],
            send_sem=r_send.at[n, half],
            recv_sem=r_recv.at[n, half],
            device_id=partner,
            device_id_type=MESH,
        )

    def w_steps(n):
        return steps[:2] if n < RELAYED else steps

    def arrived_w(n, step):
        source = along(step)
        span = pl.ds(pl.multiple_of(source * emb, emb), emb)
        return pltpu.make_async_remote_copy(
            src_ref=wall.at[pl.ds(*SPANS[n]), span, :],
            dst_ref=wall.at[pl.ds(*SPANS[n]), span, :],
            send_sem=w_send.at[n, step],
            recv_sem=w_recv.at[n, source],
            device_id=partner,
            device_id_type=MESH,
        )

    def half_of(kind):
        part = 1 - core if kind == 1 else core
        return pl.ds(pl.multiple_of(part * block, block), block)

    def x_slots(kind, place, span):
        if kind == 0:
            return xsend.at[0, place], xall.at[0, :, span]
        return xsend.at[1, place, half_of(kind), :], xall.at[1, half_of(kind), span]

    def send_x(kind, step):
        source, target = x_slots(kind, along(step), mine)
        return pltpu.make_async_remote_copy(
            src_ref=source,
            dst_ref=target,
            send_sem=x_send.at[kind, step],
            recv_sem=x_recv.at[kind, row],
            device_id=at_row(along(step)),
            device_id_type=MESH,
        )

    def arrived_x(kind, step):
        place = along(step)
        span = pl.ds(pl.multiple_of(place * emb, emb), emb)
        source, target = x_slots(kind, place, span)
        return pltpu.make_async_remote_copy(
            src_ref=source,
            dst_ref=target,
            send_sem=x_send.at[kind, step],
            recv_sem=x_recv.at[kind, place],
            device_id=partner,
            device_id_type=MESH,
        )

    def permute_rows(kind, place, store):
        x = 1 - col if kind == 0 else col
        for c in ((0, 1), (1 - core,), (core,))[kind]:
            start = ((x * RING + place) * CORES + c) * block

            def group(index, carry):
                for q in range(16):
                    source = order_ref[start + index * 16 + q]
                    permuted[pl.ds(index * 16 + q, 1), :] = pooled[pl.ds(source, 1), :]
                return carry

            lax.fori_loop(0, block // 16, group, 0)
            part = pl.ds(c * block, block) if kind == 0 else half_of(kind)
            store(part, permuted[...].astype(jnp.bfloat16))

    def permute_send(kind):
        for step in steps:
            place = along(step)

            def keep(part, value):
                xsend[min(kind, 1), place, part, :] = value

            permute_rows(kind, place, keep)
            send_x(kind, step).start()

    def permute_own(kind):
        def keep(part, value):
            xall[min(kind, 1), part, mine] = value

        permute_rows(kind, row, keep)

    for n in range(EARLY):
        for step in w_steps(n):
            send_w(n, step).start()
    pl.when(gate)(gate_towers)
    loads[0].wait()
    loads[1].wait()
    pool(ids_v, table_v, packed, pooled)
    for copy in loads[2:]:
        copy.start()
    def relay_rows(n):
        for half, near_step in ((0, 3), (1, 1)):
            arrived_w(n, near_step).wait_recv()
            forward(n, half).start()

    for n in range(AHEAD):
        relay_rows(n)
    permute_send(0)
    for n in range(AHEAD, RELAYED):
        relay_rows(n)
    for n in range(EARLY, len(SPANS)):
        for step in w_steps(n):
            send_w(n, step).start()
    permute_own(0)
    permute_send(1)
    permute_send(2)
    permute_own(1)
    permute_own(2)
    pl.when(gate)(gate_open)

    loads[4].wait()
    pairs = inter_v.shape[0]

    def widen(index, carry):
        start = pl.multiple_of(index * 16, 16)
        some = inter_v[pl.ds(start, 16), :]
        wide = jnp.broadcast_to(some[:, None, :], (16, 8, some.shape[1])).reshape(
            128, some.shape[1]
        )
        high = wide.astype(jnp.bfloat16)
        low = (wide - high.astype(jnp.float32)).astype(jnp.bfloat16)
        target = pl.multiple_of(index * 128, 128)
        spread_hi[pl.ds(target, 128), :] = high
        spread_lo[pl.ds(target, 128), :] = low
        return carry

    lax.fori_loop(0, pairs // 16, widen, 0)
    loads[2].wait()
    loads[3].wait()

    def cross_copy(kind, g):
        return pltpu.make_async_remote_copy(
            src_ref=total.at[kind, pl.ds(*GROUPS[g]), 1 - core],
            dst_ref=cross.at[kind, pl.ds(*GROUPS[g])],
            send_sem=c_send.at[kind, g],
            recv_sem=c_recv.at[kind, g],
            device_id=partner,
            device_id_type=MESH,
        )

    def final_copy(g):
        return pltpu.make_async_remote_copy(
            src_ref=relay.at[pl.ds(*GROUPS[g])],
            dst_ref=final.at[pl.ds(*GROUPS[g])],
            send_sem=f_send.at[g],
            recv_sem=f_recv.at[g],
            device_id=across,
            device_id_type=MESH,
        )

    def tiles(g):
        return range(GROUPS[g][0], sum(GROUPS[g]))

    def arrived_span(g):
        for index, (begin, _) in enumerate(SPANS):
            if begin in tiles(g):
                if index < RELAYED:
                    for half in range(2):
                        forwarded(index, half).wait_recv()
                else:
                    for step in steps:
                        arrived_w(index, step).wait_recv()

    def first_layer(kind, g):
        for n in tiles(g):
            if kind == 0:
                part = jnp.dot(xall[0], wall[n], preferred_element_type=jnp.float32)
                total[0, n] = part.reshape(CORES, block, tile)
            else:
                total[1, n, 1 - core if kind == 1 else core] = jnp.dot(
                    xall[1, half_of(kind), :], wall[n], preferred_element_type=jnp.float32
                )
        if kind < 2:
            cross_copy(kind, g).start()

    def add_cores(g):
        cross_copy(0, g).wait_recv()
        for n in tiles(g):
            part = total[0, n, core] + cross[0, n]
            exponent, fraction = encode(jnp.max(jnp.abs(part), axis=0, keepdims=True))
            steps_up = part * (LEVELS / decode(exponent, fraction)) + (LEVELS + 1.5)
            relay[n, :block, :] = (steps_up.astype(jnp.int32) - (LEVELS + 1)).astype(jnp.int16)
            line = lax.broadcasted_iota(jnp.int32, (16, tile), 0)
            code = jnp.where(line == 0, exponent, jnp.where(line == 1, fraction, 0))
            relay[n, block:, :] = code.astype(jnp.int16)
        final_copy(g).start()

    def second_layer(g):
        cross_copy(1, g).wait_recv()
        final_copy(g).wait_recv()
        hidden = []
        for n in tiles(g):
            code = final[n, block:, :].astype(jnp.int32)
            unit = decode(code[0:1], code[1:2]) * (1.0 / LEVELS)
            other = final[n, :block, :].astype(jnp.float32) * unit
            preact = total[1, n, core] + cross[1, n] + other
            hidden.append(jnp.maximum(preact, 0.0).astype(jnp.bfloat16))
        begin, count = GROUPS[g]
        part = jnp.dot(
            jnp.concatenate(hidden, axis=1),
            second_v[begin * tile : (begin + count) * tile, :],
            preferred_element_type=jnp.float32,
        )
        if g == 0:
            outsum[...] = part
        else:
            outsum[...] += part

    groups = len(GROUPS)
    for step in steps:
        arrived_x(0, step).wait_recv()
    for g in range(groups + 1):
        if g < groups:
            arrived_span(g)
            first_layer(0, g)
        if g >= 1:
            add_cores(g - 1)
    for step in steps:
        arrived_x(1, step).wait_recv()
    for g in range(groups):
        first_layer(1, g)
    for step in steps:
        arrived_x(2, step).wait_recv()
    for g in range(groups):
        first_layer(2, g)
    for g in range(groups):
        second_layer(g)

    share = outbox.shape[1]
    outbox[...] = outsum[...].reshape(towers, share, outsum.shape[1]).astype(jnp.bfloat16)

    depth = towers // 2

    def other_tower(dz, dx):
        return lax.rem(tower // 2 + dz, depth) * 2 + lax.rem(lax.rem(tower, 2) + dx, 2)

    def send_o(dz, dx):
        peer = other_tower(dz, dx)
        return pltpu.make_async_remote_copy(
            src_ref=outbox.at[peer],
            dst_ref=inbox.at[tower],
            send_sem=o_send.at[dz * 2 + dx],
            recv_sem=o_recv.at[tower],
            device_id={"tower": peer},
            device_id_type=MESH,
        )

    @pl.when(jnp.logical_not(gate))
    def _():
        pl.semaphore_wait(open_sem, 1)

    for dz, dx in reversed(HOPS):
        send_o(dz, dx).start()
    inbox[tower] = outbox[tower]

    def head_part(source):
        return jnp.dot(inbox[source], head_v[source], preferred_element_type=jnp.float32)

    head = head_part(tower)
    for dz, dx in HOPS:
        source = other_tower(dz, dx)
        pltpu.make_async_remote_copy(
            src_ref=outbox.at[source],
            dst_ref=inbox.at[source],
            send_sem=o_send.at[dz * 2 + dx],
            recv_sem=o_recv.at[source],
            device_id=partner,
            device_id_type=MESH,
        ).wait_recv()
        head = head + head_part(source)

    zwidth = inbox.shape[2]
    stacked = (
        inbox[...].astype(jnp.float32).reshape(towers * share, zwidth).astype(jnp.bfloat16)
    )
    gram = lax.dot_general(
        stacked, stacked, (((1,), (1,)), ((), ())), preferred_element_type=jnp.float32
    )
    left = lax.rem(lax.broadcasted_iota(jnp.int32, gram.shape, 0), share)
    right = lax.rem(lax.broadcasted_iota(jnp.int32, gram.shape, 1), share)
    gram = jnp.where(left == right, gram / math.sqrt(zwidth), 0.0)
    flat = jnp.concatenate(
        [gram[t * share : (t + 1) * share, :] for t in range(towers)], axis=1
    )
    flat_hi = flat.astype(jnp.bfloat16)
    rest = flat - flat_hi.astype(jnp.float32)
    both = jnp.concatenate([flat_hi.astype(jnp.float32), rest], axis=0).astype(jnp.bfloat16)
    twice = jnp.dot(both, spread_hi[...], preferred_element_type=jnp.float32)
    interact = twice[:share] + twice[share:]
    interact += jnp.dot(flat_hi, spread_lo[...], preferred_element_type=jnp.float32)
    out_ref[...] = head + interact

    for step in steps:
        send_x(0, step).wait_send()
        send_x(1, step).wait_send()
        send_x(2, step).wait_send()
        for n in range(len(SPANS)):
            if step in w_steps(n):
                send_w(n, step).wait_send()
    for n in range(RELAYED):
        for half in range(2):
            forward(n, half).wait_send()
    for g in range(groups):
        cross_copy(0, g).wait_send()
        cross_copy(1, g).wait_send()
        final_copy(g).wait_send()
    for dz, dx in HOPS:
        send_o(dz, dx).wait_send()


def on_device(ids, tables, order, w_first, w_second, w_head, w_interact):
    towers = lax.axis_size("tower")
    devices = lax.axis_size("dev")
    samples, bag = ids.shape[2:]
    active, emb = tables.shape[2:]
    hidden = w_first.shape[2]
    zwidth = w_second.shape[2]
    heads = w_head.shape[1]
    block = samples // devices
    share = block // towers
    quarter = samples // RING
    pairs = w_interact.shape[0]
    tile = hidden // CHUNKS
    vmem = pltpu.VMEM
    dma = pltpu.SemaphoreType.DMA
    anywhere = pl.BlockSpec(memory_space=pltpu.HBM)
    scores = pl.pallas_call(
        functools.partial(kernel, towers=towers),
        out_shape=jax.ShapeDtypeStruct((share, heads), jnp.float32),
        in_specs=[
            anywhere,
            anywhere,
            pl.BlockSpec(memory_space=pltpu.SMEM),
            anywhere,
            anywhere,
            anywhere,
            anywhere,
        ],
        out_specs=pl.BlockSpec(memory_space=vmem),
        scratch_shapes=[
            vmem((bag, samples), jnp.int32),
            vmem((active, emb), jnp.bfloat16),
            vmem((samples // 128, 128, 128), jnp.int32),
            vmem((samples, emb), jnp.float32),
            vmem((block, emb), jnp.float32),
            vmem((2, RING, quarter // 2, emb), jnp.bfloat16),
            vmem((2, quarter // 2, RING * emb), jnp.bfloat16),
            vmem((CHUNKS, RING * emb, tile), jnp.bfloat16),
            vmem((2, CHUNKS, CORES, block, tile), jnp.float32),
            vmem((2, CHUNKS, block, tile), jnp.float32),
            vmem((CHUNKS, block + 16, tile), jnp.int16),
            vmem((CHUNKS, block + 16, tile), jnp.int16),
            vmem((block, zwidth), jnp.float32),
            vmem((hidden, zwidth), jnp.bfloat16),
            vmem((towers, share, zwidth), jnp.bfloat16),
            vmem((towers, share, zwidth), jnp.bfloat16),
            vmem((towers, zwidth, heads), jnp.bfloat16),
            vmem((pairs, heads), jnp.float32),
            vmem((pairs * share, heads), jnp.bfloat16),
            vmem((pairs * share, heads), jnp.bfloat16),
            dma((5,)),
            dma((CHUNKS,)),
            dma((len(SPANS), RING)),
            dma((len(SPANS), RING)),
            dma((len(SPANS), 2)),
            dma((len(SPANS), 2)),
            dma((3, RING)),
            dma((3, RING)),
            dma((2, CHUNKS)),
            dma((2, CHUNKS)),
            dma((CHUNKS,)),
            dma((CHUNKS,)),
            dma((towers,)),
            dma((towers,)),
            pltpu.SemaphoreType.REGULAR,
            pltpu.SemaphoreType.REGULAR,
            pltpu.SemaphoreType.REGULAR,
        ],
        compiler_params=pltpu.CompilerParams(
            collective_id=0, has_side_effects=True, vmem_limit_bytes=32 * 1024 * 1024
        ),
    )(
        *(
            pltpu.with_memory_space_constraint(value, pltpu.HBM)
            for value in (
                jnp.swapaxes(ids[0, 0], 0, 1),
                tables[0, 0],
                order,
                w_first[0],
                w_second[0],
                w_head.reshape(towers, zwidth, heads),
                w_interact,
            )
        ),
    )
    return scores[None]


def solution(mesh):
    return jax.shard_map(
        on_device,
        mesh=mesh,
        in_specs=(
            P("tower", "dev", None, None),
            P("tower", "dev", None, None),
            P(),
            P("tower", "dev", None),
            P("tower", None, None),
            P(),
            P(),
        ),
        out_specs=P("dev", "tower", None),
        check_vma=False,
    )
```
